32 devices in a mesh: batch: 1 (over z), col: 4 (over y), row: 8 (over x, core).
Axes of the slice: x: 4, y: 4, z: 1, core: 2. Of those that a mesh axis runs over, the one named last changes fastest.
The devices are a block of a 4x4x8 slice.
Arguments:
- field: float32 [2048, 1024, 16], P(('batch', 'row'), 'col')
- lower_x: float32 [2048, 1024], P(('batch', 'row'), 'col')
- diag_x: float32 [2048, 1024], P(('batch', 'row'), 'col')
- upper_x: float32 [2048, 1024], P(('batch', 'row'), 'col')
- lower_y: float32 [2048, 1024], P(('batch', 'row'), 'col')
- diag_y: float32 [2048, 1024], P(('batch', 'row'), 'col')
- upper_y: float32 [2048, 1024], P(('batch', 'row'), 'col')
Outputs:
- output: float32 [2048, 1024, 16], P(('batch', 'row'), 'col')
All inputs are finite; a program needn't handle non-finite values.
Results may differ from the reference program's by a relative error of at most 0.001.
Values sent between devices are 32-bit elements.
A program may use at most 768 MiB of HBM per device.

```python
import jax
import jax.numpy as jnp
from jax import lax

NX = 2048
NY = 1024
FIELDS = 16
STEPS = 3


def draw_operator(key_diag, key_share):
    diagonal = 30.0 + 70.0 * jax.random.uniform(key_diag, (NX, NY), jnp.float32)
    share = 0.15 + 0.7 * jax.random.uniform(key_share, (NX, NY), jnp.float32)
    reach = diagonal - 0.2
    return -reach * share, diagonal, -reach * (1.0 - share)


def setup_inputs(seed: int = 0, part: int = 0) -> dict:
    key = jax.random.fold_in(jax.random.key(seed), part)
    keys = jax.random.split(key, 5)
    field = jax.random.normal(keys[0], (NX, NY, FIELDS), jnp.float32)
    lower_x, diag_x, upper_x = draw_operator(keys[1], keys[2])
    lower_y, diag_y, upper_y = draw_operator(keys[3], keys[4])
    return {"field": field, "lower_x": lower_x, "diag_x": diag_x, "upper_x": upper_x, "lower_y": lower_y, "diag_y": diag_y, "upper_y": upper_y}


def explicit_rows(field, lower, diag, upper):
    before = jnp.concatenate([jnp.zeros_like(field[:1]), field[:-1]], axis=0)
    after = jnp.concatenate([field[1:], jnp.zeros_like(field[:1])], axis=0)
    return field - (lower[..., None] * before + diag[..., None] * field + upper[..., None] * after)


def thomas_rows(right_side, lower, diag, upper):
    def forward(carry, slab):
        cp_prev, g_prev = carry
        low_i, dia_i, upp_i, r_i = slab
        den_i = 1.0 + dia_i - low_i * cp_prev
        cp_i = upp_i / den_i
        g_i = (r_i - low_i[:, None] * g_prev) / den_i[:, None]
        return (cp_i, g_i), (cp_i, g_i)

    start = (jnp.zeros_like(diag[0]), jnp.zeros_like(right_side[0]))
    outcome = lax.scan(forward, start, (lower, diag, upper, right_side))
    cp_all, g_all = outcome[1]

    def backward(sol_next, slab):
        cp_i, g_i = slab
        sol_i = g_i - cp_i[:, None] * sol_next
        return sol_i, sol_i

    return lax.scan(backward, jnp.zeros_like(right_side[0]), (cp_all, g_all), reverse=True)[1]


def reference(field, lower_x, diag_x, upper_x, lower_y, diag_y, upper_y):
    lower_t = lower_y.T
    diag_t = diag_y.T
    upper_t = upper_y.T

    def one_step(state, unused):
        r_one = jnp.swapaxes(explicit_rows(jnp.swapaxes(state, 0, 1), lower_t, diag_t, upper_t), 0, 1)
        s_mid = thomas_rows(r_one, lower_x, diag_x, upper_x)
        r_two = explicit_rows(s_mid, lower_x, diag_x, upper_x)
        new_state = jnp.swapaxes(thomas_rows(jnp.swapaxes(r_two, 0, 1), lower_t, diag_t, upper_t), 0, 1)
        return new_state, None

    final = lax.scan(one_step, field, None, length=STEPS)[0]
    return final
```

```python
import functools

import jax
import jax.numpy as jnp
from jax import lax
from jax.experimental import pallas as pl
from jax.experimental.pallas import tpu as pltpu
from jax.sharding import PartitionSpec as P

STEPS = 3
F32 = jnp.float32
LANES = 128
SUB = 8
MESH = pl.DeviceIdType.MESH
X, Y = 0, 1


def adi_kernel(axes, field, lower_x, diag_x, upper_x, lower_y, diag_y, upper_y, out,
               nat, rx, ry, hs, pa, pb, pc, nd, md, ne, me_, ln, cn, un, an, m2, d2, w2, v2, r0, rn,
               gs, gc_x, gc_y, red_x, red_y, sx, sy, ex, ey, gt, ss, halo_s, halo_r,
               in_sem, out_sem, gsend_x, gsend_y, grecv_x, grecv_y, ssx, ssy, rsx, rsy, hsend, hrecv):
    (row_name, parts_x), (col_name, parts_y) = axes
    n = lower_x.shape[0]
    tiles = n // LANES
    chunks = field.shape[1] // SUB
    pitch = 2 * tiles
    half = n // 2
    pos = (lax.axis_index(row_name), lax.axis_index(col_name))
    parts = (parts_x, parts_y)
    names = (row_name, col_name)
    exch = (ex, ey)
    send = (sx, sy)
    send_sems = (ssx, ssy)
    recv_sems = (rsx, rsy)
    gather = (gc_x, gc_y)
    reduced = (red_x, red_y)

    def others(axis):
        return [lax.rem(pos[axis] + off, parts[axis]) for off in range(1, parts[axis])]

    loads = []
    for slot, ref in enumerate((lower_x, diag_x, upper_x, lower_y, diag_y, upper_y)):
        loads.append(pltpu.make_async_copy(ref, nat.at[slot], in_sem.at[slot]))
    field_loads = []
    for c in range(chunks):
        for t in range(tiles):
            field_loads.append(pltpu.make_async_copy(
                field.at[:, pl.ds(c * SUB, SUB), pl.ds(t * LANES, LANES)],
                rx.at[c, t].reshape(n, SUB, LANES), in_sem.at[6 + c * tiles + t]))
    for copy in loads + field_loads:
        copy.start()

    halo_r[...] = jnp.zeros_like(halo_r)
    barrier = pltpu.get_barrier_semaphore()
    for axis in (X, Y):
        for other in others(axis):
            pl.semaphore_signal(barrier, 1, device_id={names[axis]: other}, device_id_type=MESH)
    pl.semaphore_wait(barrier, parts_x + parts_y - 2)

    for copy in loads:
        copy.wait()
    for t in range(tiles):
        cols = pl.ds(t * LANES, LANES)
        pa[pl.ds(t, n, stride=pitch), :] = nat[0, :, cols]
        pb[pl.ds(t, n, stride=pitch), :] = nat[1, :, cols] + 1.0
        pc[pl.ds(t, n, stride=pitch), :] = nat[2, :, cols]
        for s in range(tiles):
            rows = pl.ds(s * LANES, LANES)
            dest = pl.ds(t * LANES * pitch + tiles + s, LANES, stride=pitch)
            pa[dest, :] = nat[3, rows, cols].T
            pb[dest, :] = nat[4, rows, cols].T + 1.0
            pc[dest, :] = nat[5, rows, cols].T

    unroll = 8
    zero = jnp.zeros((pitch, LANES), F32)
    one = jnp.ones((pitch, LANES), F32)

    def at_row(k, u):
        return pl.ds(pl.multiple_of(k * (unroll * pitch), unroll * pitch) + u * pitch, pitch)

    def pivots(g, state):
        dp, dq, c_prev, ep, eq, a_next = state
        h = n // unroll - 1 - g
        for u in range(unroll):
            up, down = at_row(g, u), at_row(h, unroll - 1 - u)
            nd[up, :] = dp
            new = pb[up, :] * dp - (pa[up, :] * c_prev) * dq
            md[up, :] = new
            dp, dq, c_prev = new, dp, pc[up, :]
            ne[down, :] = ep
            new = pb[down, :] * ep - (a_next * pc[down, :]) * eq
            me_[down, :] = new
            ep, eq, a_next = new, ep, pa[down, :]
            if u == unroll // 2 - 1:
                scale_d, scale_e = 1.0 / dp, 1.0 / ep
        return dp * scale_d, dq * scale_d, c_prev, ep * scale_e, eq * scale_e, a_next

    lax.fori_loop(0, n // unroll, pivots, (one, zero, zero, one, zero, zero))

    low_half = lax.broadcasted_iota(jnp.int32, (SUB, LANES), 0) < pitch
    blocks = n * pitch // SUB
    step_rows = 4

    def ratios(g, state):
        prev_m, next_d = state
        for u in range(step_rows):
            up = pl.ds(pl.multiple_of(g * (SUB * step_rows), SUB * step_rows) + u * SUB, SUB)
            down = pl.ds(pl.multiple_of((blocks // step_rows - 1 - g) * (SUB * step_rows), SUB * step_rows)
                         + (step_rows - 1 - u) * SUB, SUB)
            minv = nd[up, :] / md[up, :]
            m2[up, :] = minv + minv
            cn[up, :] = -pc[up, :] * minv
            turned = pltpu.roll(minv, pitch, 0)
            ln[up, :] = -pa[up, :] * jnp.where(low_half, prev_m, turned)
            prev_m = turned
            dinv = ne[down, :] / me_[down, :]
            d2[down, :] = dinv + dinv
            an[down, :] = -pa[down, :] * dinv
            turned = pltpu.roll(dinv, pitch, 0)
            un[down, :] = -pc[down, :] * jnp.where(low_half, turned, next_d)
            next_d = turned
        return prev_m, next_d

    blank = jnp.zeros((SUB, LANES), F32)
    lax.fori_loop(0, blocks // step_rows, ratios, (blank, blank))

    first, last = pl.ds(0, pitch), pl.ds((n - 1) * pitch, pitch)

    def products(g, state):
        col0, row0, coln, rown, un_prev, ln_next = state
        h = n // unroll - 1 - g
        for u in range(unroll):
            up, down = at_row(g, u), at_row(h, unroll - 1 - u)
            start = jnp.logical_and(g == 0, u == 0) if u == 0 else None
            f0, f1 = an[up, :], un_prev
            b0, b1 = cn[down, :], ln_next
            if u == 0:
                f0, f1 = jnp.where(start, one, f0), jnp.where(start, one, f1)
                b0, b1 = jnp.where(start, one, b0), jnp.where(start, one, b1)
            col0, row0, coln, rown = col0 * f0, row0 * f1, coln * b0, rown * b1
            w2[up, :], r0[up, :], v2[down, :], rn[down, :] = col0, row0, coln, rown
            un_prev, ln_next = un[up, :], ln[down, :]
        return col0, row0, coln, rown, un_prev, ln_next

    d_first, m_last = 0.5 * d2[first, :], 0.5 * m2[last, :]
    lax.fori_loop(0, n // unroll, products,
                  (-pa[first, :] * d2[first, :], d_first, -pc[last, :] * m2[last, :], m_last, one, one))

    for q, (ref, rows) in enumerate(((w2, first), (w2, last), (v2, first), (v2, last))):
        gs[pl.ds(q * pitch, pitch), :] = -0.5 * ref[rows, :]
    gathers = ((gsend_x, grecv_x), (gsend_y, grecv_y))
    for axis in (X, Y):
        gather[axis][pos[axis]] = gs[...]
        for off, other in enumerate(others(axis)):
            pltpu.make_async_remote_copy(
                src_ref=gs, dst_ref=gather[axis].at[pos[axis]], send_sem=gathers[axis][0].at[off],
                recv_sem=gathers[axis][1].at[pos[axis]], device_id={names[axis]: other}, device_id_type=MESH).start()

    def reduce_lines(axis):
        count, me = parts[axis], pos[axis]
        for off, other in enumerate(others(axis)):
            pltpu.make_async_remote_copy(
                src_ref=gs, dst_ref=gather[axis].at[other], send_sem=gathers[axis][0].at[off],
                recv_sem=gathers[axis][1].at[other], device_id={names[axis]: other}, device_id_type=MESH).wait()
        part = lambda p, q: gather[axis][p, pl.ds(q * pitch + axis * tiles, tiles), :]
        nil = jnp.zeros((tiles, LANES), F32)
        unit = jnp.ones((tiles, LANES), F32)
        mu, rho, tau = [None] * count, [None] * count, [None] * count
        prev = nil
        for p in range(count):
            wf, wt, vf, vt = (part(p, q) for q in range(4))
            kappa = 1.0 / (1.0 - wf * prev)
            mu[p], rho[p] = wt * prev * kappa, wt * kappa
            prev = tau[p] = vt + mu[p] * vf
        nu, omega, sigma = [None] * count, [None] * count, [None] * count
        prev = nil
        for p in reversed(range(count)):
            wf, wt, vf, vt = (part(p, q) for q in range(4))
            kappa = 1.0 / (1.0 - vt * prev)
            nu[p], omega[p] = vf * prev * kappa, vf * kappa
            prev = sigma[p] = wf + nu[p] * wt
        pick = lambda values, at: sum(jnp.where(at == p, v, nil) for p, v in enumerate(values))
        tau_b, sigma_a = pick(tau, me - 1), pick(sigma, me + 1)
        mu_me, nu_me = pick(mu, me), pick(nu, me)
        wf, wt, vf, vt = (part(me, q) for q in range(4))
        det = 1.0 / ((1.0 - tau_b * wf) * (1.0 - sigma_a * vt) - (tau_b * vf) * (sigma_a * wt))
        k11, k12 = (1.0 - sigma_a * vt) * det, tau_b * vf * det
        k21, k22 = sigma_a * wt * det, (1.0 - tau_b * wf) * det
        low, high = [None] * count, [None] * count
        for p in reversed(range(count)):
            onward = -rho[p + 1] * low[p + 1] if p + 1 < count else nil
            low[p] = jnp.where(me - 1 == p, unit, jnp.where(p < me - 1, onward, nil))
        for p in range(count):
            onward = -omega[p - 1] * high[p - 1] if p else nil
            high[p] = jnp.where(me + 1 == p, unit, jnp.where(p > me + 1, onward, nil))
        table = reduced[axis]
        put = lambda index, value: table.__setitem__((pl.ds(index * tiles, tiles), slice(None)), value)
        for p in range(count):
            put(p, k11 * low[p] + k12 * high[p] + jnp.where(me == p, -k11 * tau_b, nil))
            put(count + 1 + p, k21 * low[p] + k22 * high[p] + jnp.where(me == p, -k21 * tau_b, nil))
        put(count, -k12 * sigma_a)
        put(2 * count + 1, -k22 * sigma_a)
        put(2 * count + 2, mu_me)
        put(2 * count + 3, nu_me)

    def exchange(axis, stage, c, off, slot_here, other):
        sel = jnp.where(other > pos[axis], 1, 0)
        return pltpu.make_async_remote_copy(
            src_ref=send[axis].at[stage, c, sel], dst_ref=exch[axis].at[stage, c, slot_here],
            send_sem=send_sems[axis].at[stage, c, off], recv_sem=recv_sems[axis].at[stage, c, slot_here],
            device_id={names[axis]: other}, device_id_type=MESH)

    def publish(axis, stage, c):
        count, table = parts[axis], reduced[axis]
        for t in range(tiles):
            head, tail = exch[axis][stage, c, pos[axis], t], gt[c, t]
            mu = table[pl.ds((2 * count + 2) * tiles + t, 1), :]
            nu = table[pl.ds((2 * count + 3) * tiles + t, 1), :]
            send[axis][stage, c, 1, t] = tail + mu * head
            send[axis][stage, c, 0, t] = head + nu * tail
        for off, other in enumerate(others(axis)):
            exchange(axis, stage, c, off, pos[axis], other).start()

    def neighbours(axis, stage, c):
        count, table = parts[axis], reduced[axis]
        for off, other in enumerate(others(axis)):
            exchange(axis, stage, c, off, other, other).wait()
        for t in range(tiles):
            for side in range(2):
                base = side * (count + 1) * tiles + t
                total = table[pl.ds(base + count * tiles, 1), :] * gt[c, t]
                for p in range(count):
                    total = total + table[pl.ds(base + p * tiles, 1), :] * exch[axis][stage, c, p, t]
                ss[side, t] = total

    def turn(src, dst, c, axis, to, stage, correct, dots):
        def column(f, kt):
            heads = tails = None
            for lt in range(tiles):
                block = src[c, lt, pl.ds(kt * (LANES * SUB) + f, LANES, stride=SUB), :]
                if correct:
                    rows = pl.ds(kt * (LANES * pitch) + (axis * tiles + lt), LANES, stride=pitch)
                    block = (block + w2[rows, :] * ss[0, lt, pl.ds(f, 1), :]
                             + v2[rows, :] * ss[1, lt, pl.ds(f, 1), :])
                if dots is None:
                    block = block * 0.5
                flipped = block.T
                dst[c, kt, pl.ds(lt * LANES * SUB + f, LANES, stride=SUB), :] = flipped
                if dots:
                    rows = pl.ds(lt * LANES * pitch + to * tiles + kt, LANES, stride=pitch)
                    fold = lambda v: v.reshape(LANES // SUB, SUB, LANES).sum(axis=0)
                    h, s = fold(flipped * r0[rows, :]), fold(flipped * rn[rows, :])
                    heads = h if heads is None else heads + h
                    tails = s if tails is None else tails + s
            if dots:
                exch[to][stage, c, pos[to], kt, pl.ds(f, 1), :] = jnp.sum(heads, axis=0, keepdims=True)
                gt[c, kt, pl.ds(f, 1), :] = jnp.sum(tails, axis=0, keepdims=True)
            return kt

        lax.fori_loop(0, tiles, lambda kt, carry: (lax.fori_loop(0, SUB, column, kt, unroll=True), carry)[1], 0)

    cells = [(c, t) for c in range(chunks) for t in range(tiles)]

    def solve_block(ref, axis, minus):
        def coef(array, k, t):
            return array[pl.ds(k * pitch + axis * tiles + t, 1), :]

        def forward(k, state):
            ups, downs = list(state[0]), list(state[1])
            r = n - 1 - k
            for s, (c, t) in enumerate(cells):
                here = pl.ds(pl.multiple_of(k * SUB, SUB), SUB)
                ups[s] = ref[c, t, here, :] + coef(ln, k, t) * ups[s]
                hs[c, t, here, :] = ups[s]
                here = pl.ds(pl.multiple_of(r * SUB, SUB), SUB)
                downs[s] = ref[c, t, here, :] + coef(un, r, t) * downs[s]
                hs[c, t, here, :] = downs[s]
            return tuple(ups), tuple(downs)

        init = tuple(blank for _ in cells)
        ups, downs = lax.fori_loop(0, half, forward, (init, init), unroll=unroll)
        lo, hi = half - 1, half

        def place(c, t, k, value):
            here = pl.ds(pl.multiple_of(k * SUB, SUB), SUB)
            ref[c, t, here, :] = value - ref[c, t, here, :] if minus else value

        low_s, high_s = [], []
        for s, (c, t) in enumerate(cells):
            c_lo, a_hi = coef(cn, lo, t), coef(an, hi, t)
            kappa = 1.0 / (1.0 - c_lo * a_hi)
            h_hi = coef(d2, hi, t) * downs[s]
            s_lo = kappa * (coef(m2, lo, t) * ups[s] + c_lo * h_hi)
            low_s.append(s_lo)
            high_s.append(h_hi + a_hi * s_lo)
            place(c, t, lo, low_s[s])
            place(c, t, hi, high_s[s])

        def backward(step, state):
            lows, highs = list(state[0]), list(state[1])
            k, r = half - 1 - step, half + step
            for s, (c, t) in enumerate(cells):
                here = pl.ds(pl.multiple_of(k * SUB, SUB), SUB)
                lows[s] = coef(m2, k, t) * hs[c, t, here, :] + coef(cn, k, t) * lows[s]
                place(c, t, k, lows[s])
                here = pl.ds(pl.multiple_of(r * SUB, SUB), SUB)
                highs[s] = coef(d2, r, t) * hs[c, t, here, :] + coef(an, r, t) * highs[s]
                place(c, t, r, highs[s])
            return tuple(lows), tuple(highs)

        state = lax.fori_loop(1, unroll, backward, (tuple(low_s), tuple(high_s)), unroll=True)
        lax.fori_loop(unroll, half, backward, state, unroll=unroll)

    for copy in field_loads:
        copy.wait()
    lax.fori_loop(0, chunks, lambda c, carry: (turn(rx, ry, c, X, Y, 0, False, False), carry)[1], 0)
    me_y = pos[Y]
    tail_rows = pl.ds((n - 1) * SUB, SUB)
    for c, t in cells:
        halo_s[0, c, t] = ry[c, t, pl.ds(0, SUB), :]
        halo_s[1, c, t] = ry[c, t, tail_rows, :]

    def halo(side, other):
        return pltpu.make_async_remote_copy(
            src_ref=halo_s.at[side], dst_ref=halo_r.at[1 - side], send_sem=hsend.at[side], recv_sem=hrecv.at[1 - side],
            device_id={col_name: other}, device_id_type=MESH)

    has_before, has_after = me_y > 0, me_y < parts_y - 1

    @pl.when(has_before)
    def _():
        halo(0, me_y - 1).start()

    @pl.when(has_after)
    def _():
        halo(1, me_y + 1).start()

    def explicit(k, state):
        befores, heres = list(state[0]), list(state[1])
        coef = lambda array, t: array[pl.ds(k * pitch + tiles + t, 1), :]
        for s, (c, t) in enumerate(cells):
            ahead = ry[c, t, pl.ds(pl.multiple_of(jnp.minimum(k + 1, n - 1) * SUB, SUB), SUB), :]
            ahead = jnp.where(k == n - 1, blank, ahead)
            ry[c, t, pl.ds(pl.multiple_of(k * SUB, SUB), SUB), :] = heres[s] - (
                coef(pa, t) * befores[s] + (coef(pb, t) - 1.0) * heres[s] + coef(pc, t) * ahead)
            befores[s], heres[s] = heres[s], ahead
        return tuple(befores), tuple(heres)

    lax.fori_loop(0, n, explicit,
                  (tuple(blank for _ in cells), tuple(ry[c, t, pl.ds(0, SUB), :] for c, t in cells)), unroll=unroll)

    @pl.when(has_before)
    def _():
        halo(0, me_y - 1).wait_send()
        halo(1, me_y - 1).wait_recv()

    @pl.when(has_after)
    def _():
        halo(1, me_y + 1).wait_send()
        halo(0, me_y + 1).wait_recv()

    for c, t in cells:
        ry[c, t, pl.ds(0, SUB), :] = ry[c, t, pl.ds(0, SUB), :] - pa[pl.ds(tiles + t, 1), :] * halo_r[0, c, t]
        ry[c, t, tail_rows, :] = (ry[c, t, tail_rows, :]
                                  - pc[pl.ds((n - 1) * pitch + tiles + t, 1), :] * halo_r[1, c, t])

    def each_chunk(body):
        lax.fori_loop(0, chunks, lambda c, carry: (body(c), carry)[1], 0)

    def start_x(c):
        turn(ry, rx, c, Y, X, 0, False, True)
        publish(X, 0, c)

    reduce_lines(X)
    each_chunk(start_x)
    reduce_lines(Y)

    def x_half(stage):
        def finish(c):
            neighbours(X, stage, c)
            turn(rx, ry, c, X, Y, stage, True, True)
            publish(Y, stage, c)

        solve_block(rx, X, True)
        each_chunk(finish)

    def step(stage, carry):
        def finish(c):
            neighbours(Y, stage, c)
            turn(ry, rx, c, Y, X, stage + 1, True, True)
            publish(X, stage + 1, c)

        x_half(stage)
        solve_block(ry, Y, True)
        each_chunk(finish)
        return carry

    lax.fori_loop(0, STEPS - 1, step, 0)
    x_half(STEPS - 1)
    solve_block(ry, Y, False)
    for c in range(chunks):
        neighbours(Y, STEPS - 1, c)
        turn(ry, rx, c, Y, X, STEPS, True, None)
        for t in range(tiles):
            pltpu.make_async_copy(rx.at[c, t].reshape(n, SUB, LANES),
                                  out.at[:, pl.ds(c * SUB, SUB), pl.ds(t * LANES, LANES)],
                                  out_sem.at[c * tiles + t]).start()
    for c, t in cells:
        pltpu.make_async_copy(rx.at[c, t].reshape(n, SUB, LANES),
                              out.at[:, pl.ds(c * SUB, SUB), pl.ds(t * LANES, LANES)],
                              out_sem.at[c * tiles + t]).wait()


def solution(mesh):
    parts_x, parts_y = mesh.shape["row"], mesh.shape["col"]
    field_spec = P(("batch", "row"), "col", None)
    coeff_spec = P(("batch", "row"), "col")

    def local_steps(field, *coeffs):
        n, fields = field.shape[0], field.shape[2]
        tiles, chunks = n // LANES, fields // SUB
        packed = pltpu.VMEM((n * 2 * tiles, LANES), F32)
        big = pltpu.VMEM((chunks, tiles, n * SUB, LANES), F32)
        dma = pltpu.SemaphoreType.DMA
        line = lambda count: pltpu.VMEM((STEPS, chunks, count, tiles, SUB, LANES), F32)
        table = lambda count: pltpu.VMEM(((2 * count + 4) * tiles, LANES), F32)
        small = pltpu.VMEM((2, chunks, tiles, SUB, LANES), F32)
        message = (8 * tiles, LANES)
        scratch = [
            pltpu.VMEM((6, n, n), F32), big, big, big, *([packed] * 17),
            pltpu.VMEM(message, F32), pltpu.VMEM((parts_x,) + message, F32), pltpu.VMEM((parts_y,) + message, F32),
            table(parts_x), table(parts_y), line(2), line(2), line(parts_x), line(parts_y),
            pltpu.VMEM((chunks, tiles, SUB, LANES), F32), pltpu.VMEM((2, tiles, SUB, LANES), F32), small, small,
            dma((6 + chunks * tiles,)), dma((chunks * tiles,)), dma((parts_x,)), dma((parts_y,)), dma((parts_x,)), dma((parts_y,)),
            dma((STEPS, chunks, parts_x)), dma((STEPS, chunks, parts_y)),
            dma((STEPS, chunks, parts_x)), dma((STEPS, chunks, parts_y)), dma((2,)), dma((2,)),
        ]
        anywhere = pl.BlockSpec(memory_space=pl.ANY)
        turned = jnp.transpose(field, (0, 2, 1))
        result = pl.pallas_call(
            functools.partial(adi_kernel, (("row", parts_x), ("col", parts_y))),
            out_shape=jax.ShapeDtypeStruct(turned.shape, F32),
            in_specs=[anywhere] * 7, out_specs=anywhere, scratch_shapes=scratch,
            compiler_params=pltpu.CompilerParams(collective_id=0, has_side_effects=True, vmem_limit_bytes=48 * 1024 * 1024),
            name="adi_steps",
        )(turned, *coeffs)
        return jnp.transpose(result, (0, 2, 1))

    return jax.shard_map(local_steps, mesh=mesh, in_specs=(field_spec,) + (coeff_spec,) * 6, out_specs=field_spec, check_vma=False)
```

```python
import functools

import jax
import jax.numpy as jnp
from jax import lax
from jax.experimental import pallas as pl
from jax.experimental.pallas import tpu as pltpu
from jax.sharding import PartitionSpec as P

STEPS = 3
F32 = jnp.float32
LANES = 128
SUB = 8
PITCH = SUB + 1
MESH = pl.DeviceIdType.MESH
X, Y = 0, 1


def adi_kernel(axes, field, lower_x, diag_x, upper_x, lower_y, diag_y, upper_y, out,
               nat, stage_in, rs, hs, qs, pa, pb, pc, nd, md, ne, me_, ln, cn, un, an, m2, d2, w2, v2, r0, rn,
               gs, gc_x, gc_y, red_x, red_y, sx, sy, ex, ey, gt, ss, halo_s, halo_r,
               coef_sem, field_sem, gsend, grecv, send_sem, recv_sem, hsend, hrecv):
    (row_name, parts_x), (col_name, parts_y) = axes
    n = lower_x.shape[0]
    tiles = n // LANES
    chunks = field.shape[1] // SUB
    pitch = 2 * tiles
    half = n // 2
    pos = (lax.axis_index(row_name), lax.axis_index(col_name))
    parts = (parts_x, parts_y)
    names = (row_name, col_name)
    exch = (ex, ey)
    send = (sx, sy)
    gather = (gc_x, gc_y)
    reduced = (red_x, red_y)

    def others(axis):
        return [lax.rem(pos[axis] + off, parts[axis]) for off in range(1, parts[axis])]

    for slot, ref in enumerate((lower_x, diag_x, upper_x, lower_y, diag_y, upper_y)):
        pltpu.make_async_copy(ref, nat.at[slot], coef_sem).start()
    for c in range(chunks):
        for t in range(tiles):
            pltpu.make_async_copy(field.at[:, pl.ds(c * SUB, SUB), pl.ds(t * LANES, LANES)],
                                  stage_in.at[c, t].reshape(n, SUB, LANES), field_sem).start()

    halo_r[...] = jnp.zeros_like(halo_r)
    barrier = pltpu.get_barrier_semaphore()
    for axis in (X, Y):
        for other in others(axis):
            pl.semaphore_signal(barrier, 1, device_id={names[axis]: other}, device_id_type=MESH)

    pltpu.make_async_copy(nat, nat, coef_sem).wait()
    for t in range(tiles):
        cols = pl.ds(t * LANES, LANES)
        pa[pl.ds(t, n, stride=pitch), :] = nat[0, :, cols]
        pb[pl.ds(t, n, stride=pitch), :] = nat[1, :, cols] + 1.0
        pc[pl.ds(t, n, stride=pitch), :] = nat[2, :, cols]
        for s in range(tiles):
            rows = pl.ds(s * LANES, LANES)
            dest = pl.ds(t * LANES * pitch + tiles + s, LANES, stride=pitch)
            pa[dest, :] = nat[3, rows, cols].T
            pb[dest, :] = nat[4, rows, cols].T + 1.0
            pc[dest, :] = nat[5, rows, cols].T

    unroll = 8
    zero = jnp.zeros((pitch, LANES), F32)
    one = jnp.ones((pitch, LANES), F32)

    def at_row(k, u):
        return pl.ds(pl.multiple_of(k * (unroll * pitch), unroll * pitch) + u * pitch, pitch)

    def pivots(g, state):
        dp, dq, c_prev, ep, eq, a_next = state
        h = n // unroll - 1 - g
        for u in range(unroll):
            up, down = at_row(g, u), at_row(h, unroll - 1 - u)
            nd[up, :] = dp
            new = pb[up, :] * dp - (pa[up, :] * c_prev) * dq
            md[up, :] = new
            dp, dq, c_prev = new, dp, pc[up, :]
            ne[down, :] = ep
            new = pb[down, :] * ep - (a_next * pc[down, :]) * eq
            me_[down, :] = new
            ep, eq, a_next = new, ep, pa[down, :]
            if u == unroll // 2 - 1:
                scale_d, scale_e = 1.0 / dp, 1.0 / ep
        return dp * scale_d, dq * scale_d, c_prev, ep * scale_e, eq * scale_e, a_next

    lax.fori_loop(0, n // unroll, pivots, (one, zero, zero, one, zero, zero))

    low_half = lax.broadcasted_iota(jnp.int32, (SUB, LANES), 0) < pitch
    blocks = n * pitch // SUB
    step_rows = 4

    def ratios(g, state):
        prev_m, next_d = state
        for u in range(step_rows):
            up = pl.ds(pl.multiple_of(g * (SUB * step_rows), SUB * step_rows) + u * SUB, SUB)
            down = pl.ds(pl.multiple_of((blocks // step_rows - 1 - g) * (SUB * step_rows), SUB * step_rows)
                         + (step_rows - 1 - u) * SUB, SUB)
            minv = nd[up, :] / md[up, :]
            m2[up, :] = minv + minv
            cn[up, :] = -pc[up, :] * minv
            turned = pltpu.roll(minv, pitch, 0)
            ln[up, :] = -pa[up, :] * jnp.where(low_half, prev_m, turned)
            prev_m = turned
            dinv = ne[down, :] / me_[down, :]
            d2[down, :] = dinv + dinv
            an[down, :] = -pa[down, :] * dinv
            turned = pltpu.roll(dinv, pitch, 0)
            un[down, :] = -pc[down, :] * jnp.where(low_half, turned, next_d)
            next_d = turned
        return prev_m, next_d

    blank = jnp.zeros((SUB, LANES), F32)
    lax.fori_loop(0, blocks // step_rows, ratios, (blank, blank))

    first, last = pl.ds(0, pitch), pl.ds((n - 1) * pitch, pitch)

    def products(g, state):
        col0, row0, coln, rown, un_prev, ln_next = state
        h = n // unroll - 1 - g
        for u in range(unroll):
            up, down = at_row(g, u), at_row(h, unroll - 1 - u)
            start = jnp.logical_and(g == 0, u == 0) if u == 0 else None
            f0, f1 = an[up, :], un_prev
            b0, b1 = cn[down, :], ln_next
            if u == 0:
                f0, f1 = jnp.where(start, one, f0), jnp.where(start, one, f1)
                b0, b1 = jnp.where(start, one, b0), jnp.where(start, one, b1)
            col0, row0, coln, rown = col0 * f0, row0 * f1, coln * b0, rown * b1
            w2[up, :], r0[up, :], v2[down, :], rn[down, :] = col0, row0, coln, rown
            un_prev, ln_next = un[up, :], ln[down, :]
        return col0, row0, coln, rown, un_prev, ln_next

    d_first, m_last = 0.5 * d2[first, :], 0.5 * m2[last, :]
    lax.fori_loop(0, n // unroll, products,
                  (-pa[first, :] * d2[first, :], d_first, -pc[last, :] * m2[last, :], m_last, one, one))

    for q, (ref, rows) in enumerate(((w2, first), (w2, last), (v2, first), (v2, last))):
        gs[pl.ds(q * pitch, pitch), :] = -0.5 * ref[rows, :]
    pl.semaphore_wait(barrier, parts_x + parts_y - 2)
    for axis in (X, Y):
        gather[axis][pos[axis]] = gs[...]
        for other in others(axis):
            pltpu.make_async_remote_copy(
                src_ref=gs, dst_ref=gather[axis].at[pos[axis]], send_sem=gsend, recv_sem=grecv.at[axis],
                device_id={names[axis]: other}, device_id_type=MESH).start()

    def reduce_lines(axis):
        count, me = parts[axis], pos[axis]
        arrived = gather[axis].at[pl.ds(0, count - 1)]
        pltpu.make_async_copy(arrived, arrived, grecv.at[axis]).wait()
        part = lambda p, q: gather[axis][p, pl.ds(q * pitch + axis * tiles, tiles), :]
        nil = jnp.zeros((tiles, LANES), F32)
        unit = jnp.ones((tiles, LANES), F32)
        mu, rho, tau = [None] * count, [None] * count, [None] * count
        prev = nil
        for p in range(count):
            wf, wt, vf, vt = (part(p, q) for q in range(4))
            kappa = 1.0 / (1.0 - wf * prev)
            mu[p], rho[p] = wt * prev * kappa, wt * kappa
            prev = tau[p] = vt + mu[p] * vf
        nu, omega, sigma = [None] * count, [None] * count, [None] * count
        prev = nil
        for p in reversed(range(count)):
            wf, wt, vf, vt = (part(p, q) for q in range(4))
            kappa = 1.0 / (1.0 - vt * prev)
            nu[p], omega[p] = vf * prev * kappa, vf * kappa
            prev = sigma[p] = wf + nu[p] * wt
        pick = lambda values, at: sum(jnp.where(at == p, v, nil) for p, v in enumerate(values))
        tau_b, sigma_a = pick(tau, me - 1), pick(sigma, me + 1)
        mu_me, nu_me = pick(mu, me), pick(nu, me)
        wf, wt, vf, vt = (part(me, q) for q in range(4))
        det = 1.0 / ((1.0 - tau_b * wf) * (1.0 - sigma_a * vt) - (tau_b * vf) * (sigma_a * wt))
        k11, k12 = (1.0 - sigma_a * vt) * det, tau_b * vf * det
        k21, k22 = sigma_a * wt * det, (1.0 - tau_b * wf) * det
        low, high = [None] * count, [None] * count
        for p in reversed(range(count)):
            onward = -rho[p + 1] * low[p + 1] if p + 1 < count else nil
            low[p] = jnp.where(me - 1 == p, unit, jnp.where(p < me - 1, onward, nil))
        for p in range(count):
            onward = -omega[p - 1] * high[p - 1] if p else nil
            high[p] = jnp.where(me + 1 == p, unit, jnp.where(p > me + 1, onward, nil))
        table = reduced[axis]
        put = lambda index, value: table.__setitem__((pl.ds(index * tiles, tiles), slice(None)), value)
        for p in range(count):
            put(p, k11 * low[p] + k12 * high[p] + jnp.where(me == p, -k11 * tau_b, nil))
            put(count + 1 + p, k21 * low[p] + k22 * high[p] + jnp.where(me == p, -k21 * tau_b, nil))
        put(count, -k12 * sigma_a)
        put(2 * count + 1, -k22 * sigma_a)
        put(2 * count + 2, mu_me)
        put(2 * count + 3, nu_me)

    def publish(axis, stage, c):
        count, table, way = parts[axis], reduced[axis], lax.rem(stage, 2)
        for t in range(tiles):
            head, tail = exch[axis][way, c, pos[axis], t], gt[c, t]
            mu = table[pl.ds((2 * count + 2) * tiles + t, 1), :]
            nu = table[pl.ds((2 * count + 3) * tiles + t, 1), :]
            send[axis][c, 1, t] = tail + mu * head
            send[axis][c, 0, t] = head + nu * tail
        for other in others(axis):
            sel = jnp.where(other > pos[axis], 1, 0)
            pltpu.make_async_remote_copy(
                src_ref=send[axis].at[c, sel], dst_ref=exch[axis].at[way, c, pos[axis]],
                send_sem=send_sem.at[axis, c], recv_sem=recv_sem.at[axis, way, c],
                device_id={names[axis]: other}, device_id_type=MESH).start()

    def neighbours(axis, stage, c):
        count, table, way = parts[axis], reduced[axis], lax.rem(stage, 2)
        arrived = exch[axis].at[way, c, pl.ds(0, count - 1)]
        pltpu.make_async_copy(arrived, arrived, recv_sem.at[axis, way, c]).wait()
        pltpu.make_async_copy(arrived, arrived, send_sem.at[axis, c]).wait()
        for t in range(tiles):
            for side in range(2):
                base = side * (count + 1) * tiles + t
                total = table[pl.ds(base + count * tiles, 1), :] * gt[c, t]
                for p in range(count):
                    total = total + table[pl.ds(base + p * tiles, 1), :] * exch[axis][way, c, p, t]
                ss[side, t] = total

    def turn(src, dst, c, axis, to, stage, correct, dots, step_in=PITCH):
        way = lax.rem(stage, 2)

        def column(f, kt):
            heads = tails = None
            for lt in range(tiles):
                block = src[c, lt, pl.ds(kt * (LANES * step_in) + f, LANES, stride=step_in), :]
                if correct:
                    rows = pl.ds(kt * (LANES * pitch) + (axis * tiles + lt), LANES, stride=pitch)
                    block = (block + w2[rows, :] * ss[0, lt, pl.ds(f, 1), :]
                             + v2[rows, :] * ss[1, lt, pl.ds(f, 1), :])
                if dots is None:
                    block = block * 0.5
                flipped = block.T
                dst[c, kt, pl.ds(lt * LANES * PITCH + f, LANES, stride=PITCH), :] = flipped
                if dots:
                    rows = pl.ds(lt * LANES * pitch + to * tiles + kt, LANES, stride=pitch)
                    fold = lambda v: v.reshape(LANES // SUB, SUB, LANES).sum(axis=0)
                    h, s = fold(flipped * r0[rows, :]), fold(flipped * rn[rows, :])
                    heads = h if heads is None else heads + h
                    tails = s if tails is None else tails + s
            if dots:
                exch[to][way, c, pos[to], kt, pl.ds(f, 1), :] = jnp.sum(heads, axis=0, keepdims=True)
                gt[c, kt, pl.ds(f, 1), :] = jnp.sum(tails, axis=0, keepdims=True)
            return kt

        lax.fori_loop(0, tiles, lambda kt, carry: (lax.fori_loop(0, SUB, column, kt, unroll=True), carry)[1], 0)

    cells = [(c, t) for c in range(chunks) for t in range(tiles)]

    def slab(k):
        return pl.ds(k * PITCH, SUB)

    def solve_block(axis, minus):
        def coef(array, k, t):
            return array[pl.ds(k * pitch + axis * tiles + t, 1), :]

        def forward(k, state):
            ups, downs = list(state[0]), list(state[1])
            r = n - 1 - k
            for s, (c, t) in enumerate(cells):
                ups[s] = rs[c, t, slab(k), :] + coef(ln, k, t) * ups[s]
                hs[c, t, slab(k), :] = ups[s]
                downs[s] = rs[c, t, slab(r), :] + coef(un, r, t) * downs[s]
                hs[c, t, slab(r), :] = downs[s]
            return tuple(ups), tuple(downs)

        init = tuple(blank for _ in cells)
        ups, downs = lax.fori_loop(0, half, forward, (init, init), unroll=unroll)
        lo, hi = half - 1, half

        def place(c, t, k, value):
            qs[c, t, slab(k), :] = value - rs[c, t, slab(k), :] if minus else value

        low_s, high_s = [], []
        for s, (c, t) in enumerate(cells):
            c_lo, a_hi = coef(cn, lo, t), coef(an, hi, t)
            kappa = 1.0 / (1.0 - c_lo * a_hi)
            h_hi = coef(d2, hi, t) * downs[s]
            s_lo = kappa * (coef(m2, lo, t) * ups[s] + c_lo * h_hi)
            low_s.append(s_lo)
            high_s.append(h_hi + a_hi * s_lo)
            place(c, t, lo, low_s[s])
            place(c, t, hi, high_s[s])

        def backward(step, state):
            lows, highs = list(state[0]), list(state[1])
            k, r = half - 1 - step, half + step
            for s, (c, t) in enumerate(cells):
                lows[s] = coef(m2, k, t) * hs[c, t, slab(k), :] + coef(cn, k, t) * lows[s]
                place(c, t, k, lows[s])
                highs[s] = coef(d2, r, t) * hs[c, t, slab(r), :] + coef(an, r, t) * highs[s]
                place(c, t, r, highs[s])
            return tuple(lows), tuple(highs)

        state = lax.fori_loop(1, unroll, backward, (tuple(low_s), tuple(high_s)), unroll=True)
        lax.fori_loop(unroll, half, backward, state, unroll=unroll)

    def each_chunk(body):
        lax.fori_loop(0, chunks, lambda c, carry: (body(c), carry)[1], 0)

    pltpu.make_async_copy(stage_in, stage_in, field_sem).wait()
    each_chunk(lambda c: turn(stage_in, rs, c, X, Y, 0, False, False, SUB))
    me_y = pos[Y]
    for c, t in cells:
        halo_s[0, c, t] = rs[c, t, slab(0), :]
        halo_s[1, c, t] = rs[c, t, slab(n - 1), :]

    def halo(side, other):
        return pltpu.make_async_remote_copy(
            src_ref=halo_s.at[side], dst_ref=halo_r.at[1 - side], send_sem=hsend.at[side], recv_sem=hrecv.at[1 - side],
            device_id={col_name: other}, device_id_type=MESH)

    has_before, has_after = me_y > 0, me_y < parts_y - 1

    @pl.when(has_before)
    def _():
        halo(0, me_y - 1).start()

    @pl.when(has_after)
    def _():
        halo(1, me_y + 1).start()

    def explicit(k, state):
        befores, heres = list(state[0]), list(state[1])
        coef = lambda array, t: array[pl.ds(k * pitch + tiles + t, 1), :]
        for s, (c, t) in enumerate(cells):
            ahead = rs[c, t, slab(k + 1), :]
            qs[c, t, slab(k), :] = (2.0 - coef(pb, t)) * heres[s] - (coef(pa, t) * befores[s] + coef(pc, t) * ahead)
            befores[s], heres[s] = heres[s], ahead
        return tuple(befores), tuple(heres)

    befores, heres = lax.fori_loop(
        0, n - unroll, explicit, (tuple(blank for _ in cells), tuple(rs[c, t, slab(0), :] for c, t in cells)), unroll=unroll)
    befores, heres = lax.fori_loop(n - unroll, n - 1, explicit, (befores, heres), unroll=True)

    @pl.when(has_before)
    def _():
        halo(0, me_y - 1).wait_send()
        halo(1, me_y - 1).wait_recv()

    @pl.when(has_after)
    def _():
        halo(1, me_y + 1).wait_send()
        halo(0, me_y + 1).wait_recv()

    for s, (c, t) in enumerate(cells):
        here = pl.ds((n - 1) * pitch + tiles + t, 1)
        qs[c, t, slab(n - 1), :] = (2.0 - pb[here, :]) * heres[s] - (pa[here, :] * befores[s] + pc[here, :] * halo_r[1, c, t])
        qs[c, t, slab(0), :] = qs[c, t, slab(0), :] - pa[pl.ds(tiles + t, 1), :] * halo_r[0, c, t]

    def start_x(c):
        turn(qs, rs, c, Y, X, 0, False, True)
        publish(X, 0, c)

    reduce_lines(X)
    each_chunk(start_x)
    reduce_lines(Y)
    sent = gc_x.at[pl.ds(0, parts_x - 1)]
    pltpu.make_async_copy(sent, sent, gsend).wait()
    sent = gc_y.at[pl.ds(0, parts_y - 1)]
    pltpu.make_async_copy(sent, sent, gsend).wait()

    def x_half(stage):
        def finish(c):
            neighbours(X, stage, c)
            turn(qs, rs, c, X, Y, stage, True, True)
            publish(Y, stage, c)

        solve_block(X, True)
        each_chunk(finish)

    def step(stage, carry):
        def finish(c):
            neighbours(Y, stage, c)
            turn(qs, rs, c, Y, X, stage + 1, True, True)
            publish(X, stage + 1, c)

        x_half(stage)
        solve_block(Y, True)
        each_chunk(finish)
        return carry

    lax.fori_loop(0, STEPS - 1, step, 0)
    x_half(STEPS - 1)
    solve_block(Y, False)

    def finish(c):
        neighbours(Y, STEPS - 1, c)
        turn(qs, rs, c, Y, X, STEPS, True, None)

        def unload(k, carry):
            for t in range(tiles):
                out[k, pl.ds(pl.multiple_of(c * SUB, SUB), SUB), pl.ds(t * LANES, LANES)] = rs[c, t, slab(k), :]
            return carry

        lax.fori_loop(0, n, unload, 0, unroll=unroll)

    each_chunk(finish)


def solution(mesh):
    parts_x, parts_y = mesh.shape["row"], mesh.shape["col"]
    field_spec = P(("batch", "row"), "col", None)
    coeff_spec = P(("batch", "row"), "col")

    def local_steps(field, *coeffs):
        n, fields = field.shape[0], field.shape[2]
        tiles, chunks = n // LANES, fields // SUB
        packed = pltpu.VMEM((n * 2 * tiles, LANES), F32)
        big = pltpu.VMEM((chunks, tiles, n * PITCH, LANES), F32)
        dma = pltpu.SemaphoreType.DMA
        sends = pltpu.VMEM((chunks, 2, tiles, SUB, LANES), F32)
        line = lambda count: pltpu.VMEM((2, chunks, count, tiles, SUB, LANES), F32)
        table = lambda count: pltpu.VMEM(((2 * count + 4) * tiles, LANES), F32)
        small = pltpu.VMEM((2, chunks, tiles, SUB, LANES), F32)
        message = (8 * tiles, LANES)
        scratch = [
            pltpu.VMEM((6, n, n), F32), pltpu.VMEM((chunks, tiles, n * SUB, LANES), F32), big, big, big, *([packed] * 17),
            pltpu.VMEM(message, F32), pltpu.VMEM((parts_x,) + message, F32), pltpu.VMEM((parts_y,) + message, F32),
            table(parts_x), table(parts_y), sends, sends, line(parts_x), line(parts_y),
            pltpu.VMEM((chunks, tiles, SUB, LANES), F32), pltpu.VMEM((2, tiles, SUB, LANES), F32), small, small,
            dma, dma, dma, dma((2,)), dma((2, chunks)), dma((2, 2, chunks)), dma((2,)), dma((2,)),
        ]
        in_hbm = pl.BlockSpec(memory_space=pltpu.HBM)
        turned = jnp.transpose(field, (0, 2, 1))
        result = pl.pallas_call(
            functools.partial(adi_kernel, (("row", parts_x), ("col", parts_y))),
            out_shape=jax.ShapeDtypeStruct(turned.shape, F32),
            in_specs=[in_hbm] * 7, out_specs=pl.BlockSpec(memory_space=pltpu.VMEM), scratch_shapes=scratch,
            compiler_params=pltpu.CompilerParams(collective_id=0, has_side_effects=True, vmem_limit_bytes=48 * 1024 * 1024),
            name="adi_steps",
        )(turned, *(pltpu.with_memory_space_constraint(array, pltpu.HBM) for array in coeffs))
        return jnp.transpose(result, (0, 2, 1))

    return jax.shard_map(local_steps, mesh=mesh, in_specs=(field_spec,) + (coeff_spec,) * 6, out_specs=field_spec, check_vma=False)
```

```python
import functools

import jax
import jax.numpy as jnp
from jax import lax
from jax.experimental import pallas as pl
from jax.experimental.pallas import tpu as pltpu
from jax.sharding import PartitionSpec as P

STEPS = 3
F32 = jnp.float32
LANES = 128
SUB = 8
PITCH = SUB + 1
MESH = pl.DeviceIdType.MESH
X, Y = 0, 1


def adi_kernel(axes, field, lower_x, diag_x, upper_x, lower_y, diag_y, upper_y, out,
               nat, stage_in, rs, hs, qs, pa, pb, pc, nd, md, ne, me_, ln, cn, un, an, m2, d2, w2, v2, r0, rn,
               gs, gc_x, gc_y, red_x, red_y, sx, sy, ex, ey, raw, gt, ss, part, halo_s, halo_r,
               coef_sem, field_sem, gsend, grecv, send_sem, recv_sem, raw_sem, hsend, hrecv):
    (row_name, parts_x), (col_name, parts_y) = axes
    n = lower_x.shape[0]
    tiles = n // LANES
    chunks = field.shape[1] // SUB
    pitch = 2 * tiles
    half = n // 2
    group = 2
    pos = (lax.axis_index(row_name), lax.axis_index(col_name))
    parts = (parts_x, parts_y)
    names = (row_name, col_name)
    exch = (ex, ey)
    send = (sx, sy)
    gather = (gc_x, gc_y)
    reduced = (red_x, red_y)

    def others(axis):
        count = parts[axis]
        offs = sorted(range(1, count), key=lambda off: -min(off, count - off))
        return [lax.rem(pos[axis] + off, count) for off in offs]

    def field_piece(c, t):
        return pltpu.make_async_copy(field.at[:, pl.ds(c * SUB, SUB), pl.ds(t * LANES, LANES)],
                                     stage_in.at[c, t].reshape(n, SUB, LANES), field_sem.at[c, t])

    for c in range(chunks):
        for t in range(tiles):
            field_piece(c, t).start()
    for slot, ref in enumerate((lower_x, diag_x, upper_x, lower_y, diag_y, upper_y)):
        pltpu.make_async_copy(ref, nat.at[slot], coef_sem).start()

    halo_r[...] = jnp.zeros_like(halo_r)
    barrier = pltpu.get_barrier_semaphore()
    for axis in (X, Y):
        for other in others(axis):
            pl.semaphore_signal(barrier, 1, device_id={names[axis]: other}, device_id_type=MESH)

    blank = jnp.zeros((SUB, LANES), F32)
    every = tuple(range(tiles))
    cells = [(c, t) for c in range(chunks) for t in range(tiles)]

    def slab(k):
        return pl.ds((k + 1) * PITCH, SUB)

    def each_chunk(body):
        lax.fori_loop(0, chunks, lambda c, carry: (body(c), carry)[1], 0)

    def turn(src, dst, c, axis, to, kts, lts, ends, step_in=PITCH, correct=True, explicit=False, scale=None,
             before=False, after=False):
        def column(g, carry):
            fs = [g * group + u for u in range(group)]
            for kt in kts:
                heads, tails = [None] * group, [None] * group
                for lt in lts:
                    if correct:
                        rows = pl.ds(kt * (LANES * pitch) + (axis * tiles + lt), LANES, stride=pitch)
                        near, far = w2[rows, :], v2[rows, :]
                    if explicit:
                        rows = pl.ds(kt * (LANES * pitch) + (axis * tiles + lt), LANES, stride=pitch)
                        own, low, high = 2.0 - pb[rows, :], pa[rows, :], pc[rows, :]
                    if ends:
                        rows = pl.ds(lt * LANES * pitch + to * tiles + kt, LANES, stride=pitch)
                        first_row, last_row = r0[rows, :], rn[rows, :]
                    for u, f in enumerate(fs):
                        origin = kt * LANES * step_in + (step_in if step_in == PITCH else 0) + f
                        block = src[c, lt, pl.ds(origin, LANES, stride=step_in), :]
                        if explicit:
                            block = own * block - (low * src[c, lt, pl.ds(origin - step_in, LANES, stride=step_in), :]
                                                   + high * src[c, lt, pl.ds(origin + step_in, LANES, stride=step_in), :])
                        if correct:
                            block = block + near * ss[0, lt, pl.ds(f, 1), :] + far * ss[1, lt, pl.ds(f, 1), :]
                        if scale is not None:
                            block = block * scale
                        flipped = block.T
                        dst[c, kt, pl.ds((lt * LANES + 1) * PITCH + f, LANES, stride=PITCH), :] = flipped
                        if ends:
                            fold = lambda v: v.reshape(LANES // SUB, SUB, LANES).sum(axis=0)
                            h, s = fold(flipped * first_row), fold(flipped * last_row)
                            heads[u] = h if heads[u] is None else heads[u] + h
                            tails[u] = s if tails[u] is None else tails[u] + s
                if ends:
                    for u, f in enumerate(fs):
                        if before:
                            heads[u], tails[u] = heads[u] + part[0, kt, f], tails[u] + part[1, kt, f]
                        if after:
                            part[0, kt, f], part[1, kt, f] = heads[u], tails[u]
                        else:
                            ends[0][kt, pl.ds(f, 1), :] = jnp.sum(heads[u], axis=0, keepdims=True)
                            ends[1][kt, pl.ds(f, 1), :] = jnp.sum(tails[u], axis=0, keepdims=True)
            return carry

        lax.fori_loop(0, SUB // group, column, 0, unroll=True)

    for c in range(chunks):
        for t in range(tiles):
            field_piece(c, t).wait()
            turn(stage_in, qs, c, X, Y, every, (t,), None, step_in=SUB, correct=False)
    me_y = pos[Y]
    for c, t in cells:
        halo_s[0, c, t] = qs[c, t, slab(0), :]
        halo_s[1, c, t] = qs[c, t, slab(n - 1), :]

    def halo(side, other):
        return pltpu.make_async_remote_copy(
            src_ref=halo_s.at[side], dst_ref=halo_r.at[1 - side], send_sem=hsend.at[side], recv_sem=hrecv.at[1 - side],
            device_id={col_name: other}, device_id_type=MESH)

    has_before, has_after = me_y > 0, me_y < parts_y - 1
    pl.semaphore_wait(barrier, parts_x + parts_y - 2)

    @pl.when(has_before)
    def _():
        halo(0, me_y - 1).start()

    @pl.when(has_after)
    def _():
        halo(1, me_y + 1).start()

    pltpu.make_async_copy(nat, nat, coef_sem).wait()
    for t in range(tiles):
        cols = pl.ds(t * LANES, LANES)
        pa[pl.ds(t, n, stride=pitch), :] = nat[0, :, cols]
        pb[pl.ds(t, n, stride=pitch), :] = nat[1, :, cols] + 1.0
        pc[pl.ds(t, n, stride=pitch), :] = nat[2, :, cols]
        for s in range(tiles):
            rows = pl.ds(s * LANES, LANES)
            dest = pl.ds(t * LANES * pitch + tiles + s, LANES, stride=pitch)
            pa[dest, :] = nat[3, rows, cols].T
            pb[dest, :] = nat[4, rows, cols].T + 1.0
            pc[dest, :] = nat[5, rows, cols].T

    unroll = 8
    zero = jnp.zeros((pitch, LANES), F32)
    one = jnp.ones((pitch, LANES), F32)

    def at_row(k, u):
        return pl.ds(pl.multiple_of(k * (unroll * pitch), unroll * pitch) + u * pitch, pitch)

    def pivots(g, state):
        dp, dq, c_prev, ep, eq, a_next = state
        h = n // unroll - 1 - g
        for u in range(unroll):
            up, down = at_row(g, u), at_row(h, unroll - 1 - u)
            nd[up, :] = dp
            new = pb[up, :] * dp - (pa[up, :] * c_prev) * dq
            md[up, :] = new
            dp, dq, c_prev = new, dp, pc[up, :]
            ne[down, :] = ep
            new = pb[down, :] * ep - (a_next * pc[down, :]) * eq
            me_[down, :] = new
            ep, eq, a_next = new, ep, pa[down, :]
            if u == unroll // 2 - 1:
                scale_d, scale_e = 1.0 / dp, 1.0 / ep
        return dp * scale_d, dq * scale_d, c_prev, ep * scale_e, eq * scale_e, a_next

    lax.fori_loop(0, n // unroll, pivots, (one, zero, zero, one, zero, zero))

    low_half = lax.broadcasted_iota(jnp.int32, (SUB, LANES), 0) < pitch
    blocks = n * pitch // SUB
    step_rows = 4

    def ratios(g, state):
        prev_m, next_d = state
        for u in range(step_rows):
            up = pl.ds(pl.multiple_of(g * (SUB * step_rows), SUB * step_rows) + u * SUB, SUB)
            down = pl.ds(pl.multiple_of((blocks // step_rows - 1 - g) * (SUB * step_rows), SUB * step_rows)
                         + (step_rows - 1 - u) * SUB, SUB)
            minv = nd[up, :] / md[up, :]
            m2[up, :] = minv + minv
            cn[up, :] = -pc[up, :] * minv
            turned = pltpu.roll(minv, pitch, 0)
            ln[up, :] = -pa[up, :] * jnp.where(low_half, prev_m, turned)
            prev_m = turned
            dinv = ne[down, :] / me_[down, :]
            d2[down, :] = dinv + dinv
            an[down, :] = -pa[down, :] * dinv
            turned = pltpu.roll(dinv, pitch, 0)
            un[down, :] = -pc[down, :] * jnp.where(low_half, turned, next_d)
            next_d = turned
        return prev_m, next_d

    lax.fori_loop(0, blocks // step_rows, ratios, (blank, blank))

    first, last = pl.ds(0, pitch), pl.ds((n - 1) * pitch, pitch)

    def products(g, state):
        col0, row0, coln, rown, un_prev, ln_next = state
        h = n // unroll - 1 - g
        for u in range(unroll):
            up, down = at_row(g, u), at_row(h, unroll - 1 - u)
            start = jnp.logical_and(g == 0, u == 0) if u == 0 else None
            f0, f1 = an[up, :], un_prev
            b0, b1 = cn[down, :], ln_next
            if u == 0:
                f0, f1 = jnp.where(start, one, f0), jnp.where(start, one, f1)
                b0, b1 = jnp.where(start, one, b0), jnp.where(start, one, b1)
            col0, row0, coln, rown = col0 * f0, row0 * f1, coln * b0, rown * b1
            w2[up, :], r0[up, :], v2[down, :], rn[down, :] = col0, row0, coln, rown
            un_prev, ln_next = un[up, :], ln[down, :]
        return col0, row0, coln, rown, un_prev, ln_next

    d_first, m_last = 0.5 * d2[first, :], 0.5 * m2[last, :]
    lax.fori_loop(0, n // unroll, products,
                  (-pa[first, :] * d2[first, :], d_first, -pc[last, :] * m2[last, :], m_last, one, one))

    for q, (ref, rows) in enumerate(((w2, first), (w2, last), (v2, first), (v2, last))):
        gs[pl.ds(q * pitch, pitch), :] = -0.5 * ref[rows, :]
    for axis in (X, Y):
        gather[axis][pos[axis]] = gs[...]
        for other in others(axis):
            pltpu.make_async_remote_copy(
                src_ref=gs, dst_ref=gather[axis].at[pos[axis]], send_sem=gsend, recv_sem=grecv.at[axis],
                device_id={names[axis]: other}, device_id_type=MESH).start()

    def reduce_lines(axis):
        count, me = parts[axis], pos[axis]
        arrived = gather[axis].at[pl.ds(0, count - 1)]
        pltpu.make_async_copy(arrived, arrived, grecv.at[axis]).wait()
        part = lambda p, q: gather[axis][p, pl.ds(q * pitch + axis * tiles, tiles), :]
        nil = jnp.zeros((tiles, LANES), F32)
        unit = jnp.ones((tiles, LANES), F32)
        mu, rho, tau = [None] * count, [None] * count, [None] * count
        prev = nil
        for p in range(count):
            wf, wt, vf, vt = (part(p, q) for q in range(4))
            kappa = 1.0 / (1.0 - wf * prev)
            mu[p], rho[p] = wt * prev * kappa, wt * kappa
            prev = tau[p] = vt + mu[p] * vf
        nu, omega, sigma = [None] * count, [None] * count, [None] * count
        prev = nil
        for p in reversed(range(count)):
            wf, wt, vf, vt = (part(p, q) for q in range(4))
            kappa = 1.0 / (1.0 - vt * prev)
            nu[p], omega[p] = vf * prev * kappa, vf * kappa
            prev = sigma[p] = wf + nu[p] * wt
        pick = lambda values, at: sum(jnp.where(at == p, v, nil) for p, v in enumerate(values))
        tau_b, sigma_a = pick(tau, me - 1), pick(sigma, me + 1)
        mu_me, nu_me = pick(mu, me), pick(nu, me)
        wf, wt, vf, vt = (part(me, q) for q in range(4))
        det = 1.0 / ((1.0 - tau_b * wf) * (1.0 - sigma_a * vt) - (tau_b * vf) * (sigma_a * wt))
        k11, k12 = (1.0 - sigma_a * vt) * det, tau_b * vf * det
        k21, k22 = sigma_a * wt * det, (1.0 - tau_b * wf) * det
        low, high = [None] * count, [None] * count
        for p in reversed(range(count)):
            onward = -rho[p + 1] * low[p + 1] if p + 1 < count else nil
            low[p] = jnp.where(me - 1 == p, unit, jnp.where(p < me - 1, onward, nil))
        for p in range(count):
            onward = -omega[p - 1] * high[p - 1] if p else nil
            high[p] = jnp.where(me + 1 == p, unit, jnp.where(p > me + 1, onward, nil))
        table = reduced[axis]
        put = lambda index, value: table.__setitem__((pl.ds(index * tiles, tiles), slice(None)), value)
        for p in range(count):
            put(p, k11 * low[p] + k12 * high[p] + jnp.where(me == p, -k11 * tau_b, nil))
            put(count + 1 + p, k21 * low[p] + k22 * high[p] + jnp.where(me == p, -k21 * tau_b, nil))
        put(count, -k12 * sigma_a)
        put(2 * count + 1, -k22 * sigma_a)
        put(2 * count + 2, mu_me)
        put(2 * count + 3, nu_me)
        if axis == X:
            for p in range(count):
                put(2 * count + 4 + p, jnp.where(p < me, mu[p], unit))
                put(3 * count + 4 + p, jnp.where(p < me, unit, jnp.where(p > me, nu[p], nil)))

    def publish(axis, stage, c, ts):
        count, table, way = parts[axis], reduced[axis], lax.rem(stage, 2)
        for t in ts:
            head, tail = exch[axis][way, c, t, pos[axis]], gt[c, t]
            mu = table[pl.ds((2 * count + 2) * tiles + t, 1), :]
            nu = table[pl.ds((2 * count + 3) * tiles + t, 1), :]
            send[axis][c, 1, t] = tail + mu * head
            send[axis][c, 0, t] = head + nu * tail
        some = pl.ds(ts[0], len(ts))
        for other in others(axis):
            sel = jnp.where(other > pos[axis], 1, 0)
            pltpu.make_async_remote_copy(
                src_ref=send[axis].at[c, sel, some], dst_ref=exch[axis].at[way, c, some, pos[axis]],
                send_sem=send_sem.at[axis, c, ts[0]], recv_sem=recv_sem.at[axis, way, c, ts[0]],
                device_id={names[axis]: other}, device_id_type=MESH).start()

    def combine(axis, stage, c, ts):
        count, table, way = parts[axis], reduced[axis], lax.rem(stage, 2)
        for t in ts:
            for side in range(2):
                base = side * (count + 1) * tiles + t
                total = table[pl.ds(base + count * tiles, 1), :] * gt[c, t]
                for p in range(count):
                    total = total + table[pl.ds(base + p * tiles, 1), :] * exch[axis][way, c, t, p]
                ss[side, t] = total

    def neighbours(axis, stage, c, ts):
        way = lax.rem(stage, 2)
        arrived = exch[axis].at[way, c, pl.ds(ts[0], len(ts)), pl.ds(0, parts[axis] - 1)]
        pltpu.make_async_copy(arrived, arrived, recv_sem.at[axis, way, c, ts[0]]).wait()
        pltpu.make_async_copy(arrived, arrived, send_sem.at[axis, c, ts[0]]).wait()
        combine(axis, stage, c, ts)

    def publish_raw(c):
        for t in range(tiles):
            raw[c, pos[X], 0, t] = exch[X][0, c, t, pos[X]]
            raw[c, pos[X], 1, t] = gt[c, t]
        for other in others(X):
            pltpu.make_async_remote_copy(
                src_ref=raw.at[c, pos[X]], dst_ref=raw.at[c, pos[X]], send_sem=raw_sem.at[0, c], recv_sem=raw_sem.at[1, c],
                device_id={row_name: other}, device_id_type=MESH).start()

    def neighbours_raw(c):
        count = parts_x
        arrived = raw.at[c, pl.ds(0, count - 1)]
        pltpu.make_async_copy(arrived, arrived, raw_sem.at[1, c]).wait()
        pltpu.make_async_copy(arrived, arrived, raw_sem.at[0, c]).wait()
        for t in range(tiles):
            for p in range(count):
                on_head = red_x[pl.ds((2 * count + 4 + p) * tiles + t, 1), :]
                on_tail = red_x[pl.ds((3 * count + 4 + p) * tiles + t, 1), :]
                exch[X][0, c, t, p] = on_head * raw[c, p, 0, t] + on_tail * raw[c, p, 1, t]
        combine(X, 0, c, every)

    def solve_block(axis, minus):
        def coef(array, k, t):
            return array[pl.ds(k * pitch + axis * tiles + t, 1), :]

        def forward(k, state):
            ups, downs = list(state[0]), list(state[1])
            r = n - 1 - k
            for t in range(tiles):
                up, down = coef(ln, k, t), coef(un, r, t)
                for c in range(chunks):
                    s = c * tiles + t
                    ups[s] = rs[c, t, slab(k), :] + up * ups[s]
                    hs[c, t, slab(k), :] = ups[s]
                    downs[s] = rs[c, t, slab(r), :] + down * downs[s]
                    hs[c, t, slab(r), :] = downs[s]
            return tuple(ups), tuple(downs)

        init = tuple(blank for _ in cells)
        ups, downs = lax.fori_loop(0, half, forward, (init, init), unroll=unroll)
        lo, hi = half - 1, half

        def place(c, t, k, value):
            qs[c, t, slab(k), :] = value - rs[c, t, slab(k), :] if minus else value

        low_s, high_s = [], []
        for s, (c, t) in enumerate(cells):
            c_lo, a_hi = coef(cn, lo, t), coef(an, hi, t)
            kappa = 1.0 / (1.0 - c_lo * a_hi)
            h_hi = coef(d2, hi, t) * downs[s]
            s_lo = kappa * (coef(m2, lo, t) * ups[s] + c_lo * h_hi)
            low_s.append(s_lo)
            high_s.append(h_hi + a_hi * s_lo)
            place(c, t, lo, low_s[s])
            place(c, t, hi, high_s[s])

        def backward(step, state):
            lows, highs = list(state[0]), list(state[1])
            k, r = half - 1 - step, half + step
            for t in range(tiles):
                m_low, c_low, m_high, a_high = coef(m2, k, t), coef(cn, k, t), coef(d2, r, t), coef(an, r, t)
                for c in range(chunks):
                    s = c * tiles + t
                    lows[s] = m_low * hs[c, t, slab(k), :] + c_low * lows[s]
                    place(c, t, k, lows[s])
                    highs[s] = m_high * hs[c, t, slab(r), :] + a_high * highs[s]
                    place(c, t, r, highs[s])
            return tuple(lows), tuple(highs)

        state = lax.fori_loop(1, unroll, backward, (tuple(low_s), tuple(high_s)), unroll=True)
        lax.fori_loop(unroll, half, backward, state, unroll=unroll)

    def each_chunk(body):
        lax.fori_loop(0, chunks, lambda c, carry: (body(c), carry)[1], 0)

    @pl.when(has_before)
    def _():
        halo(0, me_y - 1).wait_send()
        halo(1, me_y - 1).wait_recv()

    @pl.when(has_after)
    def _():
        halo(1, me_y + 1).wait_send()
        halo(0, me_y + 1).wait_recv()

    for c, t in cells:
        qs[c, t, slab(-1), :] = halo_r[0, c, t]
        qs[c, t, slab(n), :] = halo_r[1, c, t]

    def ends_of(axis, stage, c):
        at = exch[axis].at[lax.rem(stage, 2), c, :, pos[axis]]
        return at, gt.at[c]

    def start_x(c):
        turn(qs, rs, c, Y, X, every, every, ends_of(X, 0, c), correct=False, explicit=True)
        publish_raw(c)

    def to_y(stage, c):
        for kt in every:
            turn(qs, rs, c, X, Y, (kt,), every, ends_of(Y, stage, c))
            publish(Y, stage, c, (kt,))

    def to_x(stage, c):
        for lt in every:
            neighbours(Y, stage, c, (lt,))
            turn(qs, rs, c, Y, X, every, (lt,), ends_of(X, stage + 1, c), before=lt > 0, after=lt < tiles - 1)
        publish(X, stage + 1, c, every)

    each_chunk(start_x)
    solve_block(X, True)
    reduce_lines(X)
    reduce_lines(Y)
    sent = gc_x.at[pl.ds(0, parts_x - 1)]
    pltpu.make_async_copy(sent, sent, gsend).wait()
    sent = gc_y.at[pl.ds(0, parts_y - 1)]
    pltpu.make_async_copy(sent, sent, gsend).wait()

    def first_to_y(c):
        neighbours_raw(c)
        to_y(0, c)

    each_chunk(first_to_y)

    def step(stage, carry):
        def onward(c):
            neighbours(X, stage, c, every)
            to_y(stage, c)

        solve_block(Y, True)
        each_chunk(lambda c: to_x(stage - 1, c))
        solve_block(X, True)
        each_chunk(onward)
        return carry

    lax.fori_loop(1, STEPS, step, 0)
    solve_block(Y, False)

    def finish(c):
        for lt in every:
            neighbours(Y, STEPS - 1, c, (lt,))
            turn(qs, rs, c, Y, X, every, (lt,), None, scale=0.5)

        def unload(k, carry):
            for t in range(tiles):
                out[k, pl.ds(pl.multiple_of(c * SUB, SUB), SUB), pl.ds(t * LANES, LANES)] = rs[c, t, slab(k), :]
            return carry

        lax.fori_loop(0, n, unload, 0, unroll=unroll)

    each_chunk(finish)


def solution(mesh):
    parts_x, parts_y = mesh.shape["row"], mesh.shape["col"]
    field_spec = P(("batch", "row"), "col", None)
    coeff_spec = P(("batch", "row"), "col")

    def local_steps(field, *coeffs):
        n, fields = field.shape[0], field.shape[2]
        tiles, chunks = n // LANES, fields // SUB
        packed = pltpu.VMEM((n * 2 * tiles, LANES), F32)
        plane = -(-((n + 2) * PITCH - SUB) // (4 * SUB)) * 4 * SUB + SUB
        big = pltpu.VMEM((chunks, tiles, plane, LANES), F32)
        dma = pltpu.SemaphoreType.DMA
        sends = pltpu.VMEM((chunks, 2, tiles, SUB, LANES), F32)
        line = lambda count: pltpu.VMEM((2, chunks, tiles, count, SUB, LANES), F32)
        table = lambda count: pltpu.VMEM(((4 * count + 4) * tiles, LANES), F32)
        small = pltpu.VMEM((2, chunks, tiles, SUB, LANES), F32)
        message = (8 * tiles, LANES)
        scratch = [
            pltpu.VMEM((6, n, n), F32), pltpu.VMEM((chunks, tiles, n * SUB, LANES), F32), big, big, big, *([packed] * 17),
            pltpu.VMEM(message, F32), pltpu.VMEM((parts_x,) + message, F32), pltpu.VMEM((parts_y,) + message, F32),
            table(parts_x), table(parts_y), sends, sends, line(parts_x), line(parts_y),
            pltpu.VMEM((chunks, parts_x, 2, tiles, SUB, LANES), F32),
            pltpu.VMEM((chunks, tiles, SUB, LANES), F32), pltpu.VMEM((2, tiles, SUB, LANES), F32),
            pltpu.VMEM((2, tiles, SUB, SUB, LANES), F32), small, small,
            dma, dma((chunks, tiles)), dma, dma((2,)), dma((2, chunks, tiles)), dma((2, 2, chunks, tiles)), dma((2, chunks)), dma((2,)), dma((2,)),
        ]
        in_hbm = pl.BlockSpec(memory_space=pltpu.HBM)
        turned = jnp.transpose(field, (0, 2, 1))
        result = pl.pallas_call(
            functools.partial(adi_kernel, (("row", parts_x), ("col", parts_y))),
            out_shape=jax.ShapeDtypeStruct(turned.shape, F32),
            in_specs=[in_hbm] * 7, out_specs=pl.BlockSpec(memory_space=pltpu.VMEM), scratch_shapes=scratch,
            compiler_params=pltpu.CompilerParams(collective_id=0, has_side_effects=True, vmem_limit_bytes=48 * 1024 * 1024),
            name="adi_steps",
        )(turned, *(pltpu.with_memory_space_constraint(array, pltpu.HBM) for array in coeffs))
        return jnp.transpose(result, (0, 2, 1))

    return jax.shard_map(local_steps, mesh=mesh, in_specs=(field_spec,) + (coeff_spec,) * 6, out_specs=field_spec, check_vma=False)
```

```python
import functools

import jax
import jax.numpy as jnp
from jax import lax
from jax.experimental import pallas as pl
from jax.experimental.pallas import tpu as pltpu
from jax.sharding import PartitionSpec as P

STEPS = 3
F32 = jnp.float32
LANES = 128
SUB = 8
PITCH = SUB + 1
LOGICAL = pl.DeviceIdType.LOGICAL
X, Y = 0, 1


def adi_kernel(axes, strides, field, lower_x, diag_x, upper_x, lower_y, diag_y, upper_y, out,
               nat, rs, hs, qs, pa, pb, pc, nd, md, ne, me_, ln, cn, un, an, m2, d2, w2, v2, r0, rn,
               gs, gc_x, gc_y, red_x, red_y, sx, sy, ex, ey, raw, gt, ss, part, halo_s, halo_r,
               coef_sem, field_sem, gsend, grecv, send_sem, recv_sem, raw_sem, hsend, hrecv):
    (row_name, parts_x), (col_name, parts_y) = axes
    n = lower_x.shape[0]
    tiles = n // LANES
    chunks = field.shape[1] // SUB
    pitch = 2 * tiles
    half = n // 2
    group = 2
    pos = (lax.axis_index(row_name), lax.axis_index(col_name))
    parts = (parts_x, parts_y)
    home = sum(lax.axis_index(name) * stride for name, stride in strides.items())
    exch = (ex, ey)
    send = (sx, sy)
    gather = (gc_x, gc_y)
    reduced = (red_x, red_y)

    def device(axis, other):
        return home + (other - pos[axis]) * strides[(row_name, col_name)[axis]]

    def others(axis):
        count = parts[axis]
        offs = sorted(range(1, count), key=lambda off: -min(off, count - off))
        return [lax.rem(pos[axis] + off, count) for off in offs]

    def field_piece(c, t):
        return pltpu.make_async_copy(field.at[:, pl.ds(c * SUB, SUB), pl.ds(t * LANES, LANES)],
                                     out.at[c, t].reshape(n, SUB, LANES), field_sem.at[c, t])

    for c in range(chunks):
        for t in range(tiles):
            field_piece(c, t).start()
    for slot, ref in enumerate((lower_x, diag_x, upper_x, lower_y, diag_y, upper_y)):
        pltpu.make_async_copy(ref, nat.at[slot], coef_sem).start()

    halo_r[...] = jnp.zeros_like(halo_r)
    barrier = pltpu.get_barrier_semaphore()
    for axis in (X, Y):
        for other in others(axis):
            pl.semaphore_signal(barrier, 1, device_id=device(axis, other), device_id_type=LOGICAL)

    blank = jnp.zeros((SUB, LANES), F32)
    every = tuple(range(tiles))
    cells = [(c, t) for c in range(chunks) for t in range(tiles)]

    def slab(k):
        return pl.ds((k + 1) * PITCH, SUB)

    def each_chunk(body):
        lax.fori_loop(0, chunks, lambda c, carry: (body(c), carry)[1], 0)

    def turn(src, dst, c, axis, to, kts, lts, ends, step_in=PITCH, correct=True, explicit=False, scale=None,
             before=False, after=False, step_out=PITCH):
        def column(g, carry):
            fs = [g * group + u for u in range(group)]
            for kt in kts:
                heads, tails = [None] * group, [None] * group
                for lt in lts:
                    if correct:
                        rows = pl.ds(kt * (LANES * pitch) + (axis * tiles + lt), LANES, stride=pitch)
                        near, far = w2[rows, :], v2[rows, :]
                    if explicit:
                        rows = pl.ds(kt * (LANES * pitch) + (axis * tiles + lt), LANES, stride=pitch)
                        own, low, high = 2.0 - pb[rows, :], pa[rows, :], pc[rows, :]
                    if ends:
                        rows = pl.ds(lt * LANES * pitch + to * tiles + kt, LANES, stride=pitch)
                        first_row, last_row = r0[rows, :], rn[rows, :]
                    for u, f in enumerate(fs):
                        origin = kt * LANES * step_in + (step_in if step_in == PITCH else 0) + f
                        target = lt * LANES * step_out + (step_out if step_out == PITCH else 0) + f
                        block = src[c, lt, pl.ds(origin, LANES, stride=step_in), :]
                        if explicit:
                            block = own * block - (low * src[c, lt, pl.ds(origin - step_in, LANES, stride=step_in), :]
                                                   + high * src[c, lt, pl.ds(origin + step_in, LANES, stride=step_in), :])
                        if correct:
                            block = block + near * ss[0, lt, pl.ds(f, 1), :] + far * ss[1, lt, pl.ds(f, 1), :]
                        if scale is not None:
                            block = block * scale
                        flipped = block.T
                        dst[c, kt, pl.ds(target, LANES, stride=step_out), :] = flipped
                        if ends:
                            fold = lambda v: v.reshape(LANES // SUB, SUB, LANES).sum(axis=0)
                            h, s = fold(flipped * first_row), fold(flipped * last_row)
                            heads[u] = h if heads[u] is None else heads[u] + h
                            tails[u] = s if tails[u] is None else tails[u] + s
                if ends:
                    for u, f in enumerate(fs):
                        if before:
                            heads[u], tails[u] = heads[u] + part[0, kt, f], tails[u] + part[1, kt, f]
                        if after:
                            part[0, kt, f], part[1, kt, f] = heads[u], tails[u]
                        else:
                            ends[0][kt, pl.ds(f, 1), :] = jnp.sum(heads[u], axis=0, keepdims=True)
                            ends[1][kt, pl.ds(f, 1), :] = jnp.sum(tails[u], axis=0, keepdims=True)
            return carry

        lax.fori_loop(0, SUB // group, column, 0, unroll=True)

    for c in range(chunks):
        for t in range(tiles):
            field_piece(c, t).wait()
            turn(out, qs, c, X, Y, every, (t,), None, step_in=SUB, correct=False)
    me_y = pos[Y]
    for c, t in cells:
        halo_s[0, c, t] = qs[c, t, slab(0), :]
        halo_s[1, c, t] = qs[c, t, slab(n - 1), :]

    def halo(side, other):
        return pltpu.make_async_remote_copy(
            src_ref=halo_s.at[side], dst_ref=halo_r.at[1 - side], send_sem=hsend.at[side], recv_sem=hrecv.at[1 - side],
            device_id=device(Y, other), device_id_type=LOGICAL)

    has_before, has_after = me_y > 0, me_y < parts_y - 1
    pl.semaphore_wait(barrier, parts_x + parts_y - 2)

    @pl.when(has_before)
    def _():
        halo(0, me_y - 1).start()

    @pl.when(has_after)
    def _():
        halo(1, me_y + 1).start()

    pltpu.make_async_copy(nat, nat, coef_sem).wait()
    for t in range(tiles):
        cols = pl.ds(t * LANES, LANES)
        pa[pl.ds(t, n, stride=pitch), :] = nat[0, :, cols]
        pb[pl.ds(t, n, stride=pitch), :] = nat[1, :, cols] + 1.0
        pc[pl.ds(t, n, stride=pitch), :] = nat[2, :, cols]
        for s in range(tiles):
            rows = pl.ds(s * LANES, LANES)
            dest = pl.ds(t * LANES * pitch + tiles + s, LANES, stride=pitch)
            pa[dest, :] = nat[3, rows, cols].T
            pb[dest, :] = nat[4, rows, cols].T + 1.0
            pc[dest, :] = nat[5, rows, cols].T

    unroll = 8
    zero = jnp.zeros((pitch, LANES), F32)
    one = jnp.ones((pitch, LANES), F32)

    def at_row(k, u):
        return pl.ds(pl.multiple_of(k * (unroll * pitch), unroll * pitch) + u * pitch, pitch)

    def pivots(g, state):
        dp, dq, c_prev, ep, eq, a_next = state
        h = n // unroll - 1 - g
        for u in range(unroll):
            up, down = at_row(g, u), at_row(h, unroll - 1 - u)
            nd[up, :] = dp
            new = pb[up, :] * dp - (pa[up, :] * c_prev) * dq
            md[up, :] = new
            dp, dq, c_prev = new, dp, pc[up, :]
            ne[down, :] = ep
            new = pb[down, :] * ep - (a_next * pc[down, :]) * eq
            me_[down, :] = new
            ep, eq, a_next = new, ep, pa[down, :]
            if u == unroll // 2 - 1:
                scale_d, scale_e = 1.0 / dp, 1.0 / ep
        return dp * scale_d, dq * scale_d, c_prev, ep * scale_e, eq * scale_e, a_next

    lax.fori_loop(0, n // unroll, pivots, (one, zero, zero, one, zero, zero))

    low_half = lax.broadcasted_iota(jnp.int32, (SUB, LANES), 0) < pitch
    blocks = n * pitch // SUB
    step_rows = 4

    def ratios(g, state):
        prev_m, next_d = state
        for u in range(step_rows):
            up = pl.ds(pl.multiple_of(g * (SUB * step_rows), SUB * step_rows) + u * SUB, SUB)
            down = pl.ds(pl.multiple_of((blocks // step_rows - 1 - g) * (SUB * step_rows), SUB * step_rows)
                         + (step_rows - 1 - u) * SUB, SUB)
            minv = nd[up, :] / md[up, :]
            m2[up, :] = minv + minv
            cn[up, :] = -pc[up, :] * minv
            turned = pltpu.roll(minv, pitch, 0)
            ln[up, :] = -pa[up, :] * jnp.where(low_half, prev_m, turned)
            prev_m = turned
            dinv = ne[down, :] / me_[down, :]
            d2[down, :] = dinv + dinv
            an[down, :] = -pa[down, :] * dinv
            turned = pltpu.roll(dinv, pitch, 0)
            un[down, :] = -pc[down, :] * jnp.where(low_half, turned, next_d)
            next_d = turned
        return prev_m, next_d

    lax.fori_loop(0, blocks // step_rows, ratios, (blank, blank))

    first, last = pl.ds(0, pitch), pl.ds((n - 1) * pitch, pitch)

    def products(g, state):
        col0, row0, coln, rown, un_prev, ln_next = state
        h = n // unroll - 1 - g
        for u in range(unroll):
            up, down = at_row(g, u), at_row(h, unroll - 1 - u)
            start = jnp.logical_and(g == 0, u == 0) if u == 0 else None
            f0, f1 = an[up, :], un_prev
            b0, b1 = cn[down, :], ln_next
            if u == 0:
                f0, f1 = jnp.where(start, one, f0), jnp.where(start, one, f1)
                b0, b1 = jnp.where(start, one, b0), jnp.where(start, one, b1)
            col0, row0, coln, rown = col0 * f0, row0 * f1, coln * b0, rown * b1
            w2[up, :], r0[up, :], v2[down, :], rn[down, :] = col0, row0, coln, rown
            un_prev, ln_next = un[up, :], ln[down, :]
        return col0, row0, coln, rown, un_prev, ln_next

    d_first, m_last = 0.5 * d2[first, :], 0.5 * m2[last, :]
    lax.fori_loop(0, n // unroll, products,
                  (-pa[first, :] * d2[first, :], d_first, -pc[last, :] * m2[last, :], m_last, one, one))

    for q, (ref, rows) in enumerate(((w2, first), (w2, last), (v2, first), (v2, last))):
        gs[pl.ds(q * pitch, pitch), :] = -0.5 * ref[rows, :]
    for axis in (X, Y):
        gather[axis][pos[axis]] = gs[...]
        for other in others(axis):
            pltpu.make_async_remote_copy(
                src_ref=gs, dst_ref=gather[axis].at[pos[axis]], send_sem=gsend, recv_sem=grecv.at[axis],
                device_id=device(axis, other), device_id_type=LOGICAL).start()

    def reduce_lines(axis):
        count, me = parts[axis], pos[axis]
        arrived = gather[axis].at[pl.ds(0, count - 1)]
        pltpu.make_async_copy(arrived, arrived, grecv.at[axis]).wait()
        part = lambda p, q: gather[axis][p, pl.ds(q * pitch + axis * tiles, tiles), :]
        nil = jnp.zeros((tiles, LANES), F32)
        unit = jnp.ones((tiles, LANES), F32)
        mu, rho, tau = [None] * count, [None] * count, [None] * count
        prev = nil
        for p in range(count):
            wf, wt, vf, vt = (part(p, q) for q in range(4))
            kappa = 1.0 / (1.0 - wf * prev)
            mu[p], rho[p] = wt * prev * kappa, wt * kappa
            prev = tau[p] = vt + mu[p] * vf
        nu, omega, sigma = [None] * count, [None] * count, [None] * count
        prev = nil
        for p in reversed(range(count)):
            wf, wt, vf, vt = (part(p, q) for q in range(4))
            kappa = 1.0 / (1.0 - vt * prev)
            nu[p], omega[p] = vf * prev * kappa, vf * kappa
            prev = sigma[p] = wf + nu[p] * wt
        pick = lambda values, at: sum(jnp.where(at == p, v, nil) for p, v in enumerate(values))
        tau_b, sigma_a = pick(tau, me - 1), pick(sigma, me + 1)
        mu_me, nu_me = pick(mu, me), pick(nu, me)
        wf, wt, vf, vt = (part(me, q) for q in range(4))
        det = 1.0 / ((1.0 - tau_b * wf) * (1.0 - sigma_a * vt) - (tau_b * vf) * (sigma_a * wt))
        k11, k12 = (1.0 - sigma_a * vt) * det, tau_b * vf * det
        k21, k22 = sigma_a * wt * det, (1.0 - tau_b * wf) * det
        low, high = [None] * count, [None] * count
        for p in reversed(range(count)):
            onward = -rho[p + 1] * low[p + 1] if p + 1 < count else nil
            low[p] = jnp.where(me - 1 == p, unit, jnp.where(p < me - 1, onward, nil))
        for p in range(count):
            onward = -omega[p - 1] * high[p - 1] if p else nil
            high[p] = jnp.where(me + 1 == p, unit, jnp.where(p > me + 1, onward, nil))
        table = reduced[axis]
        put = lambda index, value: table.__setitem__((pl.ds(index * tiles, tiles), slice(None)), value)
        for p in range(count):
            put(p, k11 * low[p] + k12 * high[p] + jnp.where(me == p, -k11 * tau_b, nil))
            put(count + 1 + p, k21 * low[p] + k22 * high[p] + jnp.where(me == p, -k21 * tau_b, nil))
        put(count, -k12 * sigma_a)
        put(2 * count + 1, -k22 * sigma_a)
        put(2 * count + 2, mu_me)
        put(2 * count + 3, nu_me)
        if axis == X:
            for p in range(count):
                put(2 * count + 4 + p, jnp.where(p < me, mu[p], unit))
                put(3 * count + 4 + p, jnp.where(p < me, unit, jnp.where(p > me, nu[p], nil)))

    def slot(axis, way, c, t, p):
        return (way, c, p, t) if axis == X else (way, c, t, p)

    def publish(axis, stage, c, ts):
        count, table, way = parts[axis], reduced[axis], lax.rem(stage, 2)
        for t in ts:
            head, tail = exch[axis][slot(axis, way, c, t, pos[axis])], gt[c, t]
            mu = table[pl.ds((2 * count + 2) * tiles + t, 1), :]
            nu = table[pl.ds((2 * count + 3) * tiles + t, 1), :]
            send[axis][c, 1, t] = tail + mu * head
            send[axis][c, 0, t] = head + nu * tail
        some = pl.ds(ts[0], len(ts))
        there = exch[X].at[way, c, pos[X]] if axis == X else exch[Y].at[way, c, some, pos[Y]]
        for other in others(axis):
            sel = jnp.where(other > pos[axis], 1, 0)
            pltpu.make_async_remote_copy(
                src_ref=send[axis].at[c, sel, some], dst_ref=there,
                send_sem=send_sem.at[axis, c, ts[0]], recv_sem=recv_sem.at[axis, way, c, ts[0]],
                device_id=device(axis, other), device_id_type=LOGICAL).start()

    def combine(axis, stage, c, ts):
        count, table, way = parts[axis], reduced[axis], lax.rem(stage, 2)
        for t in ts:
            for side in range(2):
                base = side * (count + 1) * tiles + t
                total = table[pl.ds(base + count * tiles, 1), :] * gt[c, t]
                for p in range(count):
                    total = total + table[pl.ds(base + p * tiles, 1), :] * exch[axis][slot(axis, way, c, t, p)]
                ss[side, t] = total

    def neighbours(axis, stage, c, ts):
        way = lax.rem(stage, 2)
        some = pl.ds(0, parts[axis] - 1)
        arrived = exch[X].at[way, c, some] if axis == X else exch[Y].at[way, c, pl.ds(ts[0], len(ts)), some]
        pltpu.make_async_copy(arrived, arrived, recv_sem.at[axis, way, c, ts[0]]).wait()
        pltpu.make_async_copy(arrived, arrived, send_sem.at[axis, c, ts[0]]).wait()
        combine(axis, stage, c, ts)

    def publish_raw(c):
        for t in range(tiles):
            raw[c, pos[X], 0, t] = exch[X][slot(X, 0, c, t, pos[X])]
            raw[c, pos[X], 1, t] = gt[c, t]
        for other in others(X):
            pltpu.make_async_remote_copy(
                src_ref=raw.at[c, pos[X]], dst_ref=raw.at[c, pos[X]], send_sem=raw_sem.at[0, c], recv_sem=raw_sem.at[1, c],
                device_id=device(X, other), device_id_type=LOGICAL).start()

    def neighbours_raw(c):
        count = parts_x
        arrived = raw.at[c, pl.ds(0, count - 1)]
        pltpu.make_async_copy(arrived, arrived, raw_sem.at[1, c]).wait()
        pltpu.make_async_copy(arrived, arrived, raw_sem.at[0, c]).wait()
        for t in range(tiles):
            for p in range(count):
                on_head = red_x[pl.ds((2 * count + 4 + p) * tiles + t, 1), :]
                on_tail = red_x[pl.ds((3 * count + 4 + p) * tiles + t, 1), :]
                exch[X][slot(X, 0, c, t, p)] = on_head * raw[c, p, 0, t] + on_tail * raw[c, p, 1, t]
        combine(X, 0, c, every)

    def solve_block(axis, minus):
        def coef(array, k, t):
            return array[pl.ds(k * pitch + axis * tiles + t, 1), :]

        def forward(k, state):
            ups, downs = list(state[0]), list(state[1])
            r = n - 1 - k
            for t in range(tiles):
                up, down = coef(ln, k, t), coef(un, r, t)
                for c in range(chunks):
                    s = c * tiles + t
                    ups[s] = rs[c, t, slab(k), :] + up * ups[s]
                    hs[c, t, slab(k), :] = ups[s]
                    downs[s] = rs[c, t, slab(r), :] + down * downs[s]
                    hs[c, t, slab(r), :] = downs[s]
            return tuple(ups), tuple(downs)

        init = tuple(blank for _ in cells)
        ups, downs = lax.fori_loop(0, half, forward, (init, init), unroll=unroll)
        lo, hi = half - 1, half

        def place(c, t, k, value):
            qs[c, t, slab(k), :] = value - rs[c, t, slab(k), :] if minus else value

        low_s, high_s = [], []
        for s, (c, t) in enumerate(cells):
            c_lo, a_hi = coef(cn, lo, t), coef(an, hi, t)
            kappa = 1.0 / (1.0 - c_lo * a_hi)
            h_hi = coef(d2, hi, t) * downs[s]
            s_lo = kappa * (coef(m2, lo, t) * ups[s] + c_lo * h_hi)
            low_s.append(s_lo)
            high_s.append(h_hi + a_hi * s_lo)
            place(c, t, lo, low_s[s])
            place(c, t, hi, high_s[s])

        def backward(step, state):
            lows, highs = list(state[0]), list(state[1])
            k, r = half - 1 - step, half + step
            for t in range(tiles):
                m_low, c_low, m_high, a_high = coef(m2, k, t), coef(cn, k, t), coef(d2, r, t), coef(an, r, t)
                for c in range(chunks):
                    s = c * tiles + t
                    lows[s] = m_low * hs[c, t, slab(k), :] + c_low * lows[s]
                    place(c, t, k, lows[s])
                    highs[s] = m_high * hs[c, t, slab(r), :] + a_high * highs[s]
                    place(c, t, r, highs[s])
            return tuple(lows), tuple(highs)

        state = lax.fori_loop(1, unroll, backward, (tuple(low_s), tuple(high_s)), unroll=True)
        lax.fori_loop(unroll, half, backward, state, unroll=unroll)

    def each_chunk(body):
        lax.fori_loop(0, chunks, lambda c, carry: (body(c), carry)[1], 0)

    @pl.when(has_before)
    def _():
        halo(0, me_y - 1).wait_send()
        halo(1, me_y - 1).wait_recv()

    @pl.when(has_after)
    def _():
        halo(1, me_y + 1).wait_send()
        halo(0, me_y + 1).wait_recv()

    for c, t in cells:
        qs[c, t, slab(-1), :] = halo_r[0, c, t]
        qs[c, t, slab(n), :] = halo_r[1, c, t]

    def ends_of(axis, stage, c):
        way = lax.rem(stage, 2)
        return exch[X].at[way, c, pos[X]] if axis == X else exch[Y].at[way, c, :, pos[Y]], gt.at[c]

    def start_x(c):
        turn(qs, rs, c, Y, X, every, every, ends_of(X, 0, c), correct=False, explicit=True)
        publish_raw(c)

    def to_y(stage, c):
        for kt in every:
            turn(qs, rs, c, X, Y, (kt,), every, ends_of(Y, stage, c))
            publish(Y, stage, c, (kt,))

    def to_x(stage, c):
        for lt in every:
            neighbours(Y, stage, c, (lt,))
            turn(qs, rs, c, Y, X, every, (lt,), ends_of(X, stage + 1, c), before=lt > 0, after=lt < tiles - 1)
        publish(X, stage + 1, c, every)

    each_chunk(start_x)
    solve_block(X, True)
    reduce_lines(X)
    reduce_lines(Y)
    sent = gc_x.at[pl.ds(0, parts_x - 1)]
    pltpu.make_async_copy(sent, sent, gsend).wait()
    sent = gc_y.at[pl.ds(0, parts_y - 1)]
    pltpu.make_async_copy(sent, sent, gsend).wait()

    def first_to_y(c):
        neighbours_raw(c)
        to_y(0, c)

    each_chunk(first_to_y)

    def step(stage, carry):
        def onward(c):
            neighbours(X, stage, c, every)
            to_y(stage, c)

        solve_block(Y, True)
        each_chunk(lambda c: to_x(stage - 1, c))
        solve_block(X, True)
        each_chunk(onward)
        return carry

    lax.fori_loop(1, STEPS, step, 0)
    solve_block(Y, False)

    def finish(c):
        for lt in every:
            neighbours(Y, STEPS - 1, c, (lt,))
            turn(qs, out, c, Y, X, every, (lt,), None, scale=0.5, step_out=SUB)

    each_chunk(finish)


def unload_kernel(tiles_ref, out, sem):
    chunks, tiles, rows, lanes = tiles_ref.shape
    copies = [pltpu.make_async_copy(tiles_ref.at[c, t].reshape(rows // SUB, SUB, lanes),
                                    out.at[:, pl.ds(c * SUB, SUB), pl.ds(t * lanes, lanes)], sem.at[c * tiles + t])
              for c in range(chunks) for t in range(tiles)]
    for copy in copies:
        copy.start()
    for copy in copies:
        copy.wait()


def solution(mesh):
    parts_x, parts_y = mesh.shape["row"], mesh.shape["col"]
    strides, stride = {}, 1
    for name in reversed(mesh.axis_names):
        strides[name], stride = stride, stride * mesh.shape[name]
    field_spec = P(("batch", "row"), "col", None)
    coeff_spec = P(("batch", "row"), "col")

    def local_steps(field, *coeffs):
        n, fields = field.shape[0], field.shape[2]
        tiles, chunks = n // LANES, fields // SUB
        packed = pltpu.VMEM((n * 2 * tiles, LANES), F32)
        plane = -(-((n + 2) * PITCH - SUB) // (4 * SUB)) * 4 * SUB + SUB
        big = pltpu.VMEM((chunks, tiles, plane, LANES), F32)
        dma = pltpu.SemaphoreType.DMA
        sends = pltpu.VMEM((chunks, 2, tiles, SUB, LANES), F32)
        table = lambda count: pltpu.VMEM(((4 * count + 4) * tiles, LANES), F32)
        small = pltpu.VMEM((2, chunks, tiles, SUB, LANES), F32)
        message = (8 * tiles, LANES)
        scratch = [
            pltpu.VMEM((6, n, n), F32), big, big, big, *([packed] * 17),
            pltpu.VMEM(message, F32), pltpu.VMEM((parts_x,) + message, F32), pltpu.VMEM((parts_y,) + message, F32),
            table(parts_x), table(parts_y), sends, sends, pltpu.VMEM((2, chunks, parts_x, tiles, SUB, LANES), F32), pltpu.VMEM((2, chunks, tiles, parts_y, SUB, LANES), F32),
            pltpu.VMEM((chunks, parts_x, 2, tiles, SUB, LANES), F32),
            pltpu.VMEM((chunks, tiles, SUB, LANES), F32), pltpu.VMEM((2, tiles, SUB, LANES), F32),
            pltpu.VMEM((2, tiles, SUB, SUB, LANES), F32), small, small,
            dma, dma((chunks, tiles)), dma, dma((2,)), dma((2, chunks, tiles)), dma((2, 2, chunks, tiles)), dma((2, chunks)), dma((2,)), dma((2,)),
        ]
        in_hbm = pl.BlockSpec(memory_space=pltpu.HBM)
        turned = jnp.transpose(field, (0, 2, 1))
        in_vmem = pl.BlockSpec(memory_space=pltpu.VMEM)
        tiled = pl.pallas_call(
            functools.partial(adi_kernel, (("row", parts_x), ("col", parts_y)), strides),
            out_shape=jax.ShapeDtypeStruct((chunks, tiles, n * SUB, LANES), F32),
            in_specs=[in_hbm] * 7, out_specs=in_vmem, scratch_shapes=scratch,
            compiler_params=pltpu.CompilerParams(collective_id=0, has_side_effects=True, vmem_limit_bytes=40 * 1024 * 1024),
            name="adi_steps",
        )(*(pltpu.with_memory_space_constraint(array, pltpu.HBM) for array in (turned,) + coeffs))
        result = pl.pallas_call(
            unload_kernel, out_shape=jax.ShapeDtypeStruct(turned.shape, F32), in_specs=[in_vmem], out_specs=in_hbm,
            scratch_shapes=[dma((chunks * tiles,))], compiler_params=pltpu.CompilerParams(vmem_limit_bytes=1024 * 1024),
            name="unload",
        )(tiled)
        return jnp.transpose(result, (0, 2, 1))

    return jax.shard_map(local_steps, mesh=mesh, in_specs=(field_spec,) + (coeff_spec,) * 6, out_specs=field_spec, check_vma=False)
```

```python
import functools

import jax
import jax.numpy as jnp
from jax import lax
from jax.experimental import pallas as pl
from jax.experimental.pallas import tpu as pltpu
from jax.sharding import PartitionSpec as P

STEPS = 3
F32 = jnp.float32
LANES = 128
SUB = 8
PITCH = SUB + 1
LOGICAL = pl.DeviceIdType.LOGICAL
X, Y = 0, 1


def adi_kernel(axes, strides, field, lower_x, diag_x, upper_x, lower_y, diag_y, upper_y, out, qs, w2, v2, ss,
               nat, rs, hs, pa, pb, pc, nd, md, ne, me_, ln, cn, un, an, m2, d2, r0, rn,
               gs, gc_x, gc_y, red_x, red_y, sx, sy, ex, ey, raw, gt, part, halo_s, halo_r,
               load_sem, send_sem, recv_x, recv_y, grecv):
    (row_name, parts_x), (col_name, parts_y) = axes
    n = lower_x.shape[0]
    tiles = n // LANES
    chunks = field.shape[1] // SUB
    pitch = 2 * tiles
    half = n // 2
    group = 2
    pos = (lax.axis_index(row_name), lax.axis_index(col_name))
    parts = (parts_x, parts_y)
    home = sum(lax.axis_index(name) * stride for name, stride in strides.items())
    exch = (ex, ey)
    send = (sx, sy)
    gather = (gc_x, gc_y)
    reduced = (red_x, red_y)

    def device(axis, other):
        return home + (other - pos[axis]) * strides[(row_name, col_name)[axis]]

    def others(axis):
        count = parts[axis]
        offs = sorted(range(1, count), key=lambda off: -min(off, count - off))
        return [lax.rem(pos[axis] + off, count) for off in offs]

    def field_piece(c, t):
        return pltpu.make_async_copy(field.at[:, pl.ds(c * SUB, SUB), pl.ds(t * LANES, LANES)],
                                     out.at[c, t].reshape(n, SUB, LANES), send_sem.at[t, c])

    for c in range(chunks):
        for t in range(tiles):
            field_piece(c, t).start()
    for slot, ref in enumerate((lower_x, diag_x, upper_x, lower_y, diag_y, upper_y)):
        pltpu.make_async_copy(ref, nat.at[slot], load_sem).start()

    halo_r[...] = jnp.zeros_like(halo_r)
    barrier = pltpu.get_barrier_semaphore()
    for axis in (X, Y):
        for other in others(axis):
            pl.semaphore_signal(barrier, 1, device_id=device(axis, other), device_id_type=LOGICAL)

    blank = jnp.zeros((SUB, LANES), F32)
    every = tuple(range(tiles))
    cells = [(c, t) for c in range(chunks) for t in range(tiles)]

    def slab(k):
        return pl.ds((k + 1) * PITCH, SUB)

    def each_chunk(body):
        lax.fori_loop(0, chunks, lambda c, carry: (body(c), carry)[1], 0)

    def turn(src, dst, c, axis, to, kts, lts, ends, step_in=PITCH, correct=True, explicit=False, scale=None,
             before=False, after=False, step_out=PITCH):
        def column(g, carry):
            fs = [g * group + u for u in range(group)]
            for kt in kts:
                heads, tails = [None] * group, [None] * group
                for lt in lts:
                    if correct:
                        rows = pl.ds(kt * (LANES * pitch) + (axis * tiles + lt), LANES, stride=pitch)
                        near, far = w2[rows, :], v2[rows, :]
                    if explicit:
                        rows = pl.ds(kt * (LANES * pitch) + (axis * tiles + lt), LANES, stride=pitch)
                        own, low, high = 2.0 - pb[rows, :], pa[rows, :], pc[rows, :]
                    if ends:
                        rows = pl.ds(lt * LANES * pitch + to * tiles + kt, LANES, stride=pitch)
                        first_row, last_row = r0[rows, :], rn[rows, :]
                    for u, f in enumerate(fs):
                        origin = kt * LANES * step_in + (step_in if step_in == PITCH else 0) + f
                        target = lt * LANES * step_out + (step_out if step_out == PITCH else 0) + f
                        block = src[c, lt, pl.ds(origin, LANES, stride=step_in), :]
                        if explicit:
                            block = own * block - (low * src[c, lt, pl.ds(origin - step_in, LANES, stride=step_in), :]
                                                   + high * src[c, lt, pl.ds(origin + step_in, LANES, stride=step_in), :])
                        if correct:
                            block = block + near * ss[0, lt, pl.ds(f, 1), :] + far * ss[1, lt, pl.ds(f, 1), :]
                        if scale is not None:
                            block = block * scale
                        flipped = block.T
                        dst[c, kt, pl.ds(target, LANES, stride=step_out), :] = flipped
                        if ends:
                            fold = lambda v: v.reshape(LANES // SUB, SUB, LANES).sum(axis=0)
                            h, s = fold(flipped * first_row), fold(flipped * last_row)
                            heads[u] = h if heads[u] is None else heads[u] + h
                            tails[u] = s if tails[u] is None else tails[u] + s
                if ends:
                    for u, f in enumerate(fs):
                        if before:
                            heads[u], tails[u] = heads[u] + part[0, kt, f], tails[u] + part[1, kt, f]
                        if after:
                            part[0, kt, f], part[1, kt, f] = heads[u], tails[u]
                        else:
                            ends[0][kt, pl.ds(f, 1), :] = jnp.sum(heads[u], axis=0, keepdims=True)
                            ends[1][kt, pl.ds(f, 1), :] = jnp.sum(tails[u], axis=0, keepdims=True)
            return carry

        lax.fori_loop(0, SUB // group, column, 0, unroll=True)

    me_y = pos[Y]
    has_before, has_after = me_y > 0, me_y < parts_y - 1

    def halo(side, c, other):
        return pltpu.make_async_remote_copy(
            src_ref=halo_s.at[side, c], dst_ref=halo_r.at[1 - side, c], send_sem=send_sem.at[side, c], recv_sem=recv_y.at[1, c, 1 - side],
            device_id=device(Y, other), device_id_type=LOGICAL)

    def send_halo(c):
        for t in every:
            halo_s[0, c, t] = qs[c, t, slab(0), :]
            halo_s[1, c, t] = qs[c, t, slab(n - 1), :]

        @pl.when(has_before)
        def _():
            halo(0, c, me_y - 1).start()

        @pl.when(has_after)
        def _():
            halo(1, c, me_y + 1).start()

    def await_halo(c):
        @pl.when(has_before)
        def _():
            halo(0, c, me_y - 1).wait_send()
            halo(1, c, me_y - 1).wait_recv()

        @pl.when(has_after)
        def _():
            halo(1, c, me_y + 1).wait_send()
            halo(0, c, me_y + 1).wait_recv()

        for t in every:
            qs[c, t, slab(-1), :] = halo_r[0, c, t]
            qs[c, t, slab(n), :] = halo_r[1, c, t]

    for c in range(chunks):
        for t in range(tiles):
            field_piece(c, t).wait()
            turn(out, qs, c, X, Y, every, (t,), None, step_in=SUB, correct=False)
        if c == 0:
            pl.semaphore_wait(barrier, parts_x + parts_y - 2)
        send_halo(c)
    pltpu.make_async_copy(nat, nat, load_sem).wait()
    for t in range(tiles):
        cols = pl.ds(t * LANES, LANES)
        pa[pl.ds(t, n, stride=pitch), :] = nat[0, :, cols]
        pb[pl.ds(t, n, stride=pitch), :] = nat[1, :, cols] + 1.0
        pc[pl.ds(t, n, stride=pitch), :] = nat[2, :, cols]
        for s in range(tiles):
            rows = pl.ds(s * LANES, LANES)
            dest = pl.ds(t * LANES * pitch + tiles + s, LANES, stride=pitch)
            pa[dest, :] = nat[3, rows, cols].T
            pb[dest, :] = nat[4, rows, cols].T + 1.0
            pc[dest, :] = nat[5, rows, cols].T

    unroll, long = 8, 16
    zero = jnp.zeros((pitch, LANES), F32)
    one = jnp.ones((pitch, LANES), F32)

    def at_row(k, u):
        return pl.ds(pl.multiple_of(k * (long * pitch), long * pitch) + u * pitch, pitch)

    def pivots(g, state):
        dp, dq, c_prev, ep, eq, a_next = state
        h = n // long - 1 - g
        for u in range(long):
            up, down = at_row(g, u), at_row(h, long - 1 - u)
            nd[up, :] = dp
            new = pb[up, :] * dp - (pa[up, :] * c_prev) * dq
            md[up, :] = new
            dp, dq, c_prev = new, dp, pc[up, :]
            ne[down, :] = ep
            new = pb[down, :] * ep - (a_next * pc[down, :]) * eq
            me_[down, :] = new
            ep, eq, a_next = new, ep, pa[down, :]
            if u % 8 == 3:
                scale_d, scale_e = 1.0 / dp, 1.0 / ep
            if u % 8 == 7:
                dp, dq, ep, eq = dp * scale_d, dq * scale_d, ep * scale_e, eq * scale_e
        return dp, dq, c_prev, ep, eq, a_next

    lax.fori_loop(0, n // long, pivots, (one, zero, zero, one, zero, zero))

    low_half = lax.broadcasted_iota(jnp.int32, (SUB, LANES), 0) < pitch
    blocks = n * pitch // SUB
    step_rows = 8

    def ratios(g, state):
        prev_m, next_d = state
        for u in range(step_rows):
            up = pl.ds(pl.multiple_of(g * (SUB * step_rows), SUB * step_rows) + u * SUB, SUB)
            down = pl.ds(pl.multiple_of((blocks // step_rows - 1 - g) * (SUB * step_rows), SUB * step_rows)
                         + (step_rows - 1 - u) * SUB, SUB)
            minv = nd[up, :] / md[up, :]
            m2[up, :] = minv + minv
            cn[up, :] = -pc[up, :] * minv
            turned = pltpu.roll(minv, pitch, 0)
            ln[up, :] = -pa[up, :] * jnp.where(low_half, prev_m, turned)
            prev_m = turned
            dinv = ne[down, :] / me_[down, :]
            d2[down, :] = dinv + dinv
            an[down, :] = -pa[down, :] * dinv
            turned = pltpu.roll(dinv, pitch, 0)
            un[down, :] = -pc[down, :] * jnp.where(low_half, turned, next_d)
            next_d = turned
        return prev_m, next_d

    lax.fori_loop(0, blocks // step_rows, ratios, (blank, blank))

    first, last = pl.ds(0, pitch), pl.ds((n - 1) * pitch, pitch)

    def products(g, state):
        col0, row0, coln, rown, un_prev, ln_next = state
        h = n // long - 1 - g
        for u in range(long):
            up, down = at_row(g, u), at_row(h, long - 1 - u)
            start = jnp.logical_and(g == 0, u == 0) if u == 0 else None
            f0, f1 = an[up, :], un_prev
            b0, b1 = cn[down, :], ln_next
            if u == 0:
                f0, f1 = jnp.where(start, one, f0), jnp.where(start, one, f1)
                b0, b1 = jnp.where(start, one, b0), jnp.where(start, one, b1)
            col0, row0, coln, rown = col0 * f0, row0 * f1, coln * b0, rown * b1
            w2[up, :], r0[up, :], v2[down, :], rn[down, :] = col0, row0, coln, rown
            un_prev, ln_next = un[up, :], ln[down, :]
        return col0, row0, coln, rown, un_prev, ln_next

    d_first, m_last = 0.5 * d2[first, :], 0.5 * m2[last, :]
    lax.fori_loop(0, n // long, products,
                  (-pa[first, :] * d2[first, :], d_first, -pc[last, :] * m2[last, :], m_last, one, one))

    for axis in (X, Y):
        for q, (ref, line) in enumerate(((w2, 0), (w2, n - 1), (v2, 0), (v2, n - 1))):
            gs[axis, pl.ds(q * tiles, tiles), :] = -0.5 * ref[pl.ds(line * pitch + axis * tiles, tiles), :]
        gather[axis][pos[axis]] = gs[axis]
        for other in others(axis):
            pltpu.make_async_remote_copy(
                src_ref=gs.at[axis], dst_ref=gather[axis].at[pos[axis]], send_sem=load_sem, recv_sem=grecv.at[axis],
                device_id=device(axis, other), device_id_type=LOGICAL).start()

    def reduce_lines(axis):
        count, me = parts[axis], pos[axis]
        arrived = gather[axis].at[pl.ds(0, count - 1)]
        pltpu.make_async_copy(arrived, arrived, grecv.at[axis]).wait()
        part = lambda p, q: gather[axis][p, pl.ds(q * tiles, tiles), :]
        nil = jnp.zeros((tiles, LANES), F32)
        unit = jnp.ones((tiles, LANES), F32)
        mu, rho, tau = [None] * count, [None] * count, [None] * count
        prev = nil
        for p in range(count):
            wf, wt, vf, vt = (part(p, q) for q in range(4))
            kappa = 1.0 / (1.0 - wf * prev)
            mu[p], rho[p] = wt * prev * kappa, wt * kappa
            prev = tau[p] = vt + mu[p] * vf
        nu, omega, sigma = [None] * count, [None] * count, [None] * count
        prev = nil
        for p in reversed(range(count)):
            wf, wt, vf, vt = (part(p, q) for q in range(4))
            kappa = 1.0 / (1.0 - vt * prev)
            nu[p], omega[p] = vf * prev * kappa, vf * kappa
            prev = sigma[p] = wf + nu[p] * wt
        pick = lambda values, at: sum(jnp.where(at == p, v, nil) for p, v in enumerate(values))
        tau_b, sigma_a = pick(tau, me - 1), pick(sigma, me + 1)
        mu_me, nu_me = pick(mu, me), pick(nu, me)
        wf, wt, vf, vt = (part(me, q) for q in range(4))
        det = 1.0 / ((1.0 - tau_b * wf) * (1.0 - sigma_a * vt) - (tau_b * vf) * (sigma_a * wt))
        k11, k12 = (1.0 - sigma_a * vt) * det, tau_b * vf * det
        k21, k22 = sigma_a * wt * det, (1.0 - tau_b * wf) * det
        low, high = [None] * count, [None] * count
        for p in reversed(range(count)):
            onward = -rho[p + 1] * low[p + 1] if p + 1 < count else nil
            low[p] = jnp.where(me - 1 == p, unit, jnp.where(p < me - 1, onward, nil))
        for p in range(count):
            onward = -omega[p - 1] * high[p - 1] if p else nil
            high[p] = jnp.where(me + 1 == p, unit, jnp.where(p > me + 1, onward, nil))
        table = reduced[axis]
        put = lambda index, value: table.__setitem__((pl.ds(index * tiles, tiles), slice(None)), value)
        for p in range(count):
            put(p, k11 * low[p] + k12 * high[p] + jnp.where(me == p, -k11 * tau_b, nil))
            put(count + 1 + p, k21 * low[p] + k22 * high[p] + jnp.where(me == p, -k21 * tau_b, nil))
        put(count, -k12 * sigma_a)
        put(2 * count + 1, -k22 * sigma_a)
        put(2 * count + 2, mu_me)
        put(2 * count + 3, nu_me)
        if axis == X:
            for p in range(count):
                put(2 * count + 4 + p, jnp.where(p < me, mu[p], unit))
                put(3 * count + 4 + p, jnp.where(p < me, unit, jnp.where(p > me, nu[p], nil)))

    def slot(axis, way, c, t, p):
        return (way, c, p, t) if axis == X else (way, c, t, p)

    def arrival(axis, way, c, t):
        return recv_x.at[way, c] if axis == X else recv_y.at[way, c, t]

    def publish(axis, stage, c, ts):
        count, table, way = parts[axis], reduced[axis], lax.rem(stage, 2)
        for t in ts:
            head, tail = exch[axis][slot(axis, way, c, t, pos[axis])], gt[c, t]
            mu = table[pl.ds((2 * count + 2) * tiles + t, 1), :]
            nu = table[pl.ds((2 * count + 3) * tiles + t, 1), :]
            send[axis][c, 1, t] = tail + mu * head
            send[axis][c, 0, t] = head + nu * tail
        some = pl.ds(ts[0], len(ts))
        there = exch[X].at[way, c, pos[X]] if axis == X else exch[Y].at[way, c, some, pos[Y]]
        for other in others(axis):
            sel = jnp.where(other > pos[axis], 1, 0)
            pltpu.make_async_remote_copy(
                src_ref=send[axis].at[c, sel, some], dst_ref=there,
                send_sem=send_sem.at[axis, c], recv_sem=arrival(axis, way, c, ts[0]),
                device_id=device(axis, other), device_id_type=LOGICAL).start()

    def combine(axis, stage, c, ts):
        count, table, way = parts[axis], reduced[axis], lax.rem(stage, 2)
        for t in ts:
            for side in range(2):
                base = side * (count + 1) * tiles + t
                total = table[pl.ds(base + count * tiles, 1), :] * gt[c, t]
                for p in range(count):
                    total = total + table[pl.ds(base + p * tiles, 1), :] * exch[axis][slot(axis, way, c, t, p)]
                ss[side, t] = total

    def neighbours(axis, stage, c, ts):
        way = lax.rem(stage, 2)
        some = pl.ds(0, parts[axis] - 1)
        arrived = exch[X].at[way, c, some] if axis == X else exch[Y].at[way, c, pl.ds(ts[0], len(ts)), some]
        pltpu.make_async_copy(arrived, arrived, arrival(axis, way, c, ts[0])).wait()
        if ts[-1] == tiles - 1:
            sent = arrived if axis == X else exch[Y].at[way, c, :, some]
            pltpu.make_async_copy(sent, sent, send_sem.at[axis, c]).wait()
        combine(axis, stage, c, ts)

    def publish_raw(c):
        for t in range(tiles):
            raw[c, pos[X], 0, t] = exch[X][slot(X, 0, c, t, pos[X])]
            raw[c, pos[X], 1, t] = gt[c, t]
        for other in others(X):
            pltpu.make_async_remote_copy(
                src_ref=raw.at[c, pos[X]], dst_ref=raw.at[c, pos[X]], send_sem=send_sem.at[X, c], recv_sem=recv_x.at[0, c],
                device_id=device(X, other), device_id_type=LOGICAL).start()

    def neighbours_raw(c):
        count = parts_x
        arrived = raw.at[c, pl.ds(0, count - 1)]
        pltpu.make_async_copy(arrived, arrived, recv_x.at[0, c]).wait()
        pltpu.make_async_copy(arrived, arrived, send_sem.at[X, c]).wait()
        for t in range(tiles):
            for p in range(count):
                on_head = red_x[pl.ds((2 * count + 4 + p) * tiles + t, 1), :]
                on_tail = red_x[pl.ds((3 * count + 4 + p) * tiles + t, 1), :]
                exch[X][slot(X, 0, c, t, p)] = on_head * raw[c, p, 0, t] + on_tail * raw[c, p, 1, t]
        combine(X, 0, c, every)

    def solve_block(axis, minus):
        def coef(array, k, t):
            return array[pl.ds(k * pitch + axis * tiles + t, 1), :]

        def forward(k, state):
            ups, downs = list(state[0]), list(state[1])
            r = n - 1 - k
            for t in range(tiles):
                up, down = coef(ln, k, t), coef(un, r, t)
                for c in range(chunks):
                    s = c * tiles + t
                    ups[s] = rs[c, t, slab(k), :] + up * ups[s]
                    hs[c, t, slab(k), :] = ups[s]
                    downs[s] = rs[c, t, slab(r), :] + down * downs[s]
                    hs[c, t, slab(r), :] = downs[s]
            return tuple(ups), tuple(downs)

        init = tuple(blank for _ in cells)
        ups, downs = lax.fori_loop(0, half, forward, (init, init), unroll=unroll)
        lo, hi = half - 1, half

        def place(c, t, k, value):
            qs[c, t, slab(k), :] = value - rs[c, t, slab(k), :] if minus else value

        low_s, high_s = [], []
        for s, (c, t) in enumerate(cells):
            c_lo, a_hi = coef(cn, lo, t), coef(an, hi, t)
            kappa = 1.0 / (1.0 - c_lo * a_hi)
            h_hi = coef(d2, hi, t) * downs[s]
            s_lo = kappa * (coef(m2, lo, t) * ups[s] + c_lo * h_hi)
            low_s.append(s_lo)
            high_s.append(h_hi + a_hi * s_lo)
            place(c, t, lo, low_s[s])
            place(c, t, hi, high_s[s])

        def backward(step, state):
            lows, highs = list(state[0]), list(state[1])
            k, r = half - 1 - step, half + step
            for t in range(tiles):
                m_low, c_low, m_high, a_high = coef(m2, k, t), coef(cn, k, t), coef(d2, r, t), coef(an, r, t)
                for c in range(chunks):
                    s = c * tiles + t
                    lows[s] = m_low * hs[c, t, slab(k), :] + c_low * lows[s]
                    place(c, t, k, lows[s])
                    highs[s] = m_high * hs[c, t, slab(r), :] + a_high * highs[s]
                    place(c, t, r, highs[s])
            return tuple(lows), tuple(highs)

        state = lax.fori_loop(1, unroll, backward, (tuple(low_s), tuple(high_s)), unroll=True)
        lax.fori_loop(unroll, half, backward, state, unroll=unroll)

    def each_chunk(body):
        lax.fori_loop(0, chunks, lambda c, carry: (body(c), carry)[1], 0)

    def ends_of(axis, stage, c):
        way = lax.rem(stage, 2)
        return exch[X].at[way, c, pos[X]] if axis == X else exch[Y].at[way, c, :, pos[Y]], gt.at[c]

    def start_x(c):
        await_halo(c)
        turn(qs, rs, c, Y, X, every, every, ends_of(X, 0, c), correct=False, explicit=True)
        publish_raw(c)

    def to_y(stage, c):
        for kt in every:
            turn(qs, rs, c, X, Y, (kt,), every, ends_of(Y, stage, c))
            publish(Y, stage, c, (kt,))

    def to_x(stage, c):
        for lt in every:
            neighbours(Y, stage, c, (lt,))
            turn(qs, rs, c, Y, X, every, (lt,), ends_of(X, stage + 1, c), before=lt > 0, after=lt < tiles - 1)
        publish(X, stage + 1, c, every)

    each_chunk(start_x)
    solve_block(X, True)
    reduce_lines(X)
    reduce_lines(Y)
    sent = gc_x.at[pl.ds(0, parts_x - 1)]
    pltpu.make_async_copy(sent, sent, load_sem).wait()
    sent = gc_y.at[pl.ds(0, parts_y - 1)]
    pltpu.make_async_copy(sent, sent, load_sem).wait()

    def first_to_y(c):
        neighbours_raw(c)
        to_y(0, c)

    each_chunk(first_to_y)

    def step(stage, carry):
        def onward(c):
            neighbours(X, stage, c, every)
            to_y(stage, c)

        solve_block(Y, True)
        each_chunk(lambda c: to_x(stage - 1, c))
        solve_block(X, True)
        each_chunk(onward)
        return carry

    lax.fori_loop(1, STEPS, step, 0)
    solve_block(Y, False)

    def finish(c):
        for lt in every:
            neighbours(Y, STEPS - 1, c, (lt,))
            turn(qs, out, c, Y, X, every, (lt,), None, scale=0.5, step_out=SUB)

    lax.fori_loop(0, chunks - 1, lambda c, carry: (finish(c), carry)[1], 0)
    for lt in every:
        neighbours(Y, STEPS - 1, chunks - 1, (lt,))
        if lt < tiles - 1:
            turn(qs, out, chunks - 1, Y, X, every, (lt,), None, scale=0.5, step_out=SUB)


def finish_kernel(done, qs, w2, v2, ss, out, fresh, sem):
    chunks, tiles = done.shape[:2]
    pitch = 2 * tiles
    last_c, last_t = chunks - 1, tiles - 1

    def place(c, t, src, first_line, count, which):
        return pltpu.make_async_copy(src.reshape(count, SUB, LANES),
                                     out.at[pl.ds(first_line, count), pl.ds(c * SUB, SUB), pl.ds(t * LANES, LANES)], sem.at[which])

    lines = done.shape[2] // SUB
    early = lines - LANES
    copies = [place(c, t, done.at[c, t], 0, lines, c * tiles + t) for c in range(last_c) for t in range(tiles)]
    copies += [place(last_c, t, done.at[last_c, t, pl.ds(0, early * SUB)], 0, early, last_c * tiles + t) for t in range(tiles)]
    for copy in copies:
        copy.start()

    def column(f, carry):
        for kt in range(tiles):
            rows = pl.ds(kt * LANES * pitch + tiles + last_t, LANES, stride=pitch)
            block = qs[last_c, last_t, pl.ds((kt * LANES + 1) * PITCH + f, LANES, stride=PITCH), :]
            block = block + w2[rows, :] * ss[0, last_t, pl.ds(f, 1), :] + v2[rows, :] * ss[1, last_t, pl.ds(f, 1), :]
            fresh[kt, pl.ds(f, LANES, stride=SUB), :] = (block * 0.5).T
        return carry

    lax.fori_loop(0, SUB, column, 0, unroll=True)
    late = [place(last_c, t, fresh.at[t], early, LANES, chunks * tiles + t) for t in range(tiles)]
    for copy in late:
        copy.start()
    for copy in copies + late:
        copy.wait()


def solution(mesh):
    parts_x, parts_y = mesh.shape["row"], mesh.shape["col"]
    strides, stride = {}, 1
    for name in reversed(mesh.axis_names):
        strides[name], stride = stride, stride * mesh.shape[name]
    field_spec = P(("batch", "row"), "col", None)
    coeff_spec = P(("batch", "row"), "col")

    def local_steps(field, *coeffs):
        n, fields = field.shape[0], field.shape[2]
        tiles, chunks = n // LANES, fields // SUB
        packed = pltpu.VMEM((n * 2 * tiles, LANES), F32)
        plane = -(-((n + 2) * PITCH - SUB) // (4 * SUB)) * 4 * SUB + SUB
        big = pltpu.VMEM((chunks, tiles, plane, LANES), F32)
        dma = pltpu.SemaphoreType.DMA
        sends = pltpu.VMEM((chunks, 2, tiles, SUB, LANES), F32)
        table = lambda count: pltpu.VMEM(((4 * count + 4) * tiles, LANES), F32)
        small = pltpu.VMEM((2, chunks, tiles, SUB, LANES), F32)
        message = (4 * tiles, LANES)
        scratch = [
            pltpu.VMEM((6, n, n), F32), big, big, *([packed] * 15),
            pltpu.VMEM((2,) + message, F32), pltpu.VMEM((parts_x,) + message, F32), pltpu.VMEM((parts_y,) + message, F32),
            table(parts_x), table(parts_y), sends, sends,
            pltpu.VMEM((2, chunks, parts_x, tiles, SUB, LANES), F32), pltpu.VMEM((2, chunks, tiles, parts_y, SUB, LANES), F32),
            pltpu.VMEM((chunks, parts_x, 2, tiles, SUB, LANES), F32), pltpu.VMEM((chunks, tiles, SUB, LANES), F32),
            pltpu.VMEM((2, tiles, SUB, SUB, LANES), F32), small, small,
            dma, dma((2, chunks)), dma((2, chunks)), dma((2, chunks, tiles)), dma((2,)),
        ]
        in_hbm = pl.BlockSpec(memory_space=pltpu.HBM)
        turned = jnp.transpose(field, (0, 2, 1))
        in_vmem = pl.BlockSpec(memory_space=pltpu.VMEM)
        shape = lambda *dims: jax.ShapeDtypeStruct(dims, F32)
        handed = (shape(chunks, tiles, n * SUB, LANES), shape(chunks, tiles, plane, LANES), shape(n * 2 * tiles, LANES),
                  shape(n * 2 * tiles, LANES), shape(2, tiles, SUB, LANES))
        handed = pl.pallas_call(
            functools.partial(adi_kernel, (("row", parts_x), ("col", parts_y)), strides),
            out_shape=handed, in_specs=[in_hbm] * 7, out_specs=(in_vmem,) * len(handed), scratch_shapes=scratch,
            compiler_params=pltpu.CompilerParams(collective_id=0, has_side_effects=True, vmem_limit_bytes=36 * 1024 * 1024),
            name="adi_steps",
        )(*(pltpu.with_memory_space_constraint(array, pltpu.HBM) for array in (turned,) + coeffs))
        result = pl.pallas_call(
            finish_kernel, out_shape=jax.ShapeDtypeStruct(turned.shape, F32),
            in_specs=[in_vmem] * len(handed), out_specs=in_hbm,
            scratch_shapes=[pltpu.VMEM((tiles, LANES * SUB, LANES), F32), dma((chunks * tiles + tiles,))],
            compiler_params=pltpu.CompilerParams(vmem_limit_bytes=8 * 1024 * 1024), name="finish",
        )(*handed)
        return jnp.transpose(result, (0, 2, 1))

    return jax.shard_map(local_steps, mesh=mesh, in_specs=(field_spec,) + (coeff_spec,) * 6, out_specs=field_spec, check_vma=False)
```

```python
import functools

import jax
import jax.numpy as jnp
from jax import lax
from jax.experimental import pallas as pl
from jax.experimental.pallas import tpu as pltpu
from jax.sharding import PartitionSpec as P

STEPS = 3
F32 = jnp.float32
LANES = 128
SUB = 8
UNIT = SUB // 2
PITCH = SUB + 1
LOGICAL = pl.DeviceIdType.LOGICAL
X, Y = 0, 1


def adi_kernel(axes, strides, field, lower_x, diag_x, upper_x, lower_y, diag_y, upper_y, out, qs, w2, v2, ss,
               nat, rs, hs, pa, pb, pc, nd, md, ne, me_, ln, cn, un, an, m2, d2, r0, rn,
               gs, gc_x, gc_y, red_x, red_y, sx, sy, ex, ey, raw, gt, halo_s, halo_r,
               load_sem, send_sem, recv_x, recv_y, grecv):
    (row_name, parts_x), (col_name, parts_y) = axes
    n = lower_x.shape[0]
    tiles = n // LANES
    chunks = field.shape[1] // SUB
    parts_of = SUB // UNIT
    units = chunks * parts_of
    pitch = 2 * tiles
    half = n // 2
    group = 2
    pos = (lax.axis_index(row_name), lax.axis_index(col_name))
    parts = (parts_x, parts_y)
    home = sum(lax.axis_index(name) * stride for name, stride in strides.items())
    exch = (ex, ey)
    recv = (recv_x, recv_y)
    send = (sx, sy)
    gather = (gc_x, gc_y)
    reduced = (red_x, red_y)

    def device(axis, other):
        return home + (other - pos[axis]) * strides[(row_name, col_name)[axis]]

    def others(axis):
        count = parts[axis]
        offs = sorted(range(1, count), key=lambda off: -min(off, count - off))
        return [lax.rem(pos[axis] + off, count) for off in offs]

    def field_piece(c, t):
        return pltpu.make_async_copy(field.at[:, pl.ds(c * SUB, SUB), pl.ds(t * LANES, LANES)],
                                     out.at[c, t].reshape(n, SUB, LANES), send_sem.at[t, c, 0])

    for c in range(chunks):
        for t in range(tiles):
            field_piece(c, t).start()
    for slot, ref in enumerate((lower_x, diag_x, upper_x, lower_y, diag_y, upper_y)):
        pltpu.make_async_copy(ref, nat.at[slot], load_sem).start()

    halo_r[...] = jnp.zeros_like(halo_r)
    barrier = pltpu.get_barrier_semaphore()
    for axis in (X, Y):
        for other in others(axis):
            pl.semaphore_signal(barrier, 1, device_id=device(axis, other), device_id_type=LOGICAL)

    blank = jnp.zeros((SUB, LANES), F32)
    every = tuple(range(tiles))
    cells = [(c, t) for c in range(chunks) for t in range(tiles)]

    def slab(k):
        return pl.ds((k + 1) * PITCH, SUB)

    def each_chunk(body):
        lax.fori_loop(0, chunks, lambda c, carry: (body(c), carry)[1], 0)

    def turn(src, dst, c, axis, to, base, many, lts, ends=None, step_in=PITCH, step_out=PITCH, correct=True, explicit=False, scale=None):
        def column(g, carry):
            fs = [g * group + u for u in range(group)]
            for kt in every:
                heads, tails = [None] * group, [None] * group
                for lt in lts:
                    rows = pl.ds(kt * (LANES * pitch) + (axis * tiles + lt), LANES, stride=pitch)
                    if correct:
                        near, far = w2[rows, :], v2[rows, :]
                    if explicit:
                        own, low, high = 2.0 - pb[rows, :], pa[rows, :], pc[rows, :]
                    if ends:
                        rows = pl.ds(lt * LANES * pitch + to * tiles + kt, LANES, stride=pitch)
                        first_row, last_row = r0[rows, :], rn[rows, :]
                    for u, f in enumerate(fs):
                        origin = kt * LANES * step_in + (step_in if step_in == PITCH else 0) + base + f
                        target = lt * LANES * step_out + (step_out if step_out == PITCH else 0) + base + f
                        block = src[c, lt, pl.ds(origin, LANES, stride=step_in), :]
                        if explicit:
                            block = own * block - (low * src[c, lt, pl.ds(origin - step_in, LANES, stride=step_in), :]
                                                   + high * src[c, lt, pl.ds(origin + step_in, LANES, stride=step_in), :])
                        if correct:
                            block = block + near * ss[0, lt, pl.ds(f, 1), :] + far * ss[1, lt, pl.ds(f, 1), :]
                        if scale is not None:
                            block = block * scale
                        flipped = block.T
                        dst[c, kt, pl.ds(target, LANES, stride=step_out), :] = flipped
                        if ends:
                            fold = lambda v: v.reshape(LANES // SUB, SUB, LANES).sum(axis=0)
                            h, s = fold(flipped * first_row), fold(flipped * last_row)
                            heads[u] = h if heads[u] is None else heads[u] + h
                            tails[u] = s if tails[u] is None else tails[u] + s
                if ends:
                    for u, f in enumerate(fs):
                        ends[0][kt, pl.ds(f, 1), :] = jnp.sum(heads[u], axis=0, keepdims=True)
                        ends[1][kt, pl.ds(f, 1), :] = jnp.sum(tails[u], axis=0, keepdims=True)
            return carry

        lax.fori_loop(0, many // group, column, 0, unroll=True)

    me_y = pos[Y]
    has_before, has_after = me_y > 0, me_y < parts_y - 1

    def halo(side, c, other):
        return pltpu.make_async_remote_copy(
            src_ref=halo_s.at[side, c], dst_ref=halo_r.at[1 - side, c], send_sem=send_sem.at[side, c, 0], recv_sem=recv_y.at[1, c, 1 - side],
            device_id=device(Y, other), device_id_type=LOGICAL)

    def send_halo(c):
        for t in every:
            halo_s[0, c, t] = qs[c, t, slab(0), :]
            halo_s[1, c, t] = qs[c, t, slab(n - 1), :]

        @pl.when(has_before)
        def _():
            halo(0, c, me_y - 1).start()

        @pl.when(has_after)
        def _():
            halo(1, c, me_y + 1).start()

    def await_halo(c):
        @pl.when(has_before)
        def _():
            halo(0, c, me_y - 1).wait_send()
            halo(1, c, me_y - 1).wait_recv()

        @pl.when(has_after)
        def _():
            halo(1, c, me_y + 1).wait_send()
            halo(0, c, me_y + 1).wait_recv()

        for t in every:
            qs[c, t, slab(-1), :] = halo_r[0, c, t]
            qs[c, t, slab(n), :] = halo_r[1, c, t]

    for c in range(chunks):
        for t in range(tiles):
            field_piece(c, t).wait()
            turn(out, qs, c, X, Y, 0, SUB, (t,), step_in=SUB, correct=False)
        if c == 0:
            pl.semaphore_wait(barrier, parts_x + parts_y - 2)
        send_halo(c)
    pltpu.make_async_copy(nat, nat, load_sem).wait()
    for t in range(tiles):
        cols = pl.ds(t * LANES, LANES)
        pa[pl.ds(t, n, stride=pitch), :] = nat[0, :, cols]
        pb[pl.ds(t, n, stride=pitch), :] = nat[1, :, cols] + 1.0
        pc[pl.ds(t, n, stride=pitch), :] = nat[2, :, cols]
        for s in range(tiles):
            rows = pl.ds(s * LANES, LANES)
            dest = pl.ds(t * LANES * pitch + tiles + s, LANES, stride=pitch)
            pa[dest, :] = nat[3, rows, cols].T
            pb[dest, :] = nat[4, rows, cols].T + 1.0
            pc[dest, :] = nat[5, rows, cols].T

    unroll, long = 8, 16
    zero = jnp.zeros((pitch, LANES), F32)
    one = jnp.ones((pitch, LANES), F32)

    def at_row(k, u):
        return pl.ds(pl.multiple_of(k * (long * pitch), long * pitch) + u * pitch, pitch)

    def pivots(g, state):
        dp, dq, c_prev, ep, eq, a_next = state
        h = n // long - 1 - g
        for u in range(long):
            up, down = at_row(g, u), at_row(h, long - 1 - u)
            nd[up, :] = dp
            new = pb[up, :] * dp - (pa[up, :] * c_prev) * dq
            md[up, :] = new
            dp, dq, c_prev = new, dp, pc[up, :]
            ne[down, :] = ep
            new = pb[down, :] * ep - (a_next * pc[down, :]) * eq
            me_[down, :] = new
            ep, eq, a_next = new, ep, pa[down, :]
            if u % 8 == 3:
                scale_d, scale_e = 1.0 / dp, 1.0 / ep
            if u % 8 == 7:
                dp, dq, ep, eq = dp * scale_d, dq * scale_d, ep * scale_e, eq * scale_e
        return dp, dq, c_prev, ep, eq, a_next

    lax.fori_loop(0, n // long, pivots, (one, zero, zero, one, zero, zero))

    low_half = lax.broadcasted_iota(jnp.int32, (SUB, LANES), 0) < pitch
    blocks = n * pitch // SUB
    step_rows = 8

    def ratios(g, state):
        prev_m, next_d = state
        for u in range(step_rows):
            up = pl.ds(pl.multiple_of(g * (SUB * step_rows), SUB * step_rows) + u * SUB, SUB)
            down = pl.ds(pl.multiple_of((blocks // step_rows - 1 - g) * (SUB * step_rows), SUB * step_rows)
                         + (step_rows - 1 - u) * SUB, SUB)
            minv = nd[up, :] / md[up, :]
            m2[up, :] = minv + minv
            cn[up, :] = -pc[up, :] * minv
            turned = pltpu.roll(minv, pitch, 0)
            ln[up, :] = -pa[up, :] * jnp.where(low_half, prev_m, turned)
            prev_m = turned
            dinv = ne[down, :] / me_[down, :]
            d2[down, :] = dinv + dinv
            an[down, :] = -pa[down, :] * dinv
            turned = pltpu.roll(dinv, pitch, 0)
            un[down, :] = -pc[down, :] * jnp.where(low_half, turned, next_d)
            next_d = turned
        return prev_m, next_d

    lax.fori_loop(0, blocks // step_rows, ratios, (blank, blank))

    first, last = pl.ds(0, pitch), pl.ds((n - 1) * pitch, pitch)

    def products(g, state):
        col0, row0, coln, rown, un_prev, ln_next = state
        h = n // long - 1 - g
        for u in range(long):
            up, down = at_row(g, u), at_row(h, long - 1 - u)
            start = jnp.logical_and(g == 0, u == 0) if u == 0 else None
            f0, f1 = an[up, :], un_prev
            b0, b1 = cn[down, :], ln_next
            if u == 0:
                f0, f1 = jnp.where(start, one, f0), jnp.where(start, one, f1)
                b0, b1 = jnp.where(start, one, b0), jnp.where(start, one, b1)
            col0, row0, coln, rown = col0 * f0, row0 * f1, coln * b0, rown * b1
            w2[up, :], r0[up, :], v2[down, :], rn[down, :] = col0, row0, coln, rown
            un_prev, ln_next = un[up, :], ln[down, :]
        return col0, row0, coln, rown, un_prev, ln_next

    d_first, m_last = 0.5 * d2[first, :], 0.5 * m2[last, :]
    lax.fori_loop(0, n // long, products,
                  (-pa[first, :] * d2[first, :], d_first, -pc[last, :] * m2[last, :], m_last, one, one))

    for axis in (X, Y):
        for q, (ref, line) in enumerate(((w2, 0), (w2, n - 1), (v2, 0), (v2, n - 1))):
            gs[axis, pl.ds(q * tiles, tiles), :] = -0.5 * ref[pl.ds(line * pitch + axis * tiles, tiles), :]
        gather[axis][pos[axis]] = gs[axis]
        for other in others(axis):
            pltpu.make_async_remote_copy(
                src_ref=gs.at[axis], dst_ref=gather[axis].at[pos[axis]], send_sem=load_sem, recv_sem=grecv.at[axis],
                device_id=device(axis, other), device_id_type=LOGICAL).start()

    def reduce_lines(axis):
        count, me = parts[axis], pos[axis]
        arrived = gather[axis].at[pl.ds(0, count - 1)]
        pltpu.make_async_copy(arrived, arrived, grecv.at[axis]).wait()
        part = lambda p, q: gather[axis][p, pl.ds(q * tiles, tiles), :]
        nil = jnp.zeros((tiles, LANES), F32)
        unit = jnp.ones((tiles, LANES), F32)
        mu, rho, tau = [None] * count, [None] * count, [None] * count
        prev = nil
        for p in range(count):
            wf, wt, vf, vt = (part(p, q) for q in range(4))
            kappa = 1.0 / (1.0 - wf * prev)
            mu[p], rho[p] = wt * prev * kappa, wt * kappa
            prev = tau[p] = vt + mu[p] * vf
        nu, omega, sigma = [None] * count, [None] * count, [None] * count
        prev = nil
        for p in reversed(range(count)):
            wf, wt, vf, vt = (part(p, q) for q in range(4))
            kappa = 1.0 / (1.0 - vt * prev)
            nu[p], omega[p] = vf * prev * kappa, vf * kappa
            prev = sigma[p] = wf + nu[p] * wt
        pick = lambda values, at: sum(jnp.where(at == p, v, nil) for p, v in enumerate(values))
        tau_b, sigma_a = pick(tau, me - 1), pick(sigma, me + 1)
        mu_me, nu_me = pick(mu, me), pick(nu, me)
        wf, wt, vf, vt = (part(me, q) for q in range(4))
        det = 1.0 / ((1.0 - tau_b * wf) * (1.0 - sigma_a * vt) - (tau_b * vf) * (sigma_a * wt))
        k11, k12 = (1.0 - sigma_a * vt) * det, tau_b * vf * det
        k21, k22 = sigma_a * wt * det, (1.0 - tau_b * wf) * det
        low, high = [None] * count, [None] * count
        for p in reversed(range(count)):
            onward = -rho[p + 1] * low[p + 1] if p + 1 < count else nil
            low[p] = jnp.where(me - 1 == p, unit, jnp.where(p < me - 1, onward, nil))
        for p in range(count):
            onward = -omega[p - 1] * high[p - 1] if p else nil
            high[p] = jnp.where(me + 1 == p, unit, jnp.where(p > me + 1, onward, nil))
        table = reduced[axis]
        put = lambda index, value: table.__setitem__((pl.ds(index * tiles, tiles), slice(None)), value)
        for p in range(count):
            put(p, k11 * low[p] + k12 * high[p] + jnp.where(me == p, -k11 * tau_b, nil))
            put(count + 1 + p, k21 * low[p] + k22 * high[p] + jnp.where(me == p, -k21 * tau_b, nil))
        put(count, -k12 * sigma_a)
        put(2 * count + 1, -k22 * sigma_a)
        put(2 * count + 2, mu_me)
        put(2 * count + 3, nu_me)
        if axis == X:
            for p in range(count):
                put(2 * count + 4 + p, jnp.where(p < me, mu[p], unit))
                put(3 * count + 4 + p, jnp.where(p < me, unit, jnp.where(p > me, nu[p], nil)))

    def publish(axis, stage, c, g):
        count, table, way = parts[axis], reduced[axis], lax.rem(stage, 2)
        for t in every:
            head, tail = exch[axis][way, c, g, pos[axis], t], gt[c, g, t]
            mu = table[pl.ds((2 * count + 2) * tiles + t, 1), :]
            nu = table[pl.ds((2 * count + 3) * tiles + t, 1), :]
            send[axis][c, g, 1, t] = tail + mu * head
            send[axis][c, g, 0, t] = head + nu * tail
        for other in others(axis):
            sel = jnp.where(other > pos[axis], 1, 0)
            pltpu.make_async_remote_copy(
                src_ref=send[axis].at[c, g, sel], dst_ref=exch[axis].at[way, c, g, pos[axis]],
                send_sem=send_sem.at[axis, c, g], recv_sem=recv[axis].at[way, c, g],
                device_id=device(axis, other), device_id_type=LOGICAL).start()

    def combine(axis, way, c, g):
        count, table = parts[axis], reduced[axis]
        for t in every:
            for side in range(2):
                base = side * (count + 1) * tiles + t
                total = table[pl.ds(base + count * tiles, 1), :] * gt[c, g, t]
                for p in range(count):
                    total = total + table[pl.ds(base + p * tiles, 1), :] * exch[axis][way, c, g, p, t]
                ss[side, t] = total

    def neighbours(axis, stage, c, g):
        way = lax.rem(stage, 2)
        arrived = exch[axis].at[way, c, g, pl.ds(0, parts[axis] - 1)]
        pltpu.make_async_copy(arrived, arrived, recv[axis].at[way, c, g]).wait()
        pltpu.make_async_copy(arrived, arrived, send_sem.at[axis, c, g]).wait()
        combine(axis, way, c, g)

    def publish_raw(c, g):
        for t in every:
            raw[c, g, pos[X], 0, t] = exch[X][0, c, g, pos[X], t]
            raw[c, g, pos[X], 1, t] = gt[c, g, t]
        for other in others(X):
            pltpu.make_async_remote_copy(
                src_ref=raw.at[c, g, pos[X]], dst_ref=raw.at[c, g, pos[X]], send_sem=send_sem.at[X, c, g], recv_sem=recv_x.at[0, c, g],
                device_id=device(X, other), device_id_type=LOGICAL).start()

    def neighbours_raw(c, g):
        count = parts_x
        arrived = raw.at[c, g, pl.ds(0, count - 1)]
        pltpu.make_async_copy(arrived, arrived, recv_x.at[0, c, g]).wait()
        pltpu.make_async_copy(arrived, arrived, send_sem.at[X, c, g]).wait()
        for t in every:
            for p in range(count):
                on_head = red_x[pl.ds((2 * count + 4 + p) * tiles + t, 1), :]
                on_tail = red_x[pl.ds((3 * count + 4 + p) * tiles + t, 1), :]
                exch[X][0, c, g, p, t] = on_head * raw[c, g, p, 0, t] + on_tail * raw[c, g, p, 1, t]
        combine(X, 0, c, g)

    def solve_block(axis, minus):
        def coef(array, k, t):
            return array[pl.ds(k * pitch + axis * tiles + t, 1), :]

        def walk(first, sign, count, visit, state):
            def block(g, state):
                line = first + sign * unroll * g
                row, coef_row = (line + 1) * PITCH, line * pitch + axis * tiles

                def one(u, state):
                    at = lambda array, t: array[pl.ds(coef_row + t + u * (sign * pitch), 1), :]
                    return visit(pl.ds(row + u * (sign * PITCH), SUB), at, state)

                return lax.fori_loop(0, min(count, unroll), one, state, unroll=True)

            return lax.fori_loop(0, max(count // unroll, 1), block, state)

        def eliminate(mult):
            def visit(here, at, state):
                values = list(state)
                for t in every:
                    factor = at(mult, t)
                    for c in range(chunks):
                        s = c * tiles + t
                        values[s] = rs[c, t, here, :] + factor * values[s]
                        hs[c, t, here, :] = values[s]
                return tuple(values)
            return visit

        init = tuple(blank for _ in cells)
        ups = walk(0, 1, half, eliminate(ln), init)
        downs = walk(n - 1, -1, half, eliminate(un), init)
        lo, hi = half - 1, half

        def place(c, t, here, value):
            qs[c, t, here, :] = value - rs[c, t, here, :] if minus else value

        low_s, high_s = [], []
        for s, (c, t) in enumerate(cells):
            c_lo, a_hi = coef(cn, lo, t), coef(an, hi, t)
            kappa = 1.0 / (1.0 - c_lo * a_hi)
            h_hi = coef(d2, hi, t) * downs[s]
            s_lo = kappa * (coef(m2, lo, t) * ups[s] + c_lo * h_hi)
            low_s.append(s_lo)
            high_s.append(h_hi + a_hi * s_lo)
            place(c, t, slab(lo), low_s[s])
            place(c, t, slab(hi), high_s[s])

        def substitute(scale, mult):
            def visit(here, at, state):
                values = list(state)
                for t in every:
                    own, factor = at(scale, t), at(mult, t)
                    for c in range(chunks):
                        s = c * tiles + t
                        values[s] = own * hs[c, t, here, :] + factor * values[s]
                        place(c, t, here, values[s])
                return tuple(values)
            return visit

        for first, sign, visit, state in ((lo, -1, substitute(m2, cn), low_s), (hi, 1, substitute(d2, an), high_s)):
            state = walk(first + sign, sign, unroll - 1, visit, tuple(state))
            walk(first + sign * unroll, sign, half - unroll, visit, state)

    def each_unit(body, count=units):
        lax.fori_loop(0, count, lambda u, carry: (body(u // parts_of, lax.rem(u, parts_of)), carry)[1], 0)

    def ends_of(axis, stage, c, g):
        return exch[axis].at[lax.rem(stage, 2), c, g, pos[axis]], gt.at[c, g]

    def start_x(c):
        def unit(g, carry):
            turn(qs, rs, c, Y, X, g * UNIT, UNIT, every, ends_of(X, 0, c, g), correct=False, explicit=True)
            publish_raw(c, g)
            return carry

        await_halo(c)
        lax.fori_loop(0, parts_of, unit, 0)

    def onward(axis, stage, to, to_stage):
        def unit(c, g):
            neighbours(axis, stage, c, g)
            turn(qs, rs, c, axis, to, g * UNIT, UNIT, every, ends_of(to, to_stage, c, g))
            publish(to, to_stage, c, g)

        each_unit(unit)

    each_chunk(start_x)
    solve_block(X, True)
    reduce_lines(X)
    reduce_lines(Y)
    sent = gc_x.at[pl.ds(0, parts_x - 1)]
    pltpu.make_async_copy(sent, sent, load_sem).wait()
    sent = gc_y.at[pl.ds(0, parts_y - 1)]
    pltpu.make_async_copy(sent, sent, load_sem).wait()

    def first_to_y(c, g):
        neighbours_raw(c, g)
        turn(qs, rs, c, X, Y, g * UNIT, UNIT, every, ends_of(Y, 0, c, g))
        publish(Y, 0, c, g)

    each_unit(first_to_y)

    def step(stage, carry):
        solve_block(Y, True)
        onward(Y, stage - 1, X, stage)
        solve_block(X, True)
        onward(X, stage, Y, stage)
        return carry

    lax.fori_loop(1, STEPS, step, 0)
    solve_block(Y, False)

    def finish(c, g):
        neighbours(Y, STEPS - 1, c, g)
        turn(qs, out, c, Y, X, g * UNIT, UNIT, every, scale=0.5, step_out=SUB)

    each_unit(finish, units - 1)
    neighbours(Y, STEPS - 1, chunks - 1, parts_of - 1)


def finish_kernel(done, qs, w2, v2, ss, out, fresh, sem):
    chunks, tiles = done.shape[:2]
    lines, pitch, last = done.shape[2] // SUB, 2 * tiles, chunks - 1
    base = SUB - UNIT

    def place(c, t, src):
        return pltpu.make_async_copy(src.reshape(lines, SUB, LANES), out.at[:, pl.ds(c * SUB, SUB), pl.ds(t * LANES, LANES)],
                                     sem.at[c * tiles + t])

    copies = [place(c, t, done.at[c, t]) for c in range(last) for t in range(tiles)]
    for copy in copies:
        copy.start()
    for kt in range(tiles):
        fresh[kt] = done[last, kt]

        def column(f, carry):
            for lt in range(tiles):
                rows = pl.ds(kt * LANES * pitch + tiles + lt, LANES, stride=pitch)
                block = qs[last, lt, pl.ds((kt * LANES + 1) * PITCH + base + f, LANES, stride=PITCH), :]
                block = block + w2[rows, :] * ss[0, lt, pl.ds(f, 1), :] + v2[rows, :] * ss[1, lt, pl.ds(f, 1), :]
                fresh[kt, pl.ds(lt * LANES * SUB + base + f, LANES, stride=SUB), :] = (block * 0.5).T
            return carry

        lax.fori_loop(0, UNIT, column, 0, unroll=True)
        copies.append(place(last, kt, fresh.at[kt]))
        copies[-1].start()
    for copy in copies:
        copy.wait()


def solution(mesh):
    parts_x, parts_y = mesh.shape["row"], mesh.shape["col"]
    strides, stride = {}, 1
    for name in reversed(mesh.axis_names):
        strides[name], stride = stride, stride * mesh.shape[name]
    field_spec = P(("batch", "row"), "col", None)
    coeff_spec = P(("batch", "row"), "col")

    def local_steps(field, *coeffs):
        n, fields = field.shape[0], field.shape[2]
        tiles, chunks = n // LANES, fields // SUB
        packed = pltpu.VMEM((n * 2 * tiles, LANES), F32)
        plane = -(-((n + 2) * PITCH - SUB) // (4 * SUB)) * 4 * SUB + SUB
        big = pltpu.VMEM((chunks, tiles, plane, LANES), F32)
        dma = pltpu.SemaphoreType.DMA
        parts_of = SUB // UNIT
        sends = pltpu.VMEM((chunks, parts_of, 2, tiles, UNIT, LANES), F32)
        line = lambda count: pltpu.VMEM((2, chunks, parts_of, count, tiles, UNIT, LANES), F32)
        table = lambda count: pltpu.VMEM(((4 * count + 4) * tiles, LANES), F32)
        small = pltpu.VMEM((2, chunks, tiles, SUB, LANES), F32)
        message = (4 * tiles, LANES)
        scratch = [
            pltpu.VMEM((6, n, n), F32), big, big, *([packed] * 15),
            pltpu.VMEM((2,) + message, F32), pltpu.VMEM((parts_x,) + message, F32), pltpu.VMEM((parts_y,) + message, F32),
            table(parts_x), table(parts_y), sends, sends, line(parts_x), line(parts_y),
            pltpu.VMEM((chunks, parts_of, parts_x, 2, tiles, UNIT, LANES), F32), pltpu.VMEM((chunks, parts_of, tiles, UNIT, LANES), F32),
            small, small, dma, dma((2, chunks, parts_of)), dma((2, chunks, parts_of)), dma((2, chunks, parts_of)), dma((2,)),
        ]
        in_hbm = pl.BlockSpec(memory_space=pltpu.HBM)
        turned = jnp.transpose(field, (0, 2, 1))
        in_vmem = pl.BlockSpec(memory_space=pltpu.VMEM)
        shape = lambda *dims: jax.ShapeDtypeStruct(dims, F32)
        handed = (shape(chunks, tiles, n * SUB, LANES), shape(chunks, tiles, plane, LANES), shape(n * 2 * tiles, LANES),
                  shape(n * 2 * tiles, LANES), shape(2, tiles, UNIT, LANES))
        handed = pl.pallas_call(
            functools.partial(adi_kernel, (("row", parts_x), ("col", parts_y)), strides),
            out_shape=handed, in_specs=[in_hbm] * 7, out_specs=(in_vmem,) * len(handed), scratch_shapes=scratch,
            compiler_params=pltpu.CompilerParams(collective_id=0, has_side_effects=True, vmem_limit_bytes=36 * 1024 * 1024),
            name="adi_steps",
        )(*(pltpu.with_memory_space_constraint(array, pltpu.HBM) for array in (turned,) + coeffs))
        result = pl.pallas_call(
            finish_kernel, out_shape=jax.ShapeDtypeStruct(turned.shape, F32),
            in_specs=[in_vmem] * len(handed), out_specs=in_hbm,
            scratch_shapes=[pltpu.VMEM((tiles, n * SUB, LANES), F32), dma((chunks * tiles,))],
            compiler_params=pltpu.CompilerParams(vmem_limit_bytes=8 * 1024 * 1024), name="finish",
        )(*handed)
        return jnp.transpose(result, (0, 2, 1))

    return jax.shard_map(local_steps, mesh=mesh, in_specs=(field_spec,) + (coeff_spec,) * 6, out_specs=field_spec, check_vma=False)
```

```python
import functools

import jax
import jax.numpy as jnp
from jax import lax
from jax.experimental import pallas as pl
from jax.experimental.pallas import tpu as pltpu
from jax.sharding import PartitionSpec as P

STEPS = 3
F32 = jnp.float32
LANES = 128
SUB = 8
UNIT = SUB // 2
PITCH = SUB + 1
LOGICAL = pl.DeviceIdType.LOGICAL
X, Y = 0, 1


def adi_kernel(axes, strides, field, lower_x, diag_x, upper_x, lower_y, diag_y, upper_y, out, qs, w2, v2, ss,
               nat, rs, hs, pa, pb, pc, nd, md, ne, me_, ln, cn, un, an, m2, d2, r0, rn,
               gs, gc, red_x, red_y, sx, sy, ex, ey, raw, gt, halo_s, halo_r,
               load_sem, late_sem, send_sem, recv_x, recv_y, gather_sem):
    (row_name, parts_x), (col_name, parts_y) = axes
    n = lower_x.shape[0]
    tiles = n // LANES
    chunks = field.shape[1] // SUB
    parts_of = SUB // UNIT
    units = chunks * parts_of
    pitch = 2 * tiles
    half = n // 2
    pos = (lax.axis_index(row_name), lax.axis_index(col_name))
    parts = (parts_x, parts_y)
    home = sum(lax.axis_index(name) * stride for name, stride in strides.items())
    exch = (ex, ey)
    recv = (recv_x, recv_y)
    send = (sx, sy)
    reduced = (red_x, red_y)

    def device(axis, other):
        return home + (other - pos[axis]) * strides[(row_name, col_name)[axis]]

    def others(axis):
        count = parts[axis]
        offs = sorted(range(1, count), key=lambda off: -min(off, count - off))
        return [lax.rem(pos[axis] + off, count) for off in offs]

    def field_piece(c, t, first=0, count=n):
        return pltpu.make_async_copy(field.at[pl.ds(first, count), pl.ds(c * SUB, SUB), pl.ds(t * LANES, LANES)],
                                     out.at[c, t, pl.ds(first * SUB, count * SUB)].reshape(count, SUB, LANES), send_sem.at[t, c, 0])

    def load_field(c):
        for t in range(tiles):
            for first in range(0, n, LANES):
                field_piece(c, t, first, LANES).start()

    def load_coefficients(axis):
        for slot, ref in enumerate(((lower_x, diag_x, upper_x), (lower_y, diag_y, upper_y))[axis]):
            pltpu.make_async_copy(ref, nat.at[3 * axis + slot], (load_sem, late_sem)[axis]).start()

    for c in range(chunks):
        if c == chunks - 1:
            load_coefficients(X)
        load_field(c)
    load_coefficients(Y)

    halo_r[...] = jnp.zeros_like(halo_r)
    barrier = pltpu.get_barrier_semaphore()
    for axis in (X, Y):
        for other in others(axis):
            pl.semaphore_signal(barrier, 1, device_id=device(axis, other), device_id_type=LOGICAL)

    blank = jnp.zeros((SUB, LANES), F32)
    every = tuple(range(tiles))
    cells = [(c, t) for c in range(chunks) for t in range(tiles)]

    def slab(k):
        return pl.ds((k + 1) * PITCH, SUB)

    def each_chunk(body):
        lax.fori_loop(0, chunks, lambda c, carry: (body(c), carry)[1], 0)

    def turn(src, dst, c, axis, to, base, many, lts, ends=None, step_in=PITCH, step_out=PITCH, correct=True, explicit=False, scale=None,
             g_ss=0):
        group = 2

        def column(g, carry):
            fs = [g * group + u for u in range(group)]
            for kt in every:
                heads, tails = [None] * group, [None] * group
                for lt in lts:
                    rows = pl.ds(kt * (LANES * pitch) + (axis * tiles + lt), LANES, stride=pitch)
                    if correct:
                        near, far = w2[rows, :], v2[rows, :]
                    if explicit:
                        own, low, high = 2.0 - pb[rows, :], pa[rows, :], pc[rows, :]
                    if ends:
                        rows = pl.ds(lt * LANES * pitch + to * tiles + kt, LANES, stride=pitch)
                        first_row, last_row = r0[rows, :], rn[rows, :]
                    for u, f in enumerate(fs):
                        origin = kt * LANES * step_in + (step_in if step_in == PITCH else 0) + base + f
                        target = lt * LANES * step_out + (step_out if step_out == PITCH else 0) + base + f
                        block = src[c, lt, pl.ds(origin, LANES, stride=step_in), :]
                        if explicit:
                            block = own * block - (low * src[c, lt, pl.ds(origin - step_in, LANES, stride=step_in), :]
                                                   + high * src[c, lt, pl.ds(origin + step_in, LANES, stride=step_in), :])
                        if correct:
                            block = block + near * ss[g_ss, 0, lt, pl.ds(f, 1), :] + far * ss[g_ss, 1, lt, pl.ds(f, 1), :]
                        if scale is not None:
                            block = block * scale
                        flipped = block.T
                        dst[c, kt, pl.ds(target, LANES, stride=step_out), :] = flipped
                        if ends:
                            fold = lambda v: v.reshape(LANES // SUB, SUB, LANES).sum(axis=0)
                            h, s = fold(flipped * first_row), fold(flipped * last_row)
                            heads[u] = h if heads[u] is None else heads[u] + h
                            tails[u] = s if tails[u] is None else tails[u] + s
                if ends:
                    for u, f in enumerate(fs):
                        ends[0][kt, pl.ds(f, 1), :] = jnp.sum(heads[u], axis=0, keepdims=True)
                        ends[1][kt, pl.ds(f, 1), :] = jnp.sum(tails[u], axis=0, keepdims=True)
            return carry

        lax.fori_loop(0, many // group, column, 0, unroll=True)

    me_y = pos[Y]
    has_before, has_after = me_y > 0, me_y < parts_y - 1

    def halo(side, c, other):
        return pltpu.make_async_remote_copy(
            src_ref=halo_s.at[side, c], dst_ref=halo_r.at[1 - side, c], send_sem=send_sem.at[side, c, 0], recv_sem=recv_y.at[1, c, 1 - side],
            device_id=device(Y, other), device_id_type=LOGICAL)

    def send_halo(c):
        for t in every:
            halo_s[0, c, t] = qs[c, t, slab(0), :]
            halo_s[1, c, t] = qs[c, t, slab(n - 1), :]

        @pl.when(has_before)
        def _():
            halo(0, c, me_y - 1).start()

        @pl.when(has_after)
        def _():
            halo(1, c, me_y + 1).start()

    def await_halo(c):
        @pl.when(has_before)
        def _():
            halo(0, c, me_y - 1).wait_send()
            halo(1, c, me_y - 1).wait_recv()

        @pl.when(has_after)
        def _():
            halo(1, c, me_y + 1).wait_send()
            halo(0, c, me_y + 1).wait_recv()

        for t in every:
            qs[c, t, slab(-1), :] = halo_r[0, c, t]
            qs[c, t, slab(n), :] = halo_r[1, c, t]

    def pack_x():
        some = nat.at[pl.ds(0, 3)]
        pltpu.make_async_copy(some, some, load_sem).wait()
        for t in range(tiles):
            cols = pl.ds(t * LANES, LANES)
            pa[pl.ds(t, n, stride=pitch), :] = nat[0, :, cols]
            pb[pl.ds(t, n, stride=pitch), :] = nat[1, :, cols] + 1.0
            pc[pl.ds(t, n, stride=pitch), :] = nat[2, :, cols]

    for c in range(chunks):
        if c == chunks - 1:
            pack_x()
        for t in range(tiles):
            field_piece(c, t).wait()
            turn(out, qs, c, X, Y, 0, SUB, (t,), step_in=SUB, correct=False)
        if c == 0:
            pl.semaphore_wait(barrier, parts_x + parts_y - 2)
        send_halo(c)
    some = nat.at[pl.ds(3, 3)]
    pltpu.make_async_copy(some, some, late_sem).wait()
    for t in range(tiles):
        cols = pl.ds(t * LANES, LANES)
        for s in range(tiles):
            rows = pl.ds(s * LANES, LANES)
            dest = pl.ds(t * LANES * pitch + tiles + s, LANES, stride=pitch)
            pa[dest, :] = nat[3, rows, cols].T
            pb[dest, :] = nat[4, rows, cols].T + 1.0
            pc[dest, :] = nat[5, rows, cols].T

    long, deep = 16, 16
    zero = jnp.zeros((pitch, LANES), F32)
    one = jnp.ones((pitch, LANES), F32)

    def at_row(k, u):
        return pl.ds(pl.multiple_of(k * (long * pitch), long * pitch) + u * pitch, pitch)

    def pivots(g, state):
        dp, dq, c_prev, ep, eq, a_next = state
        h = n // long - 1 - g
        for u in range(0, long, 2):
            up, next_up = at_row(g, u), at_row(g, u + 1)
            b, t = pb[up, :], pa[up, :] * c_prev
            next_b, next_t = pb[next_up, :], pa[next_up, :] * pc[up, :]
            new = b * dp - t * dq
            newer = (next_b * b - next_t) * dp - (next_b * t) * dq
            nd[up, :], md[up, :], nd[next_up, :], md[next_up, :] = dp, new, new, newer
            dp, dq, c_prev = newer, new, pc[next_up, :]
            down, next_down = at_row(h, long - 1 - u), at_row(h, long - 2 - u)
            b, t = pb[down, :], a_next * pc[down, :]
            next_b, next_t = pb[next_down, :], pa[down, :] * pc[next_down, :]
            new = b * ep - t * eq
            newer = (next_b * b - next_t) * ep - (next_b * t) * eq
            ne[down, :], me_[down, :], ne[next_down, :], me_[next_down, :] = ep, new, new, newer
            ep, eq, a_next = newer, new, pa[next_down, :]
            if u % 8 == 2:
                scale_d, scale_e = 1.0 / dp, 1.0 / ep
            if u % 8 == 6:
                dp, dq, ep, eq = dp * scale_d, dq * scale_d, ep * scale_e, eq * scale_e
        return dp, dq, c_prev, ep, eq, a_next

    lax.fori_loop(0, n // long, pivots, (one, zero, zero, one, zero, zero))

    low_half = lax.broadcasted_iota(jnp.int32, (SUB, LANES), 0) < pitch
    blocks = n * pitch // SUB
    step_rows = 8

    def ratios(g, state):
        prev_m, next_d = state
        for u in range(step_rows):
            up = pl.ds(pl.multiple_of(g * (SUB * step_rows), SUB * step_rows) + u * SUB, SUB)
            down = pl.ds(pl.multiple_of((blocks // step_rows - 1 - g) * (SUB * step_rows), SUB * step_rows)
                         + (step_rows - 1 - u) * SUB, SUB)
            minv = nd[up, :] / md[up, :]
            m2[up, :] = minv + minv
            cn[up, :] = -pc[up, :] * minv
            turned = pltpu.roll(minv, pitch, 0)
            ln[up, :] = -pa[up, :] * jnp.where(low_half, prev_m, turned)
            prev_m = turned
            dinv = ne[down, :] / me_[down, :]
            d2[down, :] = dinv + dinv
            an[down, :] = -pa[down, :] * dinv
            turned = pltpu.roll(dinv, pitch, 0)
            un[down, :] = -pc[down, :] * jnp.where(low_half, turned, next_d)
            next_d = turned
        return prev_m, next_d

    lax.fori_loop(0, blocks // step_rows, ratios, (blank, blank))

    first, last = pl.ds(0, pitch), pl.ds((n - 1) * pitch, pitch)

    def products(g, state):
        col0, row0, coln, rown, un_prev, ln_next = state
        h = n // long - 1 - g
        for u in range(long):
            up, down = at_row(g, u), at_row(h, long - 1 - u)
            start = jnp.logical_and(g == 0, u == 0) if u == 0 else None
            f0, f1 = an[up, :], un_prev
            b0, b1 = cn[down, :], ln_next
            if u == 0:
                f0, f1 = jnp.where(start, one, f0), jnp.where(start, one, f1)
                b0, b1 = jnp.where(start, one, b0), jnp.where(start, one, b1)
            col0, row0, coln, rown = col0 * f0, row0 * f1, coln * b0, rown * b1
            w2[up, :], r0[up, :], v2[down, :], rn[down, :] = col0, row0, coln, rown
            un_prev, ln_next = un[up, :], ln[down, :]
        return col0, row0, coln, rown, un_prev, ln_next

    d_first, m_last = 0.5 * d2[first, :], 0.5 * m2[last, :]
    lax.fori_loop(0, n // long, products,
                  (-pa[first, :] * d2[first, :], d_first, -pc[last, :] * m2[last, :], m_last, one, one))

    def block_ends(axis):
        for q, (ref, line) in enumerate(((w2, 0), (w2, n - 1), (v2, 0), (v2, n - 1))):
            yield q * tiles, -0.5 * ref[pl.ds(line * pitch + axis * tiles, tiles), :]

    for row, values in block_ends(X):
        for t in every:
            raw[0, 0, pos[X], 2 * tiles + (row + t) // UNIT, pl.ds((row + t) % UNIT, 1), :] = values[t:t + 1]

    def spread_y():
        for row, values in block_ends(Y):
            gs[pl.ds(row, tiles), :] = values
        gc[pos[Y]] = gs[...]
        for other in others(Y):
            pltpu.make_async_remote_copy(
                src_ref=gs, dst_ref=gc.at[pos[Y]], send_sem=load_sem, recv_sem=gather_sem,
                device_id=device(Y, other), device_id_type=LOGICAL).start()

    def reduce_lines(axis):
        count, me = parts[axis], pos[axis]
        if axis == Y:
            arrived = gc.at[pl.ds(0, count - 1)]
            pltpu.make_async_copy(arrived, arrived, gather_sem).wait()
            pltpu.make_async_copy(arrived, arrived, load_sem).wait()
            part = lambda p, q: gc[p, pl.ds(q * tiles, tiles), :]
        else:
            part = lambda p, q: raw[0, 0, p, 2 * tiles + q * tiles // UNIT, pl.ds(q * tiles % UNIT, tiles), :]
        nil = jnp.zeros((tiles, LANES), F32)
        unit = jnp.ones((tiles, LANES), F32)
        mu, rho, tau = [None] * count, [None] * count, [None] * count
        prev = nil
        for p in range(count):
            wf, wt, vf, vt = (part(p, q) for q in range(4))
            kappa = 1.0 / (1.0 - wf * prev)
            mu[p], rho[p] = wt * prev * kappa, wt * kappa
            prev = tau[p] = vt + mu[p] * vf
        nu, omega, sigma = [None] * count, [None] * count, [None] * count
        prev = nil
        for p in reversed(range(count)):
            wf, wt, vf, vt = (part(p, q) for q in range(4))
            kappa = 1.0 / (1.0 - vt * prev)
            nu[p], omega[p] = vf * prev * kappa, vf * kappa
            prev = sigma[p] = wf + nu[p] * wt
        pick = lambda values, at: sum(jnp.where(at == p, v, nil) for p, v in enumerate(values))
        tau_b, sigma_a = pick(tau, me - 1), pick(sigma, me + 1)
        mu_me, nu_me = pick(mu, me), pick(nu, me)
        wf, wt, vf, vt = (part(me, q) for q in range(4))
        det = 1.0 / ((1.0 - tau_b * wf) * (1.0 - sigma_a * vt) - (tau_b * vf) * (sigma_a * wt))
        k11, k12 = (1.0 - sigma_a * vt) * det, tau_b * vf * det
        k21, k22 = sigma_a * wt * det, (1.0 - tau_b * wf) * det
        low, high = [None] * count, [None] * count
        for p in reversed(range(count)):
            onward = -rho[p + 1] * low[p + 1] if p + 1 < count else nil
            low[p] = jnp.where(me - 1 == p, unit, jnp.where(p < me - 1, onward, nil))
        for p in range(count):
            onward = -omega[p - 1] * high[p - 1] if p else nil
            high[p] = jnp.where(me + 1 == p, unit, jnp.where(p > me + 1, onward, nil))
        table = reduced[axis]
        put = lambda index, value: table.__setitem__((pl.ds(index * tiles, tiles), slice(None)), value)
        for p in range(count):
            put(p, k11 * low[p] + k12 * high[p] + jnp.where(me == p, -k11 * tau_b, nil))
            put(count + 1 + p, k21 * low[p] + k22 * high[p] + jnp.where(me == p, -k21 * tau_b, nil))
        put(count, -k12 * sigma_a)
        put(2 * count + 1, -k22 * sigma_a)
        put(2 * count + 2, mu_me)
        put(2 * count + 3, nu_me)
        if axis == X:
            for p in range(count):
                put(2 * count + 4 + p, jnp.where(p < me, mu[p], unit))
                put(3 * count + 4 + p, jnp.where(p < me, unit, jnp.where(p > me, nu[p], nil)))

    def publish(axis, stage, c, g):
        count, table, way = parts[axis], reduced[axis], lax.rem(stage, 2)
        for t in every:
            head, tail = exch[axis][way, c, g, pos[axis], t], gt[c, g, t]
            mu = table[pl.ds((2 * count + 2) * tiles + t, 1), :]
            nu = table[pl.ds((2 * count + 3) * tiles + t, 1), :]
            send[axis][c, g, 1, t] = tail + mu * head
            send[axis][c, g, 0, t] = head + nu * tail
        for other in others(axis):
            sel = jnp.where(other > pos[axis], 1, 0)
            pltpu.make_async_remote_copy(
                src_ref=send[axis].at[c, g, sel], dst_ref=exch[axis].at[way, c, g, pos[axis]],
                send_sem=send_sem.at[axis, c, g], recv_sem=recv[axis].at[way, c, g],
                device_id=device(axis, other), device_id_type=LOGICAL).start()

    def combine(axis, way, c, g, g_ss=0):
        count, table = parts[axis], reduced[axis]
        for t in every:
            for side in range(2):
                base = side * (count + 1) * tiles + t
                total = table[pl.ds(base + count * tiles, 1), :] * gt[c, g, t]
                for p in range(count):
                    total = total + table[pl.ds(base + p * tiles, 1), :] * exch[axis][way, c, g, p, t]
                ss[g_ss, side, t] = total

    def neighbours(axis, stage, c, g, g_ss=0):
        way = lax.rem(stage, 2)
        arrived = exch[axis].at[way, c, g, pl.ds(0, parts[axis] - 1)]
        pltpu.make_async_copy(arrived, arrived, recv[axis].at[way, c, g]).wait()
        pltpu.make_async_copy(arrived, arrived, send_sem.at[axis, c, g]).wait()
        combine(axis, way, c, g, g_ss)

    def publish_raw(c, g):
        for t in every:
            raw[c, g, pos[X], t] = exch[X][0, c, g, pos[X], t]
            raw[c, g, pos[X], tiles + t] = gt[c, g, t]

        def send_raw(c, g, some):
            for other in others(X):
                pltpu.make_async_remote_copy(
                    src_ref=raw.at[c, g, pos[X], some], dst_ref=raw.at[c, g, pos[X], some],
                    send_sem=send_sem.at[X, c, g], recv_sem=recv_x.at[0, c, g], device_id=device(X, other), device_id_type=LOGICAL).start()

        @pl.when((c == 0) & (g == 0))
        def _():
            send_raw(0, 0, pl.ds(0, raw.shape[3]))

        @pl.when((c > 0) | (g > 0))
        def _():
            send_raw(c, g, pl.ds(0, 2 * tiles))

    def await_raw(c, g, blocks):
        arrived = raw.at[c, g, pl.ds(0, parts_x - 1), pl.ds(0, blocks)]
        pltpu.make_async_copy(arrived, arrived, recv_x.at[0, c, g]).wait()
        pltpu.make_async_copy(arrived, arrived, send_sem.at[X, c, g]).wait()

    def neighbours_raw(c, g):
        count = parts_x
        for t in every:
            for p in range(count):
                on_head = red_x[pl.ds((2 * count + 4 + p) * tiles + t, 1), :]
                on_tail = red_x[pl.ds((3 * count + 4 + p) * tiles + t, 1), :]
                exch[X][0, c, g, p, t] = on_head * raw[c, g, p, t] + on_tail * raw[c, g, p, tiles + t]
        combine(X, 0, c, g)

    def solve_block(axis, minus):
        def coef(array, k, t):
            return array[pl.ds(k * pitch + axis * tiles + t, 1), :]

        def walk(first, sign, count, visit, state):
            def block(g, state):
                line = first + sign * deep * g
                row, coef_row = (line + 1) * PITCH, line * pitch + axis * tiles

                def one(u, state):
                    at = lambda array, t: array[pl.ds(coef_row + t + u * (sign * pitch), 1), :]
                    return visit(pl.ds(row + u * (sign * PITCH), SUB), at, state)

                return lax.fori_loop(0, min(count, deep), one, state, unroll=True)

            return lax.fori_loop(0, max(count // deep, 1), block, state)

        def eliminate(mult):
            def visit(here, at, state):
                values = list(state)
                for t in every:
                    factor = at(mult, t)
                    for c in range(chunks):
                        s = c * tiles + t
                        values[s] = rs[c, t, here, :] + factor * values[s]
                        hs[c, t, here, :] = values[s]
                return tuple(values)
            return visit

        init = tuple(blank for _ in cells)
        ups = walk(0, 1, half, eliminate(ln), init)
        downs = walk(n - 1, -1, half, eliminate(un), init)
        lo, hi = half - 1, half

        def place(c, t, here, value):
            qs[c, t, here, :] = value - rs[c, t, here, :] if minus else value

        low_s, high_s = [], []
        for s, (c, t) in enumerate(cells):
            c_lo, a_hi = coef(cn, lo, t), coef(an, hi, t)
            kappa = 1.0 / (1.0 - c_lo * a_hi)
            h_hi = coef(d2, hi, t) * downs[s]
            s_lo = kappa * (coef(m2, lo, t) * ups[s] + c_lo * h_hi)
            low_s.append(s_lo)
            high_s.append(h_hi + a_hi * s_lo)
            place(c, t, slab(lo), low_s[s])
            place(c, t, slab(hi), high_s[s])

        def substitute(scale, mult):
            def visit(here, at, state):
                values = list(state)
                for t in every:
                    own, factor = at(scale, t), at(mult, t)
                    for c in range(chunks):
                        s = c * tiles + t
                        values[s] = own * hs[c, t, here, :] + factor * values[s]
                        place(c, t, here, values[s])
                return tuple(values)
            return visit

        for first, sign, visit, state in ((lo, -1, substitute(m2, cn), low_s), (hi, 1, substitute(d2, an), high_s)):
            state = walk(first + sign, sign, deep - 1, visit, tuple(state))
            walk(first + sign * deep, sign, half - deep, visit, state)

    def each_unit(body, count=units):
        lax.fori_loop(0, count, lambda u, carry: (body(u // parts_of, lax.rem(u, parts_of)), carry)[1], 0)

    def ends_of(axis, stage, c, g):
        return exch[axis].at[lax.rem(stage, 2), c, g, pos[axis]], gt.at[c, g]

    def start_x(c):
        def unit(g, carry):
            turn(qs, rs, c, Y, X, g * UNIT, UNIT, every, ends_of(X, 0, c, g), correct=False, explicit=True)
            publish_raw(c, g)

            @pl.when((c == 0) & (g == 0))
            def _():
                spread_y()

            return carry

        await_halo(c)
        lax.fori_loop(0, parts_of, unit, 0)

    def onward(axis, stage, to, to_stage):
        def unit(c, g):
            neighbours(axis, stage, c, g)
            turn(qs, rs, c, axis, to, g * UNIT, UNIT, every, ends_of(to, to_stage, c, g))
            publish(to, to_stage, c, g)

        each_unit(unit)

    each_chunk(start_x)
    solve_block(X, True)
    reduce_lines(Y)
    await_raw(0, 0, raw.shape[3])
    reduce_lines(X)

    def first_to_y(c, g):
        @pl.when((c > 0) | (g > 0))
        def _():
            await_raw(c, g, 2 * tiles)

        neighbours_raw(c, g)
        turn(qs, rs, c, X, Y, g * UNIT, UNIT, every, ends_of(Y, 0, c, g))
        publish(Y, 0, c, g)

    each_unit(first_to_y)

    def step(stage, carry):
        solve_block(Y, True)
        onward(Y, stage - 1, X, stage)
        solve_block(X, True)
        onward(X, stage, Y, stage)
        return carry

    lax.fori_loop(1, STEPS, step, 0)
    solve_block(Y, False)

    def finish(c, g):
        neighbours(Y, STEPS - 1, c, g)
        turn(qs, out, c, Y, X, g * UNIT, UNIT, every, scale=0.5, step_out=SUB)

    each_unit(finish, units - parts_of)
    for g in range(parts_of):
        neighbours(Y, STEPS - 1, chunks - 1, g, g)


def finish_kernel(done, qs, w2, v2, ss, out, fresh, sem):
    last, tiles, lines = done.shape[0] - 1, done.shape[1], done.shape[2] // SUB
    pitch = 2 * tiles

    def place(c, t, src, whole=False):
        step = lines if whole else LANES
        for first in range(0, lines, step):
            copy = pltpu.make_async_copy(src.at[pl.ds(first * SUB, step * SUB)].reshape(step, SUB, LANES),
                                         out.at[pl.ds(first, step), pl.ds(c * SUB, SUB), pl.ds(t * LANES, LANES)], sem.at[c * tiles + t])
            if whole:
                copy.wait()
            else:
                copy.start()

    for c in range(last):
        for t in range(tiles):
            place(c, t, done.at[c, t])
    for kt in range(tiles):
        def column(f, carry):
            for lt in range(tiles):
                rows = pl.ds(kt * LANES * pitch + tiles + lt, LANES, stride=pitch)
                block = qs[last, lt, pl.ds((kt * LANES + 1) * PITCH + f, LANES, stride=PITCH), :]
                near, far = (ss[f // UNIT, side, lt, pl.ds(f % UNIT, 1), :] for side in range(2))
                block = block + w2[rows, :] * near + v2[rows, :] * far
                fresh[kt, pl.ds(lt * LANES * SUB + f, LANES, stride=SUB), :] = (block * 0.5).T
            return carry

        lax.fori_loop(0, SUB, column, 0, unroll=True)
        place(last, kt, fresh.at[kt])
    for c in range(last + 1):
        for t in range(tiles):
            place(c, t, done.at[c, t] if c < last else fresh.at[t], whole=True)


def solution(mesh):
    parts_x, parts_y = mesh.shape["row"], mesh.shape["col"]
    strides, stride = {}, 1
    for name in reversed(mesh.axis_names):
        strides[name], stride = stride, stride * mesh.shape[name]
    field_spec = P(("batch", "row"), "col", None)
    coeff_spec = P(("batch", "row"), "col")

    def local_steps(field, *coeffs):
        n, fields = field.shape[0], field.shape[2]
        tiles, chunks = n // LANES, fields // SUB
        packed = pltpu.VMEM((n * 2 * tiles, LANES), F32)
        plane = -(-((n + 2) * PITCH - SUB) // (4 * SUB)) * 4 * SUB + SUB
        big = pltpu.VMEM((chunks, tiles, plane, LANES), F32)
        dma = pltpu.SemaphoreType.DMA
        parts_of = SUB // UNIT
        sends = pltpu.VMEM((chunks, parts_of, 2, tiles, UNIT, LANES), F32)
        line = lambda count: pltpu.VMEM((2, chunks, parts_of, count, tiles, UNIT, LANES), F32)
        table = lambda count: pltpu.VMEM(((4 * count + 4) * tiles, LANES), F32)
        small = pltpu.VMEM((2, chunks, tiles, SUB, LANES), F32)
        message = (4 * tiles, LANES)
        scratch = [
            pltpu.VMEM((6, n, n), F32), big, big, *([packed] * 15),
            pltpu.VMEM(message, F32), pltpu.VMEM((parts_y,) + message, F32),
            table(parts_x), table(parts_y), sends, sends, line(parts_x), line(parts_y),
            pltpu.VMEM((chunks, parts_of, parts_x, 2 * tiles + 4 * tiles // UNIT, UNIT, LANES), F32), pltpu.VMEM((chunks, parts_of, tiles, UNIT, LANES), F32),
            small, small, dma, dma, dma((2, chunks, parts_of)), dma((2, chunks, parts_of)), dma((2, chunks, parts_of)), dma,
        ]
        in_hbm = pl.BlockSpec(memory_space=pltpu.HBM)
        turned = jnp.transpose(field, (0, 2, 1))
        in_vmem = pl.BlockSpec(memory_space=pltpu.VMEM)
        shape = lambda *dims: jax.ShapeDtypeStruct(dims, F32)
        handed = (shape(chunks, tiles, n * SUB, LANES), shape(chunks, tiles, plane, LANES), shape(n * 2 * tiles, LANES),
                  shape(n * 2 * tiles, LANES), shape(parts_of, 2, tiles, UNIT, LANES))
        handed = pl.pallas_call(
            functools.partial(adi_kernel, (("row", parts_x), ("col", parts_y)), strides),
            out_shape=handed, in_specs=[in_hbm] * 7, out_specs=(in_vmem,) * len(handed), scratch_shapes=scratch,
            compiler_params=pltpu.CompilerParams(collective_id=0, has_side_effects=True, vmem_limit_bytes=36 * 1024 * 1024),
            name="adi_steps",
        )(*(pltpu.with_memory_space_constraint(array, pltpu.HBM) for array in (turned,) + coeffs))
        result = pl.pallas_call(
            finish_kernel, out_shape=jax.ShapeDtypeStruct(turned.shape, F32),
            in_specs=[in_vmem] * len(handed), out_specs=in_hbm,
            scratch_shapes=[pltpu.VMEM((tiles, n * SUB, LANES), F32), dma((chunks * tiles,))],
            compiler_params=pltpu.CompilerParams(vmem_limit_bytes=8 * 1024 * 1024), name="finish",
        )(*handed)
        return jnp.transpose(result, (0, 2, 1))

    return jax.shard_map(local_steps, mesh=mesh, in_specs=(field_spec,) + (coeff_spec,) * 6, out_specs=field_spec, check_vma=False)
```

```python
import functools

import jax
import jax.numpy as jnp
from jax import lax
from jax.experimental import pallas as pl
from jax.experimental.pallas import tpu as pltpu
from jax.sharding import PartitionSpec as P

STEPS = 3
F32 = jnp.float32
LANES = 128
SUB = 8
UNIT = SUB // 2
PITCH = SUB + 1
LOGICAL = pl.DeviceIdType.LOGICAL
X, Y = 0, 1


def adi_kernel(axes, strides, field, lower_x, diag_x, upper_x, lower_y, diag_y, upper_y, out, qs, w2, v2, ss,
               nat, rs, hs, pa, pb, pc, nd, md, ne, me_, ln, cn, un, an, m2, d2, r0, rn,
               gs, gc, red_x, red_y, sx, sy, ex, ey, raw, gt, halo_s, halo_r,
               load_sem, late_sem, send_sem, recv_x, recv_y, gather_sem):
    (row_name, parts_x), (col_name, parts_y) = axes
    n = lower_x.shape[0]
    tiles = n // LANES
    chunks = field.shape[1] // SUB
    parts_of = SUB // UNIT
    units = chunks * parts_of
    pitch = 2 * tiles
    half = n // 2
    pos = (lax.axis_index(row_name), lax.axis_index(col_name))
    parts = (parts_x, parts_y)
    home = sum(lax.axis_index(name) * stride for name, stride in strides.items())
    exch = (ex, ey)
    recv = (recv_x, recv_y)
    send = (sx, sy)
    reduced = (red_x, red_y)

    def device(axis, other):
        return home + (other - pos[axis]) * strides[(row_name, col_name)[axis]]

    def others(axis):
        count = parts[axis]
        offs = sorted(range(1, count), key=lambda off: -min(off, count - off))
        return [lax.rem(pos[axis] + off, count) for off in offs]

    def field_piece(c, t, first=0, count=n):
        late = c == chunks - 1 and t == tiles - 1 and first > 0
        return pltpu.make_async_copy(field.at[pl.ds(first, count), pl.ds(c * SUB, SUB), pl.ds(t * LANES, LANES)],
                                     out.at[c, t, pl.ds(first * SUB, count * SUB)].reshape(count, SUB, LANES), recv_x.at[1, 0, 0] if late else send_sem.at[t, c, 0])

    def load_field(c):
        for t in range(tiles):
            for first in range(0, n, LANES):
                field_piece(c, t, first, LANES).start()

    def load_coefficients(axis):
        for slot, ref in enumerate(((lower_x, diag_x, upper_x), (lower_y, diag_y, upper_y))[axis]):
            pltpu.make_async_copy(ref, nat.at[3 * axis + slot], (load_sem, late_sem)[axis]).start()

    for c in range(chunks):
        if c == chunks - 1:
            load_coefficients(X)
        load_field(c)
    load_coefficients(Y)

    halo_r[...] = jnp.zeros_like(halo_r)
    barrier = pltpu.get_barrier_semaphore()
    for axis in (X, Y):
        for other in others(axis):
            pl.semaphore_signal(barrier, 1, device_id=device(axis, other), device_id_type=LOGICAL)

    blank = jnp.zeros((SUB, LANES), F32)
    every = tuple(range(tiles))
    cells = [(c, t) for c in range(chunks) for t in range(tiles)]

    def slab(k):
        return pl.ds((k + 1) * PITCH, SUB)

    def each_chunk(body):
        lax.fori_loop(0, chunks, lambda c, carry: (body(c), carry)[1], 0)

    def turn(src, dst, c, axis, to, base, many, lts, ends=None, kts=None, step_in=PITCH, step_out=PITCH, correct=True, explicit=False, scale=None,
             g_ss=0):
        group = 2

        def column(g, carry):
            fs = [g * group + u for u in range(group)]
            for kt in kts or every:
                heads, tails = [None] * group, [None] * group
                for lt in lts:
                    rows = pl.ds(kt * (LANES * pitch) + (axis * tiles + lt), LANES, stride=pitch)
                    if correct:
                        near, far = w2[rows, :], v2[rows, :]
                    if explicit:
                        own, low, high = 2.0 - pb[rows, :], pa[rows, :], pc[rows, :]
                    if ends:
                        rows = pl.ds(lt * LANES * pitch + to * tiles + kt, LANES, stride=pitch)
                        first_row, last_row = r0[rows, :], rn[rows, :]
                    for u, f in enumerate(fs):
                        origin = kt * LANES * step_in + (step_in if step_in == PITCH else 0) + base + f
                        target = lt * LANES * step_out + (step_out if step_out == PITCH else 0) + base + f
                        block = src[c, lt, pl.ds(origin, LANES, stride=step_in), :]
                        if explicit:
                            block = own * block - (low * src[c, lt, pl.ds(origin - step_in, LANES, stride=step_in), :]
                                                   + high * src[c, lt, pl.ds(origin + step_in, LANES, stride=step_in), :])
                        if correct:
                            block = block + near * ss[g_ss, 0, pl.ds(lt * UNIT + f, 1), :] + far * ss[g_ss, 1, pl.ds(lt * UNIT + f, 1), :]
                        if scale is not None:
                            block = block * scale
                        flipped = block.T
                        dst[c, kt, pl.ds(target, LANES, stride=step_out), :] = flipped
                        if ends:
                            fold = lambda v: v.reshape(LANES // SUB, SUB, LANES).sum(axis=0)
                            h, s = fold(flipped * first_row), fold(flipped * last_row)
                            heads[u] = h if heads[u] is None else heads[u] + h
                            tails[u] = s if tails[u] is None else tails[u] + s
                if ends:
                    for u, f in enumerate(fs):
                        ends[0][pl.ds(kt * UNIT + f, 1), :] = jnp.sum(heads[u], axis=0, keepdims=True)
                        ends[1][pl.ds(kt * UNIT + f, 1), :] = jnp.sum(tails[u], axis=0, keepdims=True)
            return carry

        lax.fori_loop(0, many // group, column, 0, unroll=True)

    me_y = pos[Y]
    has_before, has_after = me_y > 0, me_y < parts_y - 1

    def halo(side, c, other):
        return pltpu.make_async_remote_copy(
            src_ref=halo_s.at[side, c], dst_ref=halo_r.at[1 - side, c], send_sem=send_sem.at[side, c, 0], recv_sem=recv_y.at[1, c, 1 - side],
            device_id=device(Y, other), device_id_type=LOGICAL)

    def send_halo(c):
        for t in every:
            halo_s[0, c, t] = qs[c, t, slab(0), :]
            halo_s[1, c, t] = qs[c, t, slab(n - 1), :]

        @pl.when(has_before)
        def _():
            halo(0, c, me_y - 1).start()

        @pl.when(has_after)
        def _():
            halo(1, c, me_y + 1).start()

    def await_halo(c):
        @pl.when(has_before)
        def _():
            halo(0, c, me_y - 1).wait_send()
            halo(1, c, me_y - 1).wait_recv()

        @pl.when(has_after)
        def _():
            halo(1, c, me_y + 1).wait_send()
            halo(0, c, me_y + 1).wait_recv()

        for t in every:
            qs[c, t, slab(-1), :] = halo_r[0, c, t]
            qs[c, t, slab(n), :] = halo_r[1, c, t]

    def pack_x():
        some = nat.at[pl.ds(0, 3)]
        pltpu.make_async_copy(some, some, load_sem).wait()
        for t in range(tiles):
            cols = pl.ds(t * LANES, LANES)
            pa[pl.ds(t, n, stride=pitch), :] = nat[0, :, cols]
            pb[pl.ds(t, n, stride=pitch), :] = nat[1, :, cols] + 1.0
            pc[pl.ds(t, n, stride=pitch), :] = nat[2, :, cols]

    for c in range(chunks):
        if c == chunks - 1:
            pack_x()
        for t in range(tiles):
            if c < chunks - 1 or t < tiles - 1:
                field_piece(c, t).wait()
                turn(out, qs, c, X, Y, 0, SUB, (t,), step_in=SUB, correct=False)
            else:
                for kt in every:
                    field_piece(c, t, kt * LANES, LANES).wait()
                    turn(out, qs, c, X, Y, 0, SUB, (t,), kts=(kt,), step_in=SUB, correct=False)
        if c == 0:
            pl.semaphore_wait(barrier, parts_x + parts_y - 2)
        send_halo(c)
    some = nat.at[pl.ds(3, 3)]
    pltpu.make_async_copy(some, some, late_sem).wait()
    for t in range(tiles):
        cols = pl.ds(t * LANES, LANES)
        for s in range(tiles):
            rows = pl.ds(s * LANES, LANES)
            dest = pl.ds(t * LANES * pitch + tiles + s, LANES, stride=pitch)
            pa[dest, :] = nat[3, rows, cols].T
            pb[dest, :] = nat[4, rows, cols].T + 1.0
            pc[dest, :] = nat[5, rows, cols].T

    long, deep = 16, 16
    zero = jnp.zeros((pitch, LANES), F32)
    one = jnp.ones((pitch, LANES), F32)

    def at_row(k, u):
        return pl.ds(pl.multiple_of(k * (long * pitch), long * pitch) + u * pitch, pitch)

    def pivots(g, state):
        dp, dq, c_prev, ep, eq, a_next = state
        h = n // long - 1 - g
        for u in range(0, long, 2):
            up, next_up = at_row(g, u), at_row(g, u + 1)
            b, t = pb[up, :], pa[up, :] * c_prev
            next_b, next_t = pb[next_up, :], pa[next_up, :] * pc[up, :]
            new = b * dp - t * dq
            newer = (next_b * b - next_t) * dp - (next_b * t) * dq
            nd[up, :], md[up, :], nd[next_up, :], md[next_up, :] = dp, new, new, newer
            dp, dq, c_prev = newer, new, pc[next_up, :]
            down, next_down = at_row(h, long - 1 - u), at_row(h, long - 2 - u)
            b, t = pb[down, :], a_next * pc[down, :]
            next_b, next_t = pb[next_down, :], pa[down, :] * pc[next_down, :]
            new = b * ep - t * eq
            newer = (next_b * b - next_t) * ep - (next_b * t) * eq
            ne[down, :], me_[down, :], ne[next_down, :], me_[next_down, :] = ep, new, new, newer
            ep, eq, a_next = newer, new, pa[next_down, :]
            if u % 8 == 2:
                scale_d, scale_e = 1.0 / dp, 1.0 / ep
            if u % 8 == 6:
                dp, dq, ep, eq = dp * scale_d, dq * scale_d, ep * scale_e, eq * scale_e
        return dp, dq, c_prev, ep, eq, a_next


    low_half = lax.broadcasted_iota(jnp.int32, (SUB, LANES), 0) < pitch
    blocks = n * pitch // SUB
    step_rows = long * pitch // SUB

    def ratios(g, state):
        prev_m, next_d = state
        for u in range(step_rows):
            up = pl.ds(pl.multiple_of(g * (SUB * step_rows), SUB * step_rows) + u * SUB, SUB)
            down = pl.ds(pl.multiple_of((blocks // step_rows - 1 - g) * (SUB * step_rows), SUB * step_rows)
                         + (step_rows - 1 - u) * SUB, SUB)
            minv = nd[up, :] / md[up, :]
            m2[up, :] = minv + minv
            cn[up, :] = -pc[up, :] * minv
            turned = pltpu.roll(minv, pitch, 0)
            ln[up, :] = -pa[up, :] * jnp.where(low_half, prev_m, turned)
            prev_m = turned
            dinv = ne[down, :] / me_[down, :]
            d2[down, :] = dinv + dinv
            an[down, :] = -pa[down, :] * dinv
            turned = pltpu.roll(dinv, pitch, 0)
            un[down, :] = -pc[down, :] * jnp.where(low_half, turned, next_d)
            next_d = turned
        return prev_m, next_d

    stretches = n // long
    state = lax.fori_loop(1, stretches, lambda g, state: (lambda later: (pivots(g, state[0]), later))(ratios(g - 1, state[1])),
                          (pivots(0, (one, zero, zero, one, zero, zero)), (blank, blank)))
    ratios(stretches - 1, state[1])

    first, last = pl.ds(0, pitch), pl.ds((n - 1) * pitch, pitch)

    def products(g, state):
        col0, row0, coln, rown, un_prev, ln_next = state
        h = n // long - 1 - g
        for u in range(long):
            up, down = at_row(g, u), at_row(h, long - 1 - u)
            start = jnp.logical_and(g == 0, u == 0) if u == 0 else None
            f0, f1 = an[up, :], un_prev
            b0, b1 = cn[down, :], ln_next
            if u == 0:
                f0, f1 = jnp.where(start, one, f0), jnp.where(start, one, f1)
                b0, b1 = jnp.where(start, one, b0), jnp.where(start, one, b1)
            col0, row0, coln, rown = col0 * f0, row0 * f1, coln * b0, rown * b1
            w2[up, :], r0[up, :], v2[down, :], rn[down, :] = col0, row0, coln, rown
            un_prev, ln_next = un[up, :], ln[down, :]
        return col0, row0, coln, rown, un_prev, ln_next

    d_first, m_last = 0.5 * d2[first, :], 0.5 * m2[last, :]
    lax.fori_loop(0, n // long, products,
                  (-pa[first, :] * d2[first, :], d_first, -pc[last, :] * m2[last, :], m_last, one, one))

    def block_ends(axis):
        for q, (ref, line) in enumerate(((w2, 0), (w2, n - 1), (v2, 0), (v2, n - 1))):
            yield q * tiles, -0.5 * ref[pl.ds(line * pitch + axis * tiles, tiles), :]

    for row, values in block_ends(X):
        raw[0, 0, pos[X], 2, pl.ds(row, tiles), :] = values

    def spread_y():
        for row, values in block_ends(Y):
            gs[pl.ds(row, tiles), :] = values
        gc[pos[Y]] = gs[...]
        for other in others(Y):
            pltpu.make_async_remote_copy(
                src_ref=gs, dst_ref=gc.at[pos[Y]], send_sem=load_sem, recv_sem=gather_sem,
                device_id=device(Y, other), device_id_type=LOGICAL).start()

    def reduce_lines(axis):
        count, me = parts[axis], pos[axis]
        if axis == Y:
            arrived = gc.at[pl.ds(0, count - 1)]
            pltpu.make_async_copy(arrived, arrived, gather_sem).wait()
            pltpu.make_async_copy(arrived, arrived, load_sem).wait()
            part = lambda p, q: gc[p, pl.ds(q * tiles, tiles), :]
        else:
            part = lambda p, q: raw[0, 0, p, 2, pl.ds(q * tiles, tiles), :]
        nil = jnp.zeros((tiles, LANES), F32)
        unit = jnp.ones((tiles, LANES), F32)
        mu, rho, tau = [None] * count, [None] * count, [None] * count
        prev = nil
        for p in range(count):
            wf, wt, vf, vt = (part(p, q) for q in range(4))
            kappa = 1.0 / (1.0 - wf * prev)
            mu[p], rho[p] = wt * prev * kappa, wt * kappa
            prev = tau[p] = vt + mu[p] * vf
        nu, omega, sigma = [None] * count, [None] * count, [None] * count
        prev = nil
        for p in reversed(range(count)):
            wf, wt, vf, vt = (part(p, q) for q in range(4))
            kappa = 1.0 / (1.0 - vt * prev)
            nu[p], omega[p] = vf * prev * kappa, vf * kappa
            prev = sigma[p] = wf + nu[p] * wt
        pick = lambda values, at: sum(jnp.where(at == p, v, nil) for p, v in enumerate(values))
        tau_b, sigma_a = pick(tau, me - 1), pick(sigma, me + 1)
        mu_me, nu_me = pick(mu, me), pick(nu, me)
        wf, wt, vf, vt = (part(me, q) for q in range(4))
        det = 1.0 / ((1.0 - tau_b * wf) * (1.0 - sigma_a * vt) - (tau_b * vf) * (sigma_a * wt))
        k11, k12 = (1.0 - sigma_a * vt) * det, tau_b * vf * det
        k21, k22 = sigma_a * wt * det, (1.0 - tau_b * wf) * det
        low, high = [None] * count, [None] * count
        for p in reversed(range(count)):
            onward = -rho[p + 1] * low[p + 1] if p + 1 < count else nil
            low[p] = jnp.where(me - 1 == p, unit, jnp.where(p < me - 1, onward, nil))
        for p in range(count):
            onward = -omega[p - 1] * high[p - 1] if p else nil
            high[p] = jnp.where(me + 1 == p, unit, jnp.where(p > me + 1, onward, nil))
        table = reduced[axis]

        def put(index, value):
            for t in every:
                table[index, pl.ds(t * UNIT, UNIT), :] = jnp.broadcast_to(value[t:t + 1], (UNIT, LANES))

        for p in range(count):
            put(p, k11 * low[p] + k12 * high[p] + jnp.where(me == p, -k11 * tau_b, nil))
            put(count + 1 + p, k21 * low[p] + k22 * high[p] + jnp.where(me == p, -k21 * tau_b, nil))
        put(count, -k12 * sigma_a)
        put(2 * count + 1, -k22 * sigma_a)
        put(2 * count + 2, mu_me)
        put(2 * count + 3, nu_me)
        if axis == X:
            for p in range(count):
                put(2 * count + 4 + p, jnp.where(p < me, mu[p], unit))
                put(3 * count + 4 + p, jnp.where(p < me, unit, jnp.where(p > me, nu[p], nil)))

    def publish(axis, stage, c, g):
        count, table, way = parts[axis], reduced[axis], lax.rem(stage, 2)
        head, tail = exch[axis][way, c, g, pos[axis]], gt[c, g]
        send[axis][c, g, 1] = tail + table[2 * count + 2] * head
        send[axis][c, g, 0] = head + table[2 * count + 3] * tail
        for other in others(axis):
            sel = jnp.where(other > pos[axis], 1, 0)
            pltpu.make_async_remote_copy(
                src_ref=send[axis].at[c, g, sel], dst_ref=exch[axis].at[way, c, g, pos[axis]],
                send_sem=send_sem.at[axis, c, g], recv_sem=recv[axis].at[way, c, g],
                device_id=device(axis, other), device_id_type=LOGICAL).start()

    def combine(axis, way, c, g, g_ss=0):
        count, table = parts[axis], reduced[axis]
        for side in range(2):
            base = side * (count + 1)
            terms = [table[base + count] * gt[c, g]] + [table[base + p] * exch[axis][way, c, g, p] for p in range(count)]
            while len(terms) > 1:
                terms = [a + b for a, b in zip(terms[::2], terms[1::2])] + terms[len(terms) // 2 * 2:]
            ss[g_ss, side] = terms[0]

    def neighbours(axis, stage, c, g, g_ss=0):
        way = lax.rem(stage, 2)
        arrived = exch[axis].at[way, c, g, pl.ds(0, parts[axis] - 1)]
        pltpu.make_async_copy(arrived, arrived, recv[axis].at[way, c, g]).wait()
        pltpu.make_async_copy(arrived, arrived, send_sem.at[axis, c, g]).wait()
        combine(axis, way, c, g, g_ss)

    def publish_raw(c, g):
        raw[c, g, pos[X], 0] = exch[X][0, c, g, pos[X]]
        raw[c, g, pos[X], 1] = gt[c, g]

        def send_raw(c, g, some):
            for other in others(X):
                pltpu.make_async_remote_copy(
                    src_ref=raw.at[c, g, pos[X], some], dst_ref=raw.at[c, g, pos[X], some],
                    send_sem=send_sem.at[X, c, g], recv_sem=recv_x.at[0, c, g], device_id=device(X, other), device_id_type=LOGICAL).start()

        @pl.when((c == 0) & (g == 0))
        def _():
            send_raw(0, 0, pl.ds(0, raw.shape[3]))

        @pl.when((c > 0) | (g > 0))
        def _():
            send_raw(c, g, pl.ds(0, 2))

    def await_raw(c, g, blocks):
        arrived = raw.at[c, g, pl.ds(0, parts_x - 1), pl.ds(0, blocks)]
        pltpu.make_async_copy(arrived, arrived, recv_x.at[0, c, g]).wait()
        pltpu.make_async_copy(arrived, arrived, send_sem.at[X, c, g]).wait()

    def neighbours_raw(c, g):
        count = parts_x
        for p in range(count):
            exch[X][0, c, g, p] = (red_x[2 * count + 4 + p] * raw[c, g, p, 0] + red_x[3 * count + 4 + p] * raw[c, g, p, 1])
        combine(X, 0, c, g)

    def solve_block(axis, minus):
        def coef(array, k, t):
            return array[pl.ds(k * pitch + axis * tiles + t, 1), :]

        def walk(first, sign, count, visit, state):
            def block(g, state):
                line = first + sign * deep * g
                row, coef_row = (line + 1) * PITCH, line * pitch + axis * tiles

                def one(u, state):
                    at = lambda array, t: array[pl.ds(coef_row + t + u * (sign * pitch), 1), :]
                    return visit(pl.ds(row + u * (sign * PITCH), SUB), at, state)

                return lax.fori_loop(0, min(count, deep), one, state, unroll=True)

            return lax.fori_loop(0, max(count // deep, 1), block, state)

        def eliminate(mult):
            def visit(here, at, state):
                values = list(state)
                for t in every:
                    factor = at(mult, t)
                    for c in range(chunks):
                        s = c * tiles + t
                        values[s] = rs[c, t, here, :] + factor * values[s]
                        hs[c, t, here, :] = values[s]
                return tuple(values)
            return visit

        init = tuple(blank for _ in cells)
        ups = walk(0, 1, half, eliminate(ln), init)
        downs = walk(n - 1, -1, half, eliminate(un), init)
        lo, hi = half - 1, half

        def place(c, t, here, value):
            qs[c, t, here, :] = value - rs[c, t, here, :] if minus else value

        low_s, high_s = [], []
        for s, (c, t) in enumerate(cells):
            c_lo, a_hi = coef(cn, lo, t), coef(an, hi, t)
            kappa = 1.0 / (1.0 - c_lo * a_hi)
            h_hi = coef(d2, hi, t) * downs[s]
            s_lo = kappa * (coef(m2, lo, t) * ups[s] + c_lo * h_hi)
            low_s.append(s_lo)
            high_s.append(h_hi + a_hi * s_lo)
            place(c, t, slab(lo), low_s[s])
            place(c, t, slab(hi), high_s[s])

        def substitute(scale, mult):
            def visit(here, at, state):
                values = list(state)
                for t in every:
                    own, factor = at(scale, t), at(mult, t)
                    for c in range(chunks):
                        s = c * tiles + t
                        values[s] = own * hs[c, t, here, :] + factor * values[s]
                        place(c, t, here, values[s])
                return tuple(values)
            return visit

        for first, sign, visit, state in ((lo, -1, substitute(m2, cn), low_s), (hi, 1, substitute(d2, an), high_s)):
            state = walk(first + sign, sign, deep - 1, visit, tuple(state))
            walk(first + sign * deep, sign, half - deep, visit, state)

    def each_unit(body, count=units):
        lax.fori_loop(0, count, lambda u, carry: (body(u // parts_of, lax.rem(u, parts_of)), carry)[1], 0)

    def ends_of(axis, stage, c, g):
        return exch[axis].at[lax.rem(stage, 2), c, g, pos[axis]], gt.at[c, g]

    def start_x(c):
        def unit(g, carry):
            turn(qs, rs, c, Y, X, g * UNIT, UNIT, every, ends_of(X, 0, c, g), correct=False, explicit=True)
            publish_raw(c, g)

            @pl.when((c == 0) & (g == 0))
            def _():
                spread_y()

            return carry

        await_halo(c)
        lax.fori_loop(0, parts_of, unit, 0)

    def onward(axis, stage, to, to_stage):
        def unit(c, g):
            neighbours(axis, stage, c, g)
            turn(qs, rs, c, axis, to, g * UNIT, UNIT, every, ends_of(to, to_stage, c, g))
            publish(to, to_stage, c, g)

        each_unit(unit)

    each_chunk(start_x)
    solve_block(X, True)
    reduce_lines(Y)
    await_raw(0, 0, raw.shape[3])
    reduce_lines(X)

    def first_to_y(c, g):
        @pl.when((c > 0) | (g > 0))
        def _():
            await_raw(c, g, 2)

        neighbours_raw(c, g)
        turn(qs, rs, c, X, Y, g * UNIT, UNIT, every, ends_of(Y, 0, c, g))
        publish(Y, 0, c, g)

    each_unit(first_to_y)

    def step(stage, carry):
        solve_block(Y, True)
        onward(Y, stage - 1, X, stage)
        solve_block(X, True)
        onward(X, stage, Y, stage)
        return carry

    lax.fori_loop(1, STEPS, step, 0)
    solve_block(Y, False)

    def finish(c, g):
        neighbours(Y, STEPS - 1, c, g)
        turn(qs, out, c, Y, X, g * UNIT, UNIT, every, scale=0.5, step_out=SUB)

    each_unit(finish, units - parts_of)
    for g in range(parts_of):
        neighbours(Y, STEPS - 1, chunks - 1, g, g)


def finish_kernel(done, qs, w2, v2, ss, out, fresh, sem):
    last, tiles, lines = done.shape[0] - 1, done.shape[1], done.shape[2] // SUB
    pitch = 2 * tiles

    def place(c, t, src, whole=False):
        step = lines if whole else LANES
        for first in range(0, lines, step):
            copy = pltpu.make_async_copy(src.at[pl.ds(first * SUB, step * SUB)].reshape(step, SUB, LANES),
                                         out.at[pl.ds(first, step), pl.ds(c * SUB, SUB), pl.ds(t * LANES, LANES)], sem.at[c * tiles + t])
            if whole:
                copy.wait()
            else:
                copy.start()

    for c in range(last):
        for t in range(tiles):
            place(c, t, done.at[c, t])
    for kt in range(tiles):
        def column(f, carry):
            for lt in range(tiles):
                rows = pl.ds(kt * LANES * pitch + tiles + lt, LANES, stride=pitch)
                block = qs[last, lt, pl.ds((kt * LANES + 1) * PITCH + f, LANES, stride=PITCH), :]
                near, far = (ss[f // UNIT, side, pl.ds(lt * UNIT + f % UNIT, 1), :] for side in range(2))
                block = block + w2[rows, :] * near + v2[rows, :] * far
                fresh[kt, pl.ds(lt * LANES * SUB + f, LANES, stride=SUB), :] = (block * 0.5).T
            return carry

        lax.fori_loop(0, SUB, column, 0, unroll=True)
        place(last, kt, fresh.at[kt])
    for c in range(last + 1):
        for t in range(tiles):
            place(c, t, done.at[c, t] if c < last else fresh.at[t], whole=True)


def solution(mesh):
    parts_x, parts_y = mesh.shape["row"], mesh.shape["col"]
    strides, stride = {}, 1
    for name in reversed(mesh.axis_names):
        strides[name], stride = stride, stride * mesh.shape[name]
    field_spec = P(("batch", "row"), "col", None)
    coeff_spec = P(("batch", "row"), "col")

    def local_steps(field, *coeffs):
        n, fields = field.shape[0], field.shape[2]
        tiles, chunks = n // LANES, fields // SUB
        packed = pltpu.VMEM((n * 2 * tiles, LANES), F32)
        plane = -(-((n + 2) * PITCH - SUB) // (4 * SUB)) * 4 * SUB + SUB
        big = pltpu.VMEM((chunks, tiles, plane, LANES), F32)
        dma = pltpu.SemaphoreType.DMA
        parts_of = SUB // UNIT
        sends = pltpu.VMEM((chunks, parts_of, 2, tiles * UNIT, LANES), F32)
        line = lambda count: pltpu.VMEM((2, chunks, parts_of, count, tiles * UNIT, LANES), F32)
        table = lambda count: pltpu.VMEM((4 * count + 4, tiles * UNIT, LANES), F32)
        small = pltpu.VMEM((2, chunks, tiles, SUB, LANES), F32)
        message = (4 * tiles, LANES)
        scratch = [
            pltpu.VMEM((6, n, n), F32), big, big, *([packed] * 15),
            pltpu.VMEM(message, F32), pltpu.VMEM((parts_y,) + message, F32),
            table(parts_x), table(parts_y), sends, sends, line(parts_x), line(parts_y),
            pltpu.VMEM((chunks, parts_of, parts_x, 3, tiles * UNIT, LANES), F32), pltpu.VMEM((chunks, parts_of, tiles * UNIT, LANES), F32),
            small, small, dma, dma, dma((2, chunks, parts_of)), dma((2, chunks, parts_of)), dma((2, chunks, parts_of)), dma,
        ]
        in_hbm = pl.BlockSpec(memory_space=pltpu.HBM)
        turned = jnp.transpose(field, (0, 2, 1))
        in_vmem = pl.BlockSpec(memory_space=pltpu.VMEM)
        shape = lambda *dims: jax.ShapeDtypeStruct(dims, F32)
        handed = (shape(chunks, tiles, n * SUB, LANES), shape(chunks, tiles, plane, LANES), shape(n * 2 * tiles, LANES),
                  shape(n * 2 * tiles, LANES), shape(parts_of, 2, tiles * UNIT, LANES))
        handed = pl.pallas_call(
            functools.partial(adi_kernel, (("row", parts_x), ("col", parts_y)), strides),
            out_shape=handed, in_specs=[in_hbm] * 7, out_specs=(in_vmem,) * len(handed), scratch_shapes=scratch,
            compiler_params=pltpu.CompilerParams(collective_id=0, has_side_effects=True, vmem_limit_bytes=36 * 1024 * 1024),
            name="adi_steps",
        )(*(pltpu.with_memory_space_constraint(array, pltpu.HBM) for array in (turned,) + coeffs))
        result = pl.pallas_call(
            finish_kernel, out_shape=jax.ShapeDtypeStruct(turned.shape, F32),
            in_specs=[in_vmem] * len(handed), out_specs=in_hbm,
            scratch_shapes=[pltpu.VMEM((tiles, n * SUB, LANES), F32), dma((chunks * tiles,))],
            compiler_params=pltpu.CompilerParams(vmem_limit_bytes=8 * 1024 * 1024), name="finish",
        )(*handed)
        return jnp.transpose(result, (0, 2, 1))

    return jax.shard_map(local_steps, mesh=mesh, in_specs=(field_spec,) + (coeff_spec,) * 6, out_specs=field_spec, check_vma=False)
```

```python
import functools

import jax
import jax.numpy as jnp
from jax import lax
from jax.experimental import pallas as pl
from jax.experimental.pallas import tpu as pltpu
from jax.sharding import PartitionSpec as P

STEPS = 3
F32 = jnp.float32
LANES = 128
SUB = 8
UNIT = SUB // 2
PITCH = SUB + 1
LOGICAL = pl.DeviceIdType.LOGICAL
X, Y = 0, 1


def adi_kernel(axes, strides, field, lower_x, diag_x, upper_x, lower_y, diag_y, upper_y, out, qs, w2, v2, ss,
               nat, rs, hs, pa, pb, pc, nd, md, ne, me_, ln, cn, un, an, m2, d2, r0, rn,
               gs, gc, red_x, red_y, sx, sy, ex, ey, raw, gt, halo_s, halo_r,
               load_sem, late_sem, send_sem, recv_x, recv_y, gather_sem):
    (row_name, parts_x), (col_name, parts_y) = axes
    n = lower_x.shape[0]
    tiles = n // LANES
    chunks = field.shape[1] // SUB
    parts_of = SUB // UNIT
    units = chunks * parts_of
    pitch = 2 * tiles
    half = n // 2
    pos = (lax.axis_index(row_name), lax.axis_index(col_name))
    parts = (parts_x, parts_y)
    home = sum(lax.axis_index(name) * stride for name, stride in strides.items())
    exch = (ex, ey)
    recv = (recv_x, recv_y)
    send = (sx, sy)
    reduced = (red_x, red_y)

    def device(axis, other):
        return home + (other - pos[axis]) * strides[(row_name, col_name)[axis]]

    def others(axis):
        count = parts[axis]
        offs = sorted(range(1, count), key=lambda off: (-min(off, count - off), -off))
        return [lax.rem(pos[axis] + off, count) for off in offs]

    def field_piece(c, t, first=0, count=n):
        late = c == chunks - 1 and t == tiles - 1 and first > 0
        return pltpu.make_async_copy(field.at[pl.ds(first, count), pl.ds(c * SUB, SUB), pl.ds(t * LANES, LANES)],
                                     out.at[c, t, pl.ds(first * SUB, count * SUB)].reshape(count, SUB, LANES), recv_x.at[1, 0, 0] if late else send_sem.at[t, c, 0])

    def load_field(c):
        for t in range(tiles):
            for first in range(0, n, LANES):
                field_piece(c, t, first, LANES).start()

    def load_coefficients(axis):
        for slot, ref in enumerate(((lower_x, diag_x, upper_x), (lower_y, diag_y, upper_y))[axis]):
            pltpu.make_async_copy(ref, nat.at[3 * axis + slot], (load_sem, late_sem)[axis]).start()

    for c in range(chunks):
        if c == chunks - 1:
            load_coefficients(X)
        load_field(c)
    load_coefficients(Y)

    halo_r[...] = jnp.zeros_like(halo_r)
    barrier = pltpu.get_barrier_semaphore()
    for axis in (X, Y):
        for other in others(axis):
            pl.semaphore_signal(barrier, 1, device_id=device(axis, other), device_id_type=LOGICAL)

    blank = jnp.zeros((SUB, LANES), F32)
    every = tuple(range(tiles))
    cells = [(c, t) for c in range(chunks) for t in range(tiles)]

    def slab(k):
        return pl.ds((k + 1) * PITCH, SUB)

    def each_chunk(body):
        lax.fori_loop(0, chunks, lambda c, carry: (body(c), carry)[1], 0)

    def turn(src, dst, c, axis, to, base, many, lts, ends=None, kts=None, step_in=PITCH, step_out=PITCH, correct=True, explicit=False, scale=None,
             g_ss=0):
        group = 2

        def column(g, carry):
            fs = [g * group + u for u in range(group)]
            for kt in kts or every:
                heads, tails = [None] * group, [None] * group
                for lt in lts:
                    rows = pl.ds(kt * (LANES * pitch) + (axis * tiles + lt), LANES, stride=pitch)
                    if correct:
                        near, far = w2[rows, :], v2[rows, :]
                    if explicit:
                        own, low, high = 2.0 - pb[rows, :], pa[rows, :], pc[rows, :]
                    if ends:
                        rows = pl.ds(lt * LANES * pitch + to * tiles + kt, LANES, stride=pitch)
                        first_row, last_row = r0[rows, :], rn[rows, :]
                    for u, f in enumerate(fs):
                        origin = kt * LANES * step_in + (step_in if step_in == PITCH else 0) + base + f
                        target = lt * LANES * step_out + (step_out if step_out == PITCH else 0) + base + f
                        block = src[c, lt, pl.ds(origin, LANES, stride=step_in), :]
                        if explicit:
                            block = own * block - (low * src[c, lt, pl.ds(origin - step_in, LANES, stride=step_in), :]
                                                   + high * src[c, lt, pl.ds(origin + step_in, LANES, stride=step_in), :])
                        if correct:
                            block = block + near * ss[g_ss, 0, pl.ds(lt * UNIT + f, 1), :] + far * ss[g_ss, 1, pl.ds(lt * UNIT + f, 1), :]
                        if scale is not None:
                            block = block * scale
                        flipped = block.T
                        dst[c, kt, pl.ds(target, LANES, stride=step_out), :] = flipped
                        if ends:
                            fold = lambda v: v.reshape(LANES // SUB, SUB, LANES).sum(axis=0)
                            h, s = fold(flipped * first_row), fold(flipped * last_row)
                            heads[u] = h if heads[u] is None else heads[u] + h
                            tails[u] = s if tails[u] is None else tails[u] + s
                if ends:
                    for u, f in enumerate(fs):
                        ends[0][pl.ds(kt * UNIT + f, 1), :] = jnp.sum(heads[u], axis=0, keepdims=True)
                        ends[1][pl.ds(kt * UNIT + f, 1), :] = jnp.sum(tails[u], axis=0, keepdims=True)
            return carry

        lax.fori_loop(0, many // group, column, 0, unroll=True)

    me_y = pos[Y]
    has_before, has_after = me_y > 0, me_y < parts_y - 1

    def halo(side, c, other):
        return pltpu.make_async_remote_copy(
            src_ref=halo_s.at[side, c], dst_ref=halo_r.at[1 - side, c], send_sem=send_sem.at[side, c, 0], recv_sem=recv_y.at[1, c, 1 - side],
            device_id=device(Y, other), device_id_type=LOGICAL)

    def send_halo(c):
        for t in every:
            halo_s[0, c, t] = qs[c, t, slab(0), :]
            halo_s[1, c, t] = qs[c, t, slab(n - 1), :]

        @pl.when(has_before)
        def _():
            halo(0, c, me_y - 1).start()

        @pl.when(has_after)
        def _():
            halo(1, c, me_y + 1).start()

    def await_halo(c):
        @pl.when(has_before)
        def _():
            halo(0, c, me_y - 1).wait_send()
            halo(1, c, me_y - 1).wait_recv()

        @pl.when(has_after)
        def _():
            halo(1, c, me_y + 1).wait_send()
            halo(0, c, me_y + 1).wait_recv()

        for t in every:
            qs[c, t, slab(-1), :] = halo_r[0, c, t]
            qs[c, t, slab(n), :] = halo_r[1, c, t]

    def pack_x():
        some = nat.at[pl.ds(0, 3)]
        pltpu.make_async_copy(some, some, load_sem).wait()
        for t in range(tiles):
            cols = pl.ds(t * LANES, LANES)
            pa[pl.ds(t, n, stride=pitch), :] = nat[0, :, cols]
            pb[pl.ds(t, n, stride=pitch), :] = nat[1, :, cols] + 1.0
            pc[pl.ds(t, n, stride=pitch), :] = nat[2, :, cols]

    for c in range(chunks):
        if c == chunks - 1:
            pack_x()
        for t in range(tiles):
            if c < chunks - 1 or t < tiles - 1:
                field_piece(c, t).wait()
                turn(out, qs, c, X, Y, 0, SUB, (t,), step_in=SUB, correct=False)
            else:
                for kt in every:
                    field_piece(c, t, kt * LANES, LANES).wait()
                    turn(out, qs, c, X, Y, 0, SUB, (t,), kts=(kt,), step_in=SUB, correct=False)
        if c == 0:
            pl.semaphore_wait(barrier, parts_x + parts_y - 2)
        send_halo(c)
    some = nat.at[pl.ds(3, 3)]
    pltpu.make_async_copy(some, some, late_sem).wait()
    for t in range(tiles):
        cols = pl.ds(t * LANES, LANES)
        for s in range(tiles):
            rows = pl.ds(s * LANES, LANES)
            dest = pl.ds(t * LANES * pitch + tiles + s, LANES, stride=pitch)
            pa[dest, :] = nat[3, rows, cols].T
            pb[dest, :] = nat[4, rows, cols].T + 1.0
            pc[dest, :] = nat[5, rows, cols].T

    long, deep = 16, 16
    zero = jnp.zeros((pitch, LANES), F32)
    one = jnp.ones((pitch, LANES), F32)

    def at_row(k, u):
        return pl.ds(pl.multiple_of(k * (long * pitch), long * pitch) + u * pitch, pitch)

    def pivots(g, state):
        dp, dq, c_prev, ep, eq, a_next = state
        h = n // long - 1 - g
        for u in range(0, long, 2):
            up, next_up = at_row(g, u), at_row(g, u + 1)
            b, t = pb[up, :], pa[up, :] * c_prev
            next_b, next_t = pb[next_up, :], pa[next_up, :] * pc[up, :]
            new = b * dp - t * dq
            newer = (next_b * b - next_t) * dp - (next_b * t) * dq
            nd[up, :], md[up, :], nd[next_up, :], md[next_up, :] = dp, new, new, newer
            dp, dq, c_prev = newer, new, pc[next_up, :]
            down, next_down = at_row(h, long - 1 - u), at_row(h, long - 2 - u)
            b, t = pb[down, :], a_next * pc[down, :]
            next_b, next_t = pb[next_down, :], pa[down, :] * pc[next_down, :]
            new = b * ep - t * eq
            newer = (next_b * b - next_t) * ep - (next_b * t) * eq
            ne[down, :], me_[down, :], ne[next_down, :], me_[next_down, :] = ep, new, new, newer
            ep, eq, a_next = newer, new, pa[next_down, :]
            if u % 8 == 2:
                scale_d, scale_e = 1.0 / dp, 1.0 / ep
            if u % 8 == 6:
                dp, dq, ep, eq = dp * scale_d, dq * scale_d, ep * scale_e, eq * scale_e
        return dp, dq, c_prev, ep, eq, a_next


    low_half = lax.broadcasted_iota(jnp.int32, (SUB, LANES), 0) < pitch
    blocks = n * pitch // SUB
    step_rows = long * pitch // SUB

    def ratios(g, state):
        prev_m, next_d = state
        for u in range(step_rows):
            up = pl.ds(pl.multiple_of(g * (SUB * step_rows), SUB * step_rows) + u * SUB, SUB)
            down = pl.ds(pl.multiple_of((blocks // step_rows - 1 - g) * (SUB * step_rows), SUB * step_rows)
                         + (step_rows - 1 - u) * SUB, SUB)
            minv = nd[up, :] / md[up, :]
            m2[up, :] = minv + minv
            cn[up, :] = -pc[up, :] * minv
            turned = pltpu.roll(minv, pitch, 0)
            ln[up, :] = -pa[up, :] * jnp.where(low_half, prev_m, turned)
            prev_m = turned
            dinv = ne[down, :] / me_[down, :]
            d2[down, :] = dinv + dinv
            an[down, :] = -pa[down, :] * dinv
            turned = pltpu.roll(dinv, pitch, 0)
            un[down, :] = -pc[down, :] * jnp.where(low_half, turned, next_d)
            next_d = turned
        return prev_m, next_d

    stretches = n // long
    state = lax.fori_loop(1, stretches, lambda g, state: (lambda later: (pivots(g, state[0]), later))(ratios(g - 1, state[1])),
                          (pivots(0, (one, zero, zero, one, zero, zero)), (blank, blank)))
    ratios(stretches - 1, state[1])

    first, last = pl.ds(0, pitch), pl.ds((n - 1) * pitch, pitch)

    def products(g, state):
        col0, row0, coln, rown, un_prev, ln_next = state
        h = n // long - 1 - g
        for u in range(long):
            up, down = at_row(g, u), at_row(h, long - 1 - u)
            start = jnp.logical_and(g == 0, u == 0) if u == 0 else None
            f0, f1 = an[up, :], un_prev
            b0, b1 = cn[down, :], ln_next
            if u == 0:
                f0, f1 = jnp.where(start, one, f0), jnp.where(start, one, f1)
                b0, b1 = jnp.where(start, one, b0), jnp.where(start, one, b1)
            col0, row0, coln, rown = col0 * f0, row0 * f1, coln * b0, rown * b1
            w2[up, :], r0[up, :], v2[down, :], rn[down, :] = col0, row0, coln, rown
            un_prev, ln_next = un[up, :], ln[down, :]
        return col0, row0, coln, rown, un_prev, ln_next

    d_first, m_last = 0.5 * d2[first, :], 0.5 * m2[last, :]
    lax.fori_loop(0, n // long, products,
                  (-pa[first, :] * d2[first, :], d_first, -pc[last, :] * m2[last, :], m_last, one, one))

    def block_ends(axis):
        for q, (ref, line) in enumerate(((w2, 0), (w2, n - 1), (v2, 0), (v2, n - 1))):
            yield q * tiles, -0.5 * ref[pl.ds(line * pitch + axis * tiles, tiles), :]

    for row, values in block_ends(X):
        raw[0, 0, pos[X], 2, pl.ds(row, tiles), :] = values

    def spread_y():
        for row, values in block_ends(Y):
            gs[pl.ds(row, tiles), :] = values
        gc[pos[Y]] = gs[...]
        for other in others(Y):
            pltpu.make_async_remote_copy(
                src_ref=gs, dst_ref=gc.at[pos[Y]], send_sem=load_sem, recv_sem=gather_sem,
                device_id=device(Y, other), device_id_type=LOGICAL).start()

    def reduce_lines(axis):
        count, me = parts[axis], pos[axis]
        if axis == Y:
            arrived = gc.at[pl.ds(0, count - 1)]
            pltpu.make_async_copy(arrived, arrived, gather_sem).wait()
            pltpu.make_async_copy(arrived, arrived, load_sem).wait()
            part = lambda p, q: gc[p, pl.ds(q * tiles, tiles), :]
        else:
            part = lambda p, q: raw[0, 0, p, 2, pl.ds(q * tiles, tiles), :]
        nil = jnp.zeros((tiles, LANES), F32)
        unit = jnp.ones((tiles, LANES), F32)
        mu, rho, tau = [None] * count, [None] * count, [None] * count
        prev = nil
        for p in range(count):
            wf, wt, vf, vt = (part(p, q) for q in range(4))
            kappa = 1.0 / (1.0 - wf * prev)
            mu[p], rho[p] = wt * prev * kappa, wt * kappa
            prev = tau[p] = vt + mu[p] * vf
        nu, omega, sigma = [None] * count, [None] * count, [None] * count
        prev = nil
        for p in reversed(range(count)):
            wf, wt, vf, vt = (part(p, q) for q in range(4))
            kappa = 1.0 / (1.0 - vt * prev)
            nu[p], omega[p] = vf * prev * kappa, vf * kappa
            prev = sigma[p] = wf + nu[p] * wt
        pick = lambda values, at: sum(jnp.where(at == p, v, nil) for p, v in enumerate(values))
        tau_b, sigma_a = pick(tau, me - 1), pick(sigma, me + 1)
        mu_me, nu_me = pick(mu, me), pick(nu, me)
        wf, wt, vf, vt = (part(me, q) for q in range(4))
        det = 1.0 / ((1.0 - tau_b * wf) * (1.0 - sigma_a * vt) - (tau_b * vf) * (sigma_a * wt))
        k11, k12 = (1.0 - sigma_a * vt) * det, tau_b * vf * det
        k21, k22 = sigma_a * wt * det, (1.0 - tau_b * wf) * det
        low, high = [None] * count, [None] * count
        for p in reversed(range(count)):
            onward = -rho[p + 1] * low[p + 1] if p + 1 < count else nil
            low[p] = jnp.where(me - 1 == p, unit, jnp.where(p < me - 1, onward, nil))
        for p in range(count):
            onward = -omega[p - 1] * high[p - 1] if p else nil
            high[p] = jnp.where(me + 1 == p, unit, jnp.where(p > me + 1, onward, nil))
        table = reduced[axis]

        def put(index, value):
            for t in every:
                table[index, pl.ds(t * UNIT, UNIT), :] = jnp.broadcast_to(value[t:t + 1], (UNIT, LANES))

        for p in range(count):
            put(p, k11 * low[p] + k12 * high[p] + jnp.where(me == p, -k11 * tau_b, nil))
            put(count + 1 + p, k21 * low[p] + k22 * high[p] + jnp.where(me == p, -k21 * tau_b, nil))
        put(count, -k12 * sigma_a)
        put(2 * count + 1, -k22 * sigma_a)
        put(2 * count + 2, mu_me)
        put(2 * count + 3, nu_me)
        if axis == X:
            for p in range(count):
                put(2 * count + 4 + p, jnp.where(p < me, mu[p], unit))
                put(3 * count + 4 + p, jnp.where(p < me, unit, jnp.where(p > me, nu[p], nil)))

    def publish(axis, stage, c, g):
        count, table, way = parts[axis], reduced[axis], lax.rem(stage, 2)
        head, tail = exch[axis][way, c, g, pos[axis]], gt[c, g]
        send[axis][c, g, 1] = tail + table[2 * count + 2] * head
        send[axis][c, g, 0] = head + table[2 * count + 3] * tail
        for other in others(axis):
            sel = jnp.where(other > pos[axis], 1, 0)
            pltpu.make_async_remote_copy(
                src_ref=send[axis].at[c, g, sel], dst_ref=exch[axis].at[way, c, g, pos[axis]],
                send_sem=send_sem.at[axis, c, g], recv_sem=recv[axis].at[way, c, g],
                device_id=device(axis, other), device_id_type=LOGICAL).start()

    def combine(axis, way, c, g, g_ss=0):
        count, table = parts[axis], reduced[axis]
        for side in range(2):
            base = side * (count + 1)
            terms = [table[base + count] * gt[c, g]] + [table[base + p] * exch[axis][way, c, g, p] for p in range(count)]
            while len(terms) > 1:
                terms = [a + b for a, b in zip(terms[::2], terms[1::2])] + terms[len(terms) // 2 * 2:]
            ss[g_ss, side] = terms[0]

    def neighbours(axis, stage, c, g, g_ss=0):
        way = lax.rem(stage, 2)
        arrived = exch[axis].at[way, c, g, pl.ds(0, parts[axis] - 1)]
        pltpu.make_async_copy(arrived, arrived, recv[axis].at[way, c, g]).wait()
        pltpu.make_async_copy(arrived, arrived, send_sem.at[axis, c, g]).wait()
        combine(axis, way, c, g, g_ss)

    def publish_raw(c, g):
        raw[c, g, pos[X], 0] = exch[X][0, c, g, pos[X]]
        raw[c, g, pos[X], 1] = gt[c, g]

        def send_raw(c, g, some):
            for other in others(X):
                pltpu.make_async_remote_copy(
                    src_ref=raw.at[c, g, pos[X], some], dst_ref=raw.at[c, g, pos[X], some],
                    send_sem=send_sem.at[X, c, g], recv_sem=recv_x.at[0, c, g], device_id=device(X, other), device_id_type=LOGICAL).start()

        @pl.when((c == 0) & (g == 0))
        def _():
            send_raw(0, 0, pl.ds(0, raw.shape[3]))

        @pl.when((c > 0) | (g > 0))
        def _():
            send_raw(c, g, pl.ds(0, 2))

    def await_raw(c, g, blocks):
        arrived = raw.at[c, g, pl.ds(0, parts_x - 1), pl.ds(0, blocks)]
        pltpu.make_async_copy(arrived, arrived, recv_x.at[0, c, g]).wait()
        pltpu.make_async_copy(arrived, arrived, send_sem.at[X, c, g]).wait()

    def neighbours_raw(c, g):
        count = parts_x
        for p in range(count):
            exch[X][0, c, g, p] = (red_x[2 * count + 4 + p] * raw[c, g, p, 0] + red_x[3 * count + 4 + p] * raw[c, g, p, 1])
        combine(X, 0, c, g)

    def solve_block(axis, minus):
        def coef(array, k, t):
            return array[pl.ds(k * pitch + axis * tiles + t, 1), :]

        def walk(first, sign, count, visit, state):
            def block(g, state):
                line = first + sign * deep * g
                row, coef_row = (line + 1) * PITCH, line * pitch + axis * tiles

                def one(u, state):
                    at = lambda array, t: array[pl.ds(coef_row + t + u * (sign * pitch), 1), :]
                    return visit(pl.ds(row + u * (sign * PITCH), SUB), at, state)

                return lax.fori_loop(0, min(count, deep), one, state, unroll=True)

            return lax.fori_loop(0, max(count // deep, 1), block, state)

        def eliminate(mult):
            def visit(here, at, state):
                values = list(state)
                for t in every:
                    factor = at(mult, t)
                    for c in range(chunks):
                        s = c * tiles + t
                        values[s] = rs[c, t, here, :] + factor * values[s]
                        hs[c, t, here, :] = values[s]
                return tuple(values)
            return visit

        init = tuple(blank for _ in cells)
        ups = walk(0, 1, half, eliminate(ln), init)
        downs = walk(n - 1, -1, half, eliminate(un), init)
        lo, hi = half - 1, half

        def place(c, t, here, value):
            qs[c, t, here, :] = value - rs[c, t, here, :] if minus else value

        low_s, high_s = [], []
        for s, (c, t) in enumerate(cells):
            c_lo, a_hi = coef(cn, lo, t), coef(an, hi, t)
            kappa = 1.0 / (1.0 - c_lo * a_hi)
            h_hi = coef(d2, hi, t) * downs[s]
            s_lo = kappa * (coef(m2, lo, t) * ups[s] + c_lo * h_hi)
            low_s.append(s_lo)
            high_s.append(h_hi + a_hi * s_lo)
            place(c, t, slab(lo), low_s[s])
            place(c, t, slab(hi), high_s[s])

        def substitute(scale, mult):
            def visit(here, at, state):
                values = list(state)
                for t in every:
                    own, factor = at(scale, t), at(mult, t)
                    for c in range(chunks):
                        s = c * tiles + t
                        values[s] = own * hs[c, t, here, :] + factor * values[s]
                        place(c, t, here, values[s])
                return tuple(values)
            return visit

        for first, sign, visit, state in ((lo, -1, substitute(m2, cn), low_s), (hi, 1, substitute(d2, an), high_s)):
            state = walk(first + sign, sign, deep - 1, visit, tuple(state))
            walk(first + sign * deep, sign, half - deep, visit, state)

    def each_unit(body, count=units):
        lax.fori_loop(0, count, lambda u, carry: (body(u // parts_of, lax.rem(u, parts_of)), carry)[1], 0)

    def ends_of(axis, stage, c, g):
        return exch[axis].at[lax.rem(stage, 2), c, g, pos[axis]], gt.at[c, g]

    def start_x(c):
        def unit(g, carry):
            turn(qs, rs, c, Y, X, g * UNIT, UNIT, every, ends_of(X, 0, c, g), correct=False, explicit=True)
            publish_raw(c, g)

            @pl.when((c == 0) & (g == 0))
            def _():
                spread_y()

            return carry

        await_halo(c)
        lax.fori_loop(0, parts_of, unit, 0)

    def onward(axis, stage, to, to_stage):
        def unit(c, g):
            neighbours(axis, stage, c, g)
            turn(qs, rs, c, axis, to, g * UNIT, UNIT, every, ends_of(to, to_stage, c, g))
            publish(to, to_stage, c, g)

        each_unit(unit)

    each_chunk(start_x)
    solve_block(X, True)
    reduce_lines(Y)
    await_raw(0, 0, raw.shape[3])
    reduce_lines(X)

    def first_to_y(c, g):
        @pl.when((c > 0) | (g > 0))
        def _():
            await_raw(c, g, 2)

        neighbours_raw(c, g)
        turn(qs, rs, c, X, Y, g * UNIT, UNIT, every, ends_of(Y, 0, c, g))
        publish(Y, 0, c, g)

    each_unit(first_to_y)

    def step(stage, carry):
        solve_block(Y, True)
        onward(Y, stage - 1, X, stage)
        solve_block(X, True)
        onward(X, stage, Y, stage)
        return carry

    lax.fori_loop(1, STEPS, step, 0)
    solve_block(Y, False)

    def finish(c, g):
        neighbours(Y, STEPS - 1, c, g)
        turn(qs, out, c, Y, X, g * UNIT, UNIT, every, scale=0.5, step_out=SUB)

    each_unit(finish, units - parts_of)
    for g in range(parts_of):
        neighbours(Y, STEPS - 1, chunks - 1, g, g)


def finish_kernel(done, qs, w2, v2, ss, out, fresh, sem):
    last, tiles, lines = done.shape[0] - 1, done.shape[1], done.shape[2] // SUB
    pitch = 2 * tiles

    def place(c, t, src, whole=False):
        step = lines if whole else LANES
        for first in range(0, lines, step):
            copy = pltpu.make_async_copy(src.at[pl.ds(first * SUB, step * SUB)].reshape(step, SUB, LANES),
                                         out.at[pl.ds(first, step), pl.ds(c * SUB, SUB), pl.ds(t * LANES, LANES)], sem.at[c * tiles + t])
            if whole:
                copy.wait()
            else:
                copy.start()

    for c in range(last):
        for t in range(tiles):
            place(c, t, done.at[c, t])
    for kt in range(tiles):
        def column(f, carry):
            for lt in range(tiles):
                rows = pl.ds(kt * LANES * pitch + tiles + lt, LANES, stride=pitch)
                block = qs[last, lt, pl.ds((kt * LANES + 1) * PITCH + f, LANES, stride=PITCH), :]
                near, far = (ss[f // UNIT, side, pl.ds(lt * UNIT + f % UNIT, 1), :] for side in range(2))
                block = block + w2[rows, :] * near + v2[rows, :] * far
                fresh[kt, pl.ds(lt * LANES * SUB + f, LANES, stride=SUB), :] = (block * 0.5).T
            return carry

        lax.fori_loop(0, SUB, column, 0, unroll=True)
        place(last, kt, fresh.at[kt])
    for c in range(last + 1):
        for t in range(tiles):
            place(c, t, done.at[c, t] if c < last else fresh.at[t], whole=True)


def solution(mesh):
    parts_x, parts_y = mesh.shape["row"], mesh.shape["col"]
    strides, stride = {}, 1
    for name in reversed(mesh.axis_names):
        strides[name], stride = stride, stride * mesh.shape[name]
    field_spec = P(("batch", "row"), "col", None)
    coeff_spec = P(("batch", "row"), "col")

    def local_steps(field, *coeffs):
        n, fields = field.shape[0], field.shape[2]
        tiles, chunks = n // LANES, fields // SUB
        packed = pltpu.VMEM((n * 2 * tiles, LANES), F32)
        plane = -(-((n + 2) * PITCH - SUB) // (4 * SUB)) * 4 * SUB + SUB
        big = pltpu.VMEM((chunks, tiles, plane, LANES), F32)
        dma = pltpu.SemaphoreType.DMA
        parts_of = SUB // UNIT
        sends = pltpu.VMEM((chunks, parts_of, 2, tiles * UNIT, LANES), F32)
        line = lambda count: pltpu.VMEM((2, chunks, parts_of, count, tiles * UNIT, LANES), F32)
        table = lambda count: pltpu.VMEM((4 * count + 4, tiles * UNIT, LANES), F32)
        small = pltpu.VMEM((2, chunks, tiles, SUB, LANES), F32)
        message = (4 * tiles, LANES)
        scratch = [
            pltpu.VMEM((6, n, n), F32), big, big, *([packed] * 15),
            pltpu.VMEM(message, F32), pltpu.VMEM((parts_y,) + message, F32),
            table(parts_x), table(parts_y), sends, sends, line(parts_x), line(parts_y),
            pltpu.VMEM((chunks, parts_of, parts_x, 3, tiles * UNIT, LANES), F32), pltpu.VMEM((chunks, parts_of, tiles * UNIT, LANES), F32),
            small, small, dma, dma, dma((2, chunks, parts_of)), dma((2, chunks, parts_of)), dma((2, chunks, parts_of)), dma,
        ]
        in_hbm = pl.BlockSpec(memory_space=pltpu.HBM)
        turned = jnp.transpose(field, (0, 2, 1))
        in_vmem = pl.BlockSpec(memory_space=pltpu.VMEM)
        shape = lambda *dims: jax.ShapeDtypeStruct(dims, F32)
        handed = (shape(chunks, tiles, n * SUB, LANES), shape(chunks, tiles, plane, LANES), shape(n * 2 * tiles, LANES),
                  shape(n * 2 * tiles, LANES), shape(parts_of, 2, tiles * UNIT, LANES))
        handed = pl.pallas_call(
            functools.partial(adi_kernel, (("row", parts_x), ("col", parts_y)), strides),
            out_shape=handed, in_specs=[in_hbm] * 7, out_specs=(in_vmem,) * len(handed), scratch_shapes=scratch,
            compiler_params=pltpu.CompilerParams(
                collective_id=0, has_side_effects=True, vmem_limit_bytes=36 * 1024 * 1024),
            name="adi_steps",
        )(*(pltpu.with_memory_space_constraint(array, pltpu.HBM) for array in (turned,) + coeffs))
        result = pl.pallas_call(
            finish_kernel, out_shape=jax.ShapeDtypeStruct(turned.shape, F32),
            in_specs=[in_vmem] * len(handed), out_specs=in_hbm,
            scratch_shapes=[pltpu.VMEM((tiles, n * SUB, LANES), F32), dma((chunks * tiles,))],
            compiler_params=pltpu.CompilerParams(vmem_limit_bytes=8 * 1024 * 1024), name="finish",
        )(*handed)
        return jnp.transpose(result, (0, 2, 1))

    return jax.shard_map(local_steps, mesh=mesh, in_specs=(field_spec,) + (coeff_spec,) * 6, out_specs=field_spec, check_vma=False)
```

```python
import functools

import jax
import jax.numpy as jnp
from jax import lax
from jax.experimental import pallas as pl
from jax.experimental.pallas import tpu as pltpu
from jax.sharding import PartitionSpec as P

STEPS = 3
F32 = jnp.float32
LANES = 128
SUB = 8
UNIT = SUB // 2
PITCH = SUB + 1
LOGICAL = pl.DeviceIdType.LOGICAL
X, Y = 0, 1


def adi_kernel(axes, strides, field, lower_x, diag_x, upper_x, lower_y, diag_y, upper_y, out, qs, w2, v2, ss,
               nat, rs, hs, pa, pb, pc, nd, md, ne, me_, ln, cn, un, an, m2, d2, r0, rn,
               gs, gc_x, gc_y, red_x, red_y, sx, sy, ex, ey, raw, gt, halo_s, halo_r,
               load_sem, late_sem, send_sem, recv_x, recv_y, gather_sem):
    (row_name, parts_x), (col_name, parts_y) = axes
    n = lower_x.shape[0]
    tiles = n // LANES
    chunks = field.shape[1] // SUB
    parts_of = SUB // UNIT
    units = chunks * parts_of
    pitch = 2 * tiles
    half = n // 2
    pos = (lax.axis_index(row_name), lax.axis_index(col_name))
    parts = (parts_x, parts_y)
    home = sum(lax.axis_index(name) * stride for name, stride in strides.items())
    exch = (ex, ey)
    recv = (recv_x, recv_y)
    send = (sx, sy)
    reduced = (red_x, red_y)
    gather, gather_sends = (gc_x, gc_y), (late_sem, load_sem)

    def device(axis, other):
        return home + (other - pos[axis]) * strides[(row_name, col_name)[axis]]

    def others(axis):
        count = parts[axis]
        offs = sorted(range(1, count), key=lambda off: (-min(off, count - off), -off))
        return [lax.rem(pos[axis] + off, count) for off in offs]

    def field_piece(c, t, first=0, count=n):
        late = c == chunks - 1 and t == tiles - 1 and first > 0
        return pltpu.make_async_copy(field.at[pl.ds(first, count), pl.ds(c * SUB, SUB), pl.ds(t * LANES, LANES)],
                                     out.at[c, t, pl.ds(first * SUB, count * SUB)].reshape(count, SUB, LANES), recv_x.at[1, 0, 0] if late else send_sem.at[t, c, 0])

    def load_field(c):
        for t in range(tiles):
            for first in range(0, n, LANES):
                field_piece(c, t, first, LANES).start()

    def load_coefficients(axis):
        for slot, ref in enumerate(((lower_x, diag_x, upper_x), (lower_y, diag_y, upper_y))[axis]):
            pltpu.make_async_copy(ref, nat.at[3 * axis + slot], (load_sem, late_sem)[axis]).start()

    for c in range(chunks):
        if c == chunks - 1:
            load_coefficients(X)
        load_field(c)
    load_coefficients(Y)

    halo_r[...] = jnp.zeros_like(halo_r)
    barrier = pltpu.get_barrier_semaphore()
    for axis in (X, Y):
        for other in others(axis):
            pl.semaphore_signal(barrier, 1, device_id=device(axis, other), device_id_type=LOGICAL)

    blank = jnp.zeros((SUB, LANES), F32)
    every = tuple(range(tiles))
    cells = [(c, t) for c in range(chunks) for t in range(tiles)]

    def slab(k):
        return pl.ds((k + 1) * PITCH, SUB)

    def each_chunk(body):
        lax.fori_loop(0, chunks, lambda c, carry: (body(c), carry)[1], 0)

    def turn(src, dst, c, axis, to, base, many, lts, ends=None, kts=None, step_in=PITCH, step_out=PITCH, correct=True, explicit=False, scale=None,
             g_ss=0):
        group = 2

        def column(g, carry):
            fs = [g * group + u for u in range(group)]
            for kt in kts or every:
                heads, tails = [None] * group, [None] * group
                for lt in lts:
                    rows = pl.ds(kt * (LANES * pitch) + (axis * tiles + lt), LANES, stride=pitch)
                    if correct:
                        near, far = w2[rows, :], v2[rows, :]
                    if explicit:
                        own, low, high = 2.0 - pb[rows, :], pa[rows, :], pc[rows, :]
                    if ends:
                        rows = pl.ds(lt * LANES * pitch + to * tiles + kt, LANES, stride=pitch)
                        first_row, last_row = r0[rows, :], rn[rows, :]
                    for u, f in enumerate(fs):
                        origin = kt * LANES * step_in + (step_in if step_in == PITCH else 0) + base + f
                        target = lt * LANES * step_out + (step_out if step_out == PITCH else 0) + base + f
                        block = src[c, lt, pl.ds(origin, LANES, stride=step_in), :]
                        if explicit:
                            block = own * block - (low * src[c, lt, pl.ds(origin - step_in, LANES, stride=step_in), :]
                                                   + high * src[c, lt, pl.ds(origin + step_in, LANES, stride=step_in), :])
                        if correct:
                            block = block + near * ss[g_ss, 0, pl.ds(lt * UNIT + f, 1), :] + far * ss[g_ss, 1, pl.ds(lt * UNIT + f, 1), :]
                        if scale is not None:
                            block = block * scale
                        flipped = block.T
                        dst[c, kt, pl.ds(target, LANES, stride=step_out), :] = flipped
                        if ends:
                            fold = lambda v: v.reshape(LANES // SUB, SUB, LANES).sum(axis=0)
                            h, s = fold(flipped * first_row), fold(flipped * last_row)
                            heads[u] = h if heads[u] is None else heads[u] + h
                            tails[u] = s if tails[u] is None else tails[u] + s
                if ends:
                    for u, f in enumerate(fs):
                        ends[0][pl.ds(kt * UNIT + f, 1), :] = jnp.sum(heads[u], axis=0, keepdims=True)
                        ends[1][pl.ds(kt * UNIT + f, 1), :] = jnp.sum(tails[u], axis=0, keepdims=True)
            return carry

        lax.fori_loop(0, many // group, column, 0, unroll=True)

    me_y = pos[Y]
    has_before, has_after = me_y > 0, me_y < parts_y - 1

    def halo(side, c, other):
        return pltpu.make_async_remote_copy(
            src_ref=halo_s.at[side, c], dst_ref=halo_r.at[1 - side, c], send_sem=send_sem.at[side, c, 0], recv_sem=recv_y.at[1, c, 1 - side],
            device_id=device(Y, other), device_id_type=LOGICAL)

    def send_halo(c):
        for t in every:
            halo_s[0, c, t] = qs[c, t, slab(0), :]
            halo_s[1, c, t] = qs[c, t, slab(n - 1), :]

        @pl.when(has_before)
        def _():
            halo(0, c, me_y - 1).start()

        @pl.when(has_after)
        def _():
            halo(1, c, me_y + 1).start()

    def await_halo(c):
        @pl.when(has_before)
        def _():
            halo(0, c, me_y - 1).wait_send()
            halo(1, c, me_y - 1).wait_recv()

        @pl.when(has_after)
        def _():
            halo(1, c, me_y + 1).wait_send()
            halo(0, c, me_y + 1).wait_recv()

        for t in every:
            qs[c, t, slab(-1), :] = halo_r[0, c, t]
            qs[c, t, slab(n), :] = halo_r[1, c, t]

    def pack_x():
        some = nat.at[pl.ds(0, 3)]
        pltpu.make_async_copy(some, some, load_sem).wait()
        for t in range(tiles):
            cols = pl.ds(t * LANES, LANES)
            pa[pl.ds(t, n, stride=pitch), :] = nat[0, :, cols]
            pb[pl.ds(t, n, stride=pitch), :] = nat[1, :, cols] + 1.0
            pc[pl.ds(t, n, stride=pitch), :] = nat[2, :, cols]

    for c in range(chunks):
        if c == chunks - 1:
            pack_x()
        for t in range(tiles):
            if c < chunks - 1 or t < tiles - 1:
                field_piece(c, t).wait()
                turn(out, qs, c, X, Y, 0, SUB, (t,), step_in=SUB, correct=False)
            else:
                for kt in every:
                    field_piece(c, t, kt * LANES, LANES).wait()
                    turn(out, qs, c, X, Y, 0, SUB, (t,), kts=(kt,), step_in=SUB, correct=False)
        if c == 0:
            pl.semaphore_wait(barrier, parts_x + parts_y - 2)
        send_halo(c)
    some = nat.at[pl.ds(3, 3)]
    pltpu.make_async_copy(some, some, late_sem).wait()
    for t in range(tiles):
        cols = pl.ds(t * LANES, LANES)
        for s in range(tiles):
            rows = pl.ds(s * LANES, LANES)
            dest = pl.ds(t * LANES * pitch + tiles + s, LANES, stride=pitch)
            pa[dest, :] = nat[3, rows, cols].T
            pb[dest, :] = nat[4, rows, cols].T + 1.0
            pc[dest, :] = nat[5, rows, cols].T

    long, deep = 16, 16
    zero = jnp.zeros((pitch, LANES), F32)
    one = jnp.ones((pitch, LANES), F32)

    def at_row(k, u):
        return pl.ds(pl.multiple_of(k * (long * pitch), long * pitch) + u * pitch, pitch)

    def pivots(g, state):
        dp, dq, c_prev, ep, eq, a_next = state
        h = n // long - 1 - g
        for u in range(0, long, 2):
            up, next_up = at_row(g, u), at_row(g, u + 1)
            b, t = pb[up, :], pa[up, :] * c_prev
            next_b, next_t = pb[next_up, :], pa[next_up, :] * pc[up, :]
            new = b * dp - t * dq
            newer = (next_b * b - next_t) * dp - (next_b * t) * dq
            nd[up, :], md[up, :], nd[next_up, :], md[next_up, :] = dp, new, new, newer
            dp, dq, c_prev = newer, new, pc[next_up, :]
            down, next_down = at_row(h, long - 1 - u), at_row(h, long - 2 - u)
            b, t = pb[down, :], a_next * pc[down, :]
            next_b, next_t = pb[next_down, :], pa[down, :] * pc[next_down, :]
            new = b * ep - t * eq
            newer = (next_b * b - next_t) * ep - (next_b * t) * eq
            ne[down, :], me_[down, :], ne[next_down, :], me_[next_down, :] = ep, new, new, newer
            ep, eq, a_next = newer, new, pa[next_down, :]
            if u % 8 == 2:
                scale_d, scale_e = 1.0 / dp, 1.0 / ep
            if u % 8 == 6:
                dp, dq, ep, eq = dp * scale_d, dq * scale_d, ep * scale_e, eq * scale_e
        return dp, dq, c_prev, ep, eq, a_next


    low_half = lax.broadcasted_iota(jnp.int32, (SUB, LANES), 0) < pitch
    blocks = n * pitch // SUB
    step_rows = long * pitch // SUB

    def ratios(g, state):
        prev_m, next_d = state
        for u in range(step_rows):
            up = pl.ds(pl.multiple_of(g * (SUB * step_rows), SUB * step_rows) + u * SUB, SUB)
            down = pl.ds(pl.multiple_of((blocks // step_rows - 1 - g) * (SUB * step_rows), SUB * step_rows)
                         + (step_rows - 1 - u) * SUB, SUB)
            minv = nd[up, :] / md[up, :]
            m2[up, :] = minv + minv
            cn[up, :] = -pc[up, :] * minv
            turned = pltpu.roll(minv, pitch, 0)
            ln[up, :] = -pa[up, :] * jnp.where(low_half, prev_m, turned)
            prev_m = turned
            dinv = ne[down, :] / me_[down, :]
            d2[down, :] = dinv + dinv
            an[down, :] = -pa[down, :] * dinv
            turned = pltpu.roll(dinv, pitch, 0)
            un[down, :] = -pc[down, :] * jnp.where(low_half, turned, next_d)
            next_d = turned
        return prev_m, next_d

    stretches = n // long
    state = lax.fori_loop(1, stretches, lambda g, state: (lambda later: (pivots(g, state[0]), later))(ratios(g - 1, state[1])),
                          (pivots(0, (one, zero, zero, one, zero, zero)), (blank, blank)))
    ratios(stretches - 1, state[1])

    first, last = pl.ds(0, pitch), pl.ds((n - 1) * pitch, pitch)

    def products(g, state):
        col0, row0, coln, rown, un_prev, ln_next = state
        h = n // long - 1 - g
        for u in range(long):
            up, down = at_row(g, u), at_row(h, long - 1 - u)
            start = jnp.logical_and(g == 0, u == 0) if u == 0 else None
            f0, f1 = an[up, :], un_prev
            b0, b1 = cn[down, :], ln_next
            if u == 0:
                f0, f1 = jnp.where(start, one, f0), jnp.where(start, one, f1)
                b0, b1 = jnp.where(start, one, b0), jnp.where(start, one, b1)
            col0, row0, coln, rown = col0 * f0, row0 * f1, coln * b0, rown * b1
            w2[up, :], r0[up, :], v2[down, :], rn[down, :] = col0, row0, coln, rown
            un_prev, ln_next = un[up, :], ln[down, :]
        return col0, row0, coln, rown, un_prev, ln_next

    d_first, m_last = 0.5 * d2[first, :], 0.5 * m2[last, :]
    lax.fori_loop(0, n // long, products,
                  (-pa[first, :] * d2[first, :], d_first, -pc[last, :] * m2[last, :], m_last, one, one))

    def spread(axis):
        for q, (ref, line) in enumerate(((w2, 0), (w2, n - 1), (v2, 0), (v2, n - 1))):
            gs[axis, pl.ds(q * tiles, tiles), :] = -0.5 * ref[pl.ds(line * pitch + axis * tiles, tiles), :]
        gather[axis][pos[axis]] = gs[axis]
        for other in others(axis):
            pltpu.make_async_remote_copy(
                src_ref=gs.at[axis], dst_ref=gather[axis].at[pos[axis]], send_sem=gather_sends[axis], recv_sem=gather_sem.at[axis],
                device_id=device(axis, other), device_id_type=LOGICAL).start()

    spread(X)

    def reduce_lines(axis):
        count, me = parts[axis], pos[axis]
        arrived = gather[axis].at[pl.ds(0, count - 1)]
        pltpu.make_async_copy(arrived, arrived, gather_sem.at[axis]).wait()
        pltpu.make_async_copy(arrived, arrived, gather_sends[axis]).wait()
        part = lambda p, q: gather[axis][p, pl.ds(q * tiles, tiles), :]
        nil = jnp.zeros((tiles, LANES), F32)
        unit = jnp.ones((tiles, LANES), F32)

        def eliminate(order, wf, wt, vf, vt):
            mu, rho, tau = [None] * count, [None] * count, [None] * count
            top, bottom = nil, unit
            for p in order:
                new_top = vt[p] * bottom + (wt[p] * vf[p] - vt[p] * wf[p]) * top
                new_bottom = bottom - wf[p] * top
                inverse = 1.0 / new_bottom
                mu[p], rho[p], tau[p] = wt[p] * top * inverse, wt[p] * bottom * inverse, new_top * inverse
                top, bottom = new_top, new_bottom
            return mu, rho, tau

        wf, wt, vf, vt = ([part(p, q) for p in range(count)] for q in range(4))
        mu, rho, tau = eliminate(range(count), wf, wt, vf, vt)
        nu, omega, sigma = eliminate(reversed(range(count)), vt, vf, wt, wf)
        pick = lambda values, at: sum(jnp.where(at == p, v, nil) for p, v in enumerate(values))
        tau_b, sigma_a = pick(tau, me - 1), pick(sigma, me + 1)
        mu_me, nu_me = pick(mu, me), pick(nu, me)
        wf, wt, vf, vt = (part(me, q) for q in range(4))
        det = 1.0 / ((1.0 - tau_b * wf) * (1.0 - sigma_a * vt) - (tau_b * vf) * (sigma_a * wt))
        k11, k12 = (1.0 - sigma_a * vt) * det, tau_b * vf * det
        k21, k22 = sigma_a * wt * det, (1.0 - tau_b * wf) * det
        low, high = [None] * count, [None] * count
        for p in reversed(range(count)):
            onward = -rho[p + 1] * low[p + 1] if p + 1 < count else nil
            low[p] = jnp.where(me - 1 == p, unit, jnp.where(p < me - 1, onward, nil))
        for p in range(count):
            onward = -omega[p - 1] * high[p - 1] if p else nil
            high[p] = jnp.where(me + 1 == p, unit, jnp.where(p > me + 1, onward, nil))
        table = reduced[axis]

        def put(index, value):
            for t in every:
                table[index, pl.ds(t * UNIT, UNIT), :] = jnp.broadcast_to(value[t:t + 1], (UNIT, LANES))

        for p in range(count):
            put(p, k11 * low[p] + k12 * high[p] + jnp.where(me == p, -k11 * tau_b, nil))
            put(count + 1 + p, k21 * low[p] + k22 * high[p] + jnp.where(me == p, -k21 * tau_b, nil))
        put(count, -k12 * sigma_a)
        put(2 * count + 1, -k22 * sigma_a)
        put(2 * count + 2, mu_me)
        put(2 * count + 3, nu_me)
        if axis == X:
            for p in range(count):
                put(2 * count + 4 + p, jnp.where(p < me, mu[p], unit))
                put(3 * count + 4 + p, jnp.where(p < me, unit, jnp.where(p > me, nu[p], nil)))

    def publish(axis, stage, c, g):
        count, table, way = parts[axis], reduced[axis], lax.rem(stage, 2)
        head, tail = exch[axis][way, c, g, pos[axis]], gt[c, g]
        send[axis][c, g, 1] = tail + table[2 * count + 2] * head
        send[axis][c, g, 0] = head + table[2 * count + 3] * tail
        for other in others(axis):
            sel = jnp.where(other > pos[axis], 1, 0)
            pltpu.make_async_remote_copy(
                src_ref=send[axis].at[c, g, sel], dst_ref=exch[axis].at[way, c, g, pos[axis]],
                send_sem=send_sem.at[axis, c, g], recv_sem=recv[axis].at[way, c, g],
                device_id=device(axis, other), device_id_type=LOGICAL).start()

    def combine(axis, way, c, g, g_ss=0):
        count, table = parts[axis], reduced[axis]
        for side in range(2):
            base = side * (count + 1)
            terms = [table[base + count] * gt[c, g]] + [table[base + p] * exch[axis][way, c, g, p] for p in range(count)]
            while len(terms) > 1:
                terms = [a + b for a, b in zip(terms[::2], terms[1::2])] + terms[len(terms) // 2 * 2:]
            ss[g_ss, side] = terms[0]

    def neighbours(axis, stage, c, g, g_ss=0):
        way = lax.rem(stage, 2)
        arrived = exch[axis].at[way, c, g, pl.ds(0, parts[axis] - 1)]
        pltpu.make_async_copy(arrived, arrived, recv[axis].at[way, c, g]).wait()
        pltpu.make_async_copy(arrived, arrived, send_sem.at[axis, c, g]).wait()
        combine(axis, way, c, g, g_ss)

    def publish_raw(c, g):
        raw[c, g, pos[X], 0] = exch[X][0, c, g, pos[X]]
        raw[c, g, pos[X], 1] = gt[c, g]

        for other in others(X):
            pltpu.make_async_remote_copy(
                src_ref=raw.at[c, g, pos[X]], dst_ref=raw.at[c, g, pos[X]], send_sem=send_sem.at[X, c, g], recv_sem=recv_x.at[0, c, g],
                device_id=device(X, other), device_id_type=LOGICAL).start()

    def neighbours_raw(c, g):
        arrived = raw.at[c, g, pl.ds(0, parts_x - 1)]
        pltpu.make_async_copy(arrived, arrived, recv_x.at[0, c, g]).wait()
        pltpu.make_async_copy(arrived, arrived, send_sem.at[X, c, g]).wait()
        count = parts_x
        for p in range(count):
            exch[X][0, c, g, p] = (red_x[2 * count + 4 + p] * raw[c, g, p, 0] + red_x[3 * count + 4 + p] * raw[c, g, p, 1])
        combine(X, 0, c, g)

    def solve_block(axis, minus):
        def coef(array, k, t):
            return array[pl.ds(k * pitch + axis * tiles + t, 1), :]

        def walk(first, sign, count, visit, state):
            def block(g, state):
                line = first + sign * deep * g
                row, coef_row = (line + 1) * PITCH, line * pitch + axis * tiles

                def one(u, state):
                    at = lambda array, t: array[pl.ds(coef_row + t + u * (sign * pitch), 1), :]
                    return visit(pl.ds(row + u * (sign * PITCH), SUB), at, state)

                return lax.fori_loop(0, min(count, deep), one, state, unroll=True)

            return lax.fori_loop(0, max(count // deep, 1), block, state)

        def eliminate(mult):
            def visit(here, at, state):
                values = list(state)
                for t in every:
                    factor = at(mult, t)
                    for c in range(chunks):
                        s = c * tiles + t
                        values[s] = rs[c, t, here, :] + factor * values[s]
                        hs[c, t, here, :] = values[s]
                return tuple(values)
            return visit

        init = tuple(blank for _ in cells)
        ups = walk(0, 1, half, eliminate(ln), init)
        downs = walk(n - 1, -1, half, eliminate(un), init)
        lo, hi = half - 1, half

        def place(c, t, here, value):
            qs[c, t, here, :] = value - rs[c, t, here, :] if minus else value

        low_s, high_s = [], []
        for s, (c, t) in enumerate(cells):
            c_lo, a_hi = coef(cn, lo, t), coef(an, hi, t)
            kappa = 1.0 / (1.0 - c_lo * a_hi)
            h_hi = coef(d2, hi, t) * downs[s]
            s_lo = kappa * (coef(m2, lo, t) * ups[s] + c_lo * h_hi)
            low_s.append(s_lo)
            high_s.append(h_hi + a_hi * s_lo)
            place(c, t, slab(lo), low_s[s])
            place(c, t, slab(hi), high_s[s])

        def substitute(scale, mult):
            def visit(here, at, state):
                values = list(state)
                for t in every:
                    own, factor = at(scale, t), at(mult, t)
                    for c in range(chunks):
                        s = c * tiles + t
                        values[s] = own * hs[c, t, here, :] + factor * values[s]
                        place(c, t, here, values[s])
                return tuple(values)
            return visit

        for first, sign, visit, state in ((lo, -1, substitute(m2, cn), low_s), (hi, 1, substitute(d2, an), high_s)):
            state = walk(first + sign, sign, deep - 1, visit, tuple(state))
            walk(first + sign * deep, sign, half - deep, visit, state)

    def each_unit(body, count=units):
        lax.fori_loop(0, count, lambda u, carry: (body(u // parts_of, lax.rem(u, parts_of)), carry)[1], 0)

    def ends_of(axis, stage, c, g):
        return exch[axis].at[lax.rem(stage, 2), c, g, pos[axis]], gt.at[c, g]

    def start_x(c):
        def unit(g, carry):
            turn(qs, rs, c, Y, X, g * UNIT, UNIT, every, ends_of(X, 0, c, g), correct=False, explicit=True)
            publish_raw(c, g)

            @pl.when((c == 0) & (g == 0))
            def _():
                spread(Y)

            return carry

        await_halo(c)
        lax.fori_loop(0, parts_of, unit, 0)

    def onward(axis, stage, to, to_stage):
        def unit(c, g):
            neighbours(axis, stage, c, g)
            turn(qs, rs, c, axis, to, g * UNIT, UNIT, every, ends_of(to, to_stage, c, g))
            publish(to, to_stage, c, g)

        each_unit(unit)

    each_chunk(start_x)
    solve_block(X, True)
    reduce_lines(X)
    reduce_lines(Y)

    def first_to_y(c, g):
        neighbours_raw(c, g)
        turn(qs, rs, c, X, Y, g * UNIT, UNIT, every, ends_of(Y, 0, c, g))
        publish(Y, 0, c, g)

    each_unit(first_to_y)

    def step(stage, carry):
        solve_block(Y, True)
        onward(Y, stage - 1, X, stage)
        solve_block(X, True)
        onward(X, stage, Y, stage)
        return carry

    lax.fori_loop(1, STEPS, step, 0)
    solve_block(Y, False)

    def finish(c, g):
        neighbours(Y, STEPS - 1, c, g)
        turn(qs, out, c, Y, X, g * UNIT, UNIT, every, scale=0.5, step_out=SUB)

    each_unit(finish, units - parts_of)
    for g in range(parts_of):
        neighbours(Y, STEPS - 1, chunks - 1, g, g)


def finish_kernel(done, qs, w2, v2, ss, out, fresh, sem):
    last, tiles, lines = done.shape[0] - 1, done.shape[1], done.shape[2] // SUB
    pitch = 2 * tiles

    def place(c, t, src, whole=False):
        step = lines if whole else LANES
        for first in range(0, lines, step):
            copy = pltpu.make_async_copy(src.at[pl.ds(first * SUB, step * SUB)].reshape(step, SUB, LANES),
                                         out.at[pl.ds(first, step), pl.ds(c * SUB, SUB), pl.ds(t * LANES, LANES)], sem.at[c * tiles + t])
            if whole:
                copy.wait()
            else:
                copy.start()

    for c in range(last):
        for t in range(tiles):
            place(c, t, done.at[c, t])
    for kt in range(tiles):
        def column(f, carry):
            for lt in range(tiles):
                rows = pl.ds(kt * LANES * pitch + tiles + lt, LANES, stride=pitch)
                block = qs[last, lt, pl.ds((kt * LANES + 1) * PITCH + f, LANES, stride=PITCH), :]
                near, far = (ss[f // UNIT, side, pl.ds(lt * UNIT + f % UNIT, 1), :] for side in range(2))
                block = block + w2[rows, :] * near + v2[rows, :] * far
                fresh[kt, pl.ds(lt * LANES * SUB + f, LANES, stride=SUB), :] = (block * 0.5).T
            return carry

        lax.fori_loop(0, SUB, column, 0, unroll=True)
        place(last, kt, fresh.at[kt])
    for c in range(last + 1):
        for t in range(tiles):
            place(c, t, done.at[c, t] if c < last else fresh.at[t], whole=True)


def solution(mesh):
    parts_x, parts_y = mesh.shape["row"], mesh.shape["col"]
    strides, stride = {}, 1
    for name in reversed(mesh.axis_names):
        strides[name], stride = stride, stride * mesh.shape[name]
    field_spec = P(("batch", "row"), "col", None)
    coeff_spec = P(("batch", "row"), "col")

    def local_steps(field, *coeffs):
        n, fields = field.shape[0], field.shape[2]
        tiles, chunks = n // LANES, fields // SUB
        packed = pltpu.VMEM((n * 2 * tiles, LANES), F32)
        plane = -(-((n + 2) * PITCH - SUB) // (4 * SUB)) * 4 * SUB + SUB
        big = pltpu.VMEM((chunks, tiles, plane, LANES), F32)
        dma = pltpu.SemaphoreType.DMA
        parts_of = SUB // UNIT
        sends = pltpu.VMEM((chunks, parts_of, 2, tiles * UNIT, LANES), F32)
        line = lambda count: pltpu.VMEM((2, chunks, parts_of, count, tiles * UNIT, LANES), F32)
        table = lambda count: pltpu.VMEM((4 * count + 4, tiles * UNIT, LANES), F32)
        small = pltpu.VMEM((2, chunks, tiles, SUB, LANES), F32)
        message = (4 * tiles, LANES)
        scratch = [
            pltpu.VMEM((6, n, n), F32), big, big, *([packed] * 15),
            pltpu.VMEM((2,) + message, F32), pltpu.VMEM((parts_x,) + message, F32), pltpu.VMEM((parts_y,) + message, F32),
            table(parts_x), table(parts_y), sends, sends, line(parts_x), line(parts_y),
            pltpu.VMEM((chunks, parts_of, parts_x, 2, tiles * UNIT, LANES), F32), pltpu.VMEM((chunks, parts_of, tiles * UNIT, LANES), F32),
            small, small, dma, dma, dma((2, chunks, parts_of)), dma((2, chunks, parts_of)), dma((2, chunks, parts_of)), dma((2,)),
        ]
        in_hbm = pl.BlockSpec(memory_space=pltpu.HBM)
        turned = jnp.transpose(field, (0, 2, 1))
        in_vmem = pl.BlockSpec(memory_space=pltpu.VMEM)
        shape = lambda *dims: jax.ShapeDtypeStruct(dims, F32)
        handed = (shape(chunks, tiles, n * SUB, LANES), shape(chunks, tiles, plane, LANES), shape(n * 2 * tiles, LANES),
                  shape(n * 2 * tiles, LANES), shape(parts_of, 2, tiles * UNIT, LANES))
        handed = pl.pallas_call(
            functools.partial(adi_kernel, (("row", parts_x), ("col", parts_y)), strides),
            out_shape=handed, in_specs=[in_hbm] * 7, out_specs=(in_vmem,) * len(handed), scratch_shapes=scratch,
            compiler_params=pltpu.CompilerParams(
                collective_id=0, has_side_effects=True, vmem_limit_bytes=36 * 1024 * 1024),
            name="adi_steps",
        )(*(pltpu.with_memory_space_constraint(array, pltpu.HBM) for array in (turned,) + coeffs))
        result = pl.pallas_call(
            finish_kernel, out_shape=jax.ShapeDtypeStruct(turned.shape, F32),
            in_specs=[in_vmem] * len(handed), out_specs=in_hbm,
            scratch_shapes=[pltpu.VMEM((tiles, n * SUB, LANES), F32), dma((chunks * tiles,))],
            compiler_params=pltpu.CompilerParams(vmem_limit_bytes=8 * 1024 * 1024), name="finish",
        )(*handed)
        return jnp.transpose(result, (0, 2, 1))

    return jax.shard_map(local_steps, mesh=mesh, in_specs=(field_spec,) + (coeff_spec,) * 6, out_specs=field_spec, check_vma=False)
```

```python
import functools

import jax
import jax.numpy as jnp
from jax import lax
from jax.experimental import pallas as pl
from jax.experimental.pallas import tpu as pltpu
from jax.sharding import PartitionSpec as P

STEPS = 3
F32 = jnp.float32
LANES = 128
SUB = 8
UNIT = SUB // 2
PITCH = SUB + 1
LOGICAL = pl.DeviceIdType.LOGICAL
X, Y = 0, 1


def adi_kernel(axes, strides, field, lower_x, diag_x, upper_x, lower_y, diag_y, upper_y, out, qs, w2, v2, ss,
               nat, rs, hs, pa, pb, pc, nd, md, ne, me_, ln, cn, un, an, m2, d2, r0, rn,
               gs, gc_x, gc_y, red_x, red_y, sx, sy, ex, ey, raw, gt, halo_s, halo_r,
               load_sem, late_sem, send_sem, recv_x, recv_y, gather_sem):
    (row_name, parts_x), (col_name, parts_y) = axes
    n = lower_x.shape[0]
    tiles = n // LANES
    chunks = field.shape[1] // SUB
    parts_of = SUB // UNIT
    units = chunks * parts_of
    pitch = 2 * tiles
    half = n // 2
    pos = (lax.axis_index(row_name), lax.axis_index(col_name))
    parts = (parts_x, parts_y)
    home = sum(lax.axis_index(name) * stride for name, stride in strides.items())
    exch = (ex, ey)
    recv = (recv_x, recv_y)
    send = (sx, sy)
    reduced = (red_x, red_y)
    gather, gather_sends = (gc_x, gc_y), (late_sem, load_sem)

    def device(axis, other):
        return home + (other - pos[axis]) * strides[(row_name, col_name)[axis]]

    def others(axis):
        count = parts[axis]
        offs = sorted(range(1, count), key=lambda off: (-min(off, count - off), -off))
        return [lax.rem(pos[axis] + off, count) for off in offs]

    def field_piece(c, t, first=0, count=n):
        late = c == chunks - 1 and t == tiles - 1 and first > 0
        return pltpu.make_async_copy(field.at[pl.ds(first, count), pl.ds(c * SUB, SUB), pl.ds(t * LANES, LANES)],
                                     out.at[c, t, pl.ds(first * SUB, count * SUB)].reshape(count, SUB, LANES), recv_x.at[1, 0, 0] if late else send_sem.at[c, t])

    def load_field(c):
        for t in range(tiles):
            for first in range(0, n, LANES):
                field_piece(c, t, first, LANES).start()

    def load_coefficients(axis):
        for slot, ref in enumerate(((lower_x, diag_x, upper_x), (lower_y, diag_y, upper_y))[axis]):
            pltpu.make_async_copy(ref, nat.at[3 * axis + slot], (load_sem, late_sem)[axis]).start()

    for c in range(chunks):
        if c == chunks - 1:
            load_coefficients(X)
        load_field(c)
    load_coefficients(Y)

    halo_r[...] = jnp.zeros_like(halo_r)
    barrier = pltpu.get_barrier_semaphore()
    for axis in (X, Y):
        for other in others(axis):
            pl.semaphore_signal(barrier, 1, device_id=device(axis, other), device_id_type=LOGICAL)

    blank = jnp.zeros((SUB, LANES), F32)
    every = tuple(range(tiles))
    cells = [(c, t) for c in range(chunks) for t in range(tiles)]

    def slab(k):
        return pl.ds((k + 1) * PITCH, SUB)

    def each_chunk(body):
        lax.fori_loop(0, chunks, lambda c, carry: (body(c), carry)[1], 0)

    def turn(src, dst, c, axis, to, base, many, lts, ends=None, kts=None, step_in=PITCH, step_out=PITCH, correct=True, explicit=False, scale=None,
             g_ss=0):
        group = 2

        def column(g, carry):
            fs = [g * group + u for u in range(group)]
            for kt in kts or every:
                heads, tails = [None] * group, [None] * group
                for lt in lts:
                    rows = pl.ds(kt * (LANES * pitch) + (axis * tiles + lt), LANES, stride=pitch)
                    if correct:
                        near, far = w2[rows, :], v2[rows, :]
                    if explicit:
                        own, low, high = 2.0 - pb[rows, :], pa[rows, :], pc[rows, :]
                    if ends:
                        rows = pl.ds(lt * LANES * pitch + to * tiles + kt, LANES, stride=pitch)
                        first_row, last_row = r0[rows, :], rn[rows, :]
                    for u, f in enumerate(fs):
                        origin = kt * LANES * step_in + (step_in if step_in == PITCH else 0) + base + f
                        target = lt * LANES * step_out + (step_out if step_out == PITCH else 0) + base + f
                        block = src[c, lt, pl.ds(origin, LANES, stride=step_in), :]
                        if explicit:
                            block = own * block - (low * src[c, lt, pl.ds(origin - step_in, LANES, stride=step_in), :]
                                                   + high * src[c, lt, pl.ds(origin + step_in, LANES, stride=step_in), :])
                        if correct:
                            block = block + near * ss[g_ss, 0, pl.ds(lt * UNIT + f, 1), :] + far * ss[g_ss, 1, pl.ds(lt * UNIT + f, 1), :]
                        if scale is not None:
                            block = block * scale
                        flipped = block.T
                        dst[c, kt, pl.ds(target, LANES, stride=step_out), :] = flipped
                        if ends:
                            fold = lambda v: v.reshape(LANES // SUB, SUB, LANES).sum(axis=0)
                            h, s = fold(flipped * first_row), fold(flipped * last_row)
                            heads[u] = h if heads[u] is None else heads[u] + h
                            tails[u] = s if tails[u] is None else tails[u] + s
                if ends:
                    for u, f in enumerate(fs):
                        ends[0][pl.ds(kt * UNIT + f, 1), :] = jnp.sum(heads[u], axis=0, keepdims=True)
                        ends[1][pl.ds(kt * UNIT + f, 1), :] = jnp.sum(tails[u], axis=0, keepdims=True)
            return carry

        lax.fori_loop(0, many // group, column, 0, unroll=True)

    me_y = pos[Y]
    has_before, has_after = me_y > 0, me_y < parts_y - 1

    def halo(side, c, other):
        return pltpu.make_async_remote_copy(
            src_ref=halo_s.at[side, c], dst_ref=halo_r.at[1 - side, c], send_sem=send_sem.at[c, side], recv_sem=recv_y.at[1, c, 1 - side],
            device_id=device(Y, other), device_id_type=LOGICAL)

    def send_halo(c):
        for t in every:
            halo_s[0, c, t] = qs[c, t, slab(0), :]
            halo_s[1, c, t] = qs[c, t, slab(n - 1), :]

        @pl.when(has_before)
        def _():
            halo(0, c, me_y - 1).start()

        @pl.when(has_after)
        def _():
            halo(1, c, me_y + 1).start()

    def await_halo(c):
        @pl.when(has_before)
        def _():
            halo(0, c, me_y - 1).wait_send()
            halo(1, c, me_y - 1).wait_recv()

        @pl.when(has_after)
        def _():
            halo(1, c, me_y + 1).wait_send()
            halo(0, c, me_y + 1).wait_recv()

        for t in every:
            qs[c, t, slab(-1), :] = halo_r[0, c, t]
            qs[c, t, slab(n), :] = halo_r[1, c, t]

    def pack_x():
        some = nat.at[pl.ds(0, 3)]
        pltpu.make_async_copy(some, some, load_sem).wait()
        for t in range(tiles):
            cols = pl.ds(t * LANES, LANES)
            pa[pl.ds(t, n, stride=pitch), :] = nat[0, :, cols]
            pb[pl.ds(t, n, stride=pitch), :] = nat[1, :, cols] + 1.0
            pc[pl.ds(t, n, stride=pitch), :] = nat[2, :, cols]

    for c in range(chunks):
        if c == chunks - 1:
            pack_x()
        for t in range(tiles):
            if c < chunks - 1 or t < tiles - 1:
                field_piece(c, t).wait()
                turn(out, qs, c, X, Y, 0, SUB, (t,), step_in=SUB, correct=False)
            else:
                for kt in every:
                    field_piece(c, t, kt * LANES, LANES).wait()
                    turn(out, qs, c, X, Y, 0, SUB, (t,), kts=(kt,), step_in=SUB, correct=False)
        if c == 0:
            pl.semaphore_wait(barrier, parts_x + parts_y - 2)
        send_halo(c)
    some = nat.at[pl.ds(3, 3)]
    pltpu.make_async_copy(some, some, late_sem).wait()
    for t in range(tiles):
        cols = pl.ds(t * LANES, LANES)
        for s in range(tiles):
            rows = pl.ds(s * LANES, LANES)
            dest = pl.ds(t * LANES * pitch + tiles + s, LANES, stride=pitch)
            pa[dest, :] = nat[3, rows, cols].T
            pb[dest, :] = nat[4, rows, cols].T + 1.0
            pc[dest, :] = nat[5, rows, cols].T

    long, deep = 16, 16
    zero = jnp.zeros((pitch, LANES), F32)
    one = jnp.ones((pitch, LANES), F32)

    def at_row(k, u):
        return pl.ds(pl.multiple_of(k * (long * pitch), long * pitch) + u * pitch, pitch)

    def pivots(g, state):
        dp, dq, c_prev, ep, eq, a_next = state
        h = n // long - 1 - g
        for u in range(0, long, 2):
            up, next_up = at_row(g, u), at_row(g, u + 1)
            b, t = pb[up, :], pa[up, :] * c_prev
            next_b, next_t = pb[next_up, :], pa[next_up, :] * pc[up, :]
            new = b * dp - t * dq
            newer = (next_b * b - next_t) * dp - (next_b * t) * dq
            nd[up, :], md[up, :], nd[next_up, :], md[next_up, :] = dp, new, new, newer
            dp, dq, c_prev = newer, new, pc[next_up, :]
            down, next_down = at_row(h, long - 1 - u), at_row(h, long - 2 - u)
            b, t = pb[down, :], a_next * pc[down, :]
            next_b, next_t = pb[next_down, :], pa[down, :] * pc[next_down, :]
            new = b * ep - t * eq
            newer = (next_b * b - next_t) * ep - (next_b * t) * eq
            ne[down, :], me_[down, :], ne[next_down, :], me_[next_down, :] = ep, new, new, newer
            ep, eq, a_next = newer, new, pa[next_down, :]
            if u % 8 == 2:
                scale_d, scale_e = 1.0 / dp, 1.0 / ep
            if u % 8 == 6:
                dp, dq, ep, eq = dp * scale_d, dq * scale_d, ep * scale_e, eq * scale_e
        return dp, dq, c_prev, ep, eq, a_next


    low_half = lax.broadcasted_iota(jnp.int32, (SUB, LANES), 0) < pitch
    blocks = n * pitch // SUB
    step_rows = long * pitch // SUB

    def ratios(g, state):
        prev_m, next_d = state
        for u in range(step_rows):
            up = pl.ds(pl.multiple_of(g * (SUB * step_rows), SUB * step_rows) + u * SUB, SUB)
            down = pl.ds(pl.multiple_of((blocks // step_rows - 1 - g) * (SUB * step_rows), SUB * step_rows)
                         + (step_rows - 1 - u) * SUB, SUB)
            minv = nd[up, :] / md[up, :]
            m2[up, :] = minv + minv
            cn[up, :] = -pc[up, :] * minv
            turned = pltpu.roll(minv, pitch, 0)
            ln[up, :] = -pa[up, :] * jnp.where(low_half, prev_m, turned)
            prev_m = turned
            dinv = ne[down, :] / me_[down, :]
            d2[down, :] = dinv + dinv
            an[down, :] = -pa[down, :] * dinv
            turned = pltpu.roll(dinv, pitch, 0)
            un[down, :] = -pc[down, :] * jnp.where(low_half, turned, next_d)
            next_d = turned
        return prev_m, next_d

    stretches = n // long
    state = lax.fori_loop(1, stretches, lambda g, state: (lambda later: (pivots(g, state[0]), later))(ratios(g - 1, state[1])),
                          (pivots(0, (one, zero, zero, one, zero, zero)), (blank, blank)))
    ratios(stretches - 1, state[1])

    first, last = pl.ds(0, pitch), pl.ds((n - 1) * pitch, pitch)

    def products(g, state):
        col0, row0, coln, rown, un_prev, ln_next = state
        h = n // long - 1 - g
        for u in range(long):
            up, down = at_row(g, u), at_row(h, long - 1 - u)
            start = jnp.logical_and(g == 0, u == 0) if u == 0 else None
            f0, f1 = an[up, :], un_prev
            b0, b1 = cn[down, :], ln_next
            if u == 0:
                f0, f1 = jnp.where(start, one, f0), jnp.where(start, one, f1)
                b0, b1 = jnp.where(start, one, b0), jnp.where(start, one, b1)
            col0, row0, coln, rown = col0 * f0, row0 * f1, coln * b0, rown * b1
            w2[up, :], r0[up, :], v2[down, :], rn[down, :] = col0, row0, coln, rown
            un_prev, ln_next = un[up, :], ln[down, :]
        return col0, row0, coln, rown, un_prev, ln_next

    d_first, m_last = 0.5 * d2[first, :], 0.5 * m2[last, :]
    lax.fori_loop(0, n // long, products,
                  (-pa[first, :] * d2[first, :], d_first, -pc[last, :] * m2[last, :], m_last, one, one))

    def spread(axis):
        for q, (ref, line) in enumerate(((w2, 0), (w2, n - 1), (v2, 0), (v2, n - 1))):
            gs[axis, pl.ds(q * tiles, tiles), :] = -0.5 * ref[pl.ds(line * pitch + axis * tiles, tiles), :]
        gather[axis][pos[axis]] = gs[axis]
        for other in others(axis):
            pltpu.make_async_remote_copy(
                src_ref=gs.at[axis], dst_ref=gather[axis].at[pos[axis]], send_sem=gather_sends[axis], recv_sem=gather_sem.at[axis],
                device_id=device(axis, other), device_id_type=LOGICAL).start()

    spread(X)

    def reduce_lines(axis):
        count, me = parts[axis], pos[axis]
        arrived = gather[axis].at[pl.ds(0, count - 1)]
        pltpu.make_async_copy(arrived, arrived, gather_sem.at[axis]).wait()
        pltpu.make_async_copy(arrived, arrived, gather_sends[axis]).wait()
        part = lambda p, q: gather[axis][p, pl.ds(q * tiles, tiles), :]
        nil = jnp.zeros((tiles, LANES), F32)
        unit = jnp.ones((tiles, LANES), F32)

        def eliminate(order, wf, wt, vf, vt):
            mu, rho, tau = [None] * count, [None] * count, [None] * count
            top, bottom = nil, unit
            for p in order:
                new_top = vt[p] * bottom + (wt[p] * vf[p] - vt[p] * wf[p]) * top
                new_bottom = bottom - wf[p] * top
                inverse = 1.0 / new_bottom
                mu[p], rho[p], tau[p] = wt[p] * top * inverse, wt[p] * bottom * inverse, new_top * inverse
                top, bottom = new_top, new_bottom
            return mu, rho, tau

        wf, wt, vf, vt = ([part(p, q) for p in range(count)] for q in range(4))
        mu, rho, tau = eliminate(range(count), wf, wt, vf, vt)
        nu, omega, sigma = eliminate(reversed(range(count)), vt, vf, wt, wf)
        pick = lambda values, at: sum(jnp.where(at == p, v, nil) for p, v in enumerate(values))
        tau_b, sigma_a = pick(tau, me - 1), pick(sigma, me + 1)
        mu_me, nu_me = pick(mu, me), pick(nu, me)
        wf, wt, vf, vt = (part(me, q) for q in range(4))
        det = 1.0 / ((1.0 - tau_b * wf) * (1.0 - sigma_a * vt) - (tau_b * vf) * (sigma_a * wt))
        k11, k12 = (1.0 - sigma_a * vt) * det, tau_b * vf * det
        k21, k22 = sigma_a * wt * det, (1.0 - tau_b * wf) * det
        low, high = [None] * count, [None] * count
        for p in reversed(range(count)):
            onward = -rho[p + 1] * low[p + 1] if p + 1 < count else nil
            low[p] = jnp.where(me - 1 == p, unit, jnp.where(p < me - 1, onward, nil))
        for p in range(count):
            onward = -omega[p - 1] * high[p - 1] if p else nil
            high[p] = jnp.where(me + 1 == p, unit, jnp.where(p > me + 1, onward, nil))
        table = reduced[axis]

        def put(index, value):
            for t in every:
                table[index, pl.ds(t * UNIT, UNIT), :] = jnp.broadcast_to(value[t:t + 1], (UNIT, LANES))

        for p in range(count):
            put(p, k11 * low[p] + k12 * high[p] + jnp.where(me == p, -k11 * tau_b, nil))
            put(count + 1 + p, k21 * low[p] + k22 * high[p] + jnp.where(me == p, -k21 * tau_b, nil))
        put(count, -k12 * sigma_a)
        put(2 * count + 1, -k22 * sigma_a)
        put(2 * count + 2, mu_me)
        put(2 * count + 3, nu_me)
        if axis == X:
            for p in range(count):
                put(2 * count + 4 + p, jnp.where(p < me, mu[p], unit))
                put(3 * count + 4 + p, jnp.where(p < me, unit, jnp.where(p > me, nu[p], nil)))

    def publish(axis, stage, c, g):
        count, table, way = parts[axis], reduced[axis], lax.rem(stage, 2)
        head, tail = exch[axis][way, c, g, pos[axis]], gt[c, g]
        send[axis][c, g, 1] = tail + table[2 * count + 2] * head
        send[axis][c, g, 0] = head + table[2 * count + 3] * tail
        for other in others(axis):
            sel = jnp.where(other > pos[axis], 1, 0)
            pltpu.make_async_remote_copy(
                src_ref=send[axis].at[c, g, sel], dst_ref=exch[axis].at[way, c, g, pos[axis]],
                send_sem=send_sem.at[c, g], recv_sem=recv[axis].at[way, c, g],
                device_id=device(axis, other), device_id_type=LOGICAL).start()

    def combine(axis, way, c, g, g_ss=0):
        count, table = parts[axis], reduced[axis]
        for side in range(2):
            base = side * (count + 1)
            terms = [table[base + count] * gt[c, g]] + [table[base + p] * exch[axis][way, c, g, p] for p in range(count)]
            while len(terms) > 1:
                terms = [a + b for a, b in zip(terms[::2], terms[1::2])] + terms[len(terms) // 2 * 2:]
            ss[g_ss, side] = terms[0]

    def neighbours(axis, stage, c, g, g_ss=0):
        way = lax.rem(stage, 2)
        arrived = exch[axis].at[way, c, g, pl.ds(0, parts[axis] - 1)]
        pltpu.make_async_copy(arrived, arrived, recv[axis].at[way, c, g]).wait()
        pltpu.make_async_copy(arrived, arrived, send_sem.at[c, g]).wait()
        combine(axis, way, c, g, g_ss)

    def publish_raw(c, g):
        raw[c, g, pos[X], 0] = exch[X][0, c, g, pos[X]]
        raw[c, g, pos[X], 1] = gt[c, g]

        for other in others(X):
            pltpu.make_async_remote_copy(
                src_ref=raw.at[c, g, pos[X]], dst_ref=raw.at[c, g, pos[X]], send_sem=send_sem.at[c, g], recv_sem=recv_x.at[0, c, g],
                device_id=device(X, other), device_id_type=LOGICAL).start()

    def neighbours_raw(c, g):
        arrived = raw.at[c, g, pl.ds(0, parts_x - 1)]
        pltpu.make_async_copy(arrived, arrived, recv_x.at[0, c, g]).wait()
        pltpu.make_async_copy(arrived, arrived, send_sem.at[c, g]).wait()
        count = parts_x
        for p in range(count):
            exch[X][0, c, g, p] = (red_x[2 * count + 4 + p] * raw[c, g, p, 0] + red_x[3 * count + 4 + p] * raw[c, g, p, 1])
        combine(X, 0, c, g)

    def solve_block(axis, minus):
        def coef(array, k, t):
            return array[pl.ds(k * pitch + axis * tiles + t, 1), :]

        def walk(first, sign, count, visit, state):
            def block(g, state):
                line = first + sign * deep * g
                row, coef_row = (line + 1) * PITCH, line * pitch + axis * tiles

                def one(u, state):
                    at = lambda array, t: array[pl.ds(coef_row + t + u * (sign * pitch), 1), :]
                    return visit(pl.ds(row + u * (sign * PITCH), SUB), at, state)

                return lax.fori_loop(0, min(count, deep), one, state, unroll=True)

            return lax.fori_loop(0, max(count // deep, 1), block, state)

        def eliminate(mult):
            def visit(here, at, state):
                values = list(state)
                for t in every:
                    factor = at(mult, t)
                    for c in range(chunks):
                        s = c * tiles + t
                        values[s] = rs[c, t, here, :] + factor * values[s]
                        hs[c, t, here, :] = values[s]
                return tuple(values)
            return visit

        init = tuple(blank for _ in cells)
        ups = walk(0, 1, half, eliminate(ln), init)
        downs = walk(n - 1, -1, half, eliminate(un), init)
        lo, hi = half - 1, half

        def place(c, t, here, value):
            qs[c, t, here, :] = value - rs[c, t, here, :] if minus else value

        low_s, high_s = [], []
        for s, (c, t) in enumerate(cells):
            c_lo, a_hi = coef(cn, lo, t), coef(an, hi, t)
            kappa = 1.0 / (1.0 - c_lo * a_hi)
            h_hi = coef(d2, hi, t) * downs[s]
            s_lo = kappa * (coef(m2, lo, t) * ups[s] + c_lo * h_hi)
            low_s.append(s_lo)
            high_s.append(h_hi + a_hi * s_lo)
            place(c, t, slab(lo), low_s[s])
            place(c, t, slab(hi), high_s[s])

        def substitute(scale, mult):
            def visit(here, at, state):
                values = list(state)
                for t in every:
                    own, factor = at(scale, t), at(mult, t)
                    for c in range(chunks):
                        s = c * tiles + t
                        values[s] = own * hs[c, t, here, :] + factor * values[s]
                        place(c, t, here, values[s])
                return tuple(values)
            return visit

        for first, sign, visit, state in ((lo, -1, substitute(m2, cn), low_s), (hi, 1, substitute(d2, an), high_s)):
            state = walk(first + sign, sign, deep - 1, visit, tuple(state))
            walk(first + sign * deep, sign, half - deep, visit, state)

    def each_unit(body, count=units):
        lax.fori_loop(0, count, lambda u, carry: (body(u // parts_of, lax.rem(u, parts_of)), carry)[1], 0)

    def ends_of(axis, stage, c, g):
        return exch[axis].at[lax.rem(stage, 2), c, g, pos[axis]], gt.at[c, g]

    def start_x(c):
        def unit(g, carry):
            turn(qs, rs, c, Y, X, g * UNIT, UNIT, every, ends_of(X, 0, c, g), correct=False, explicit=True)
            publish_raw(c, g)

            @pl.when((c == 0) & (g == 0))
            def _():
                spread(Y)

            return carry

        await_halo(c)
        lax.fori_loop(0, parts_of, unit, 0)

    def onward(axis, stage, to, to_stage):
        def unit(c, g):
            neighbours(axis, stage, c, g)
            turn(qs, rs, c, axis, to, g * UNIT, UNIT, every, ends_of(to, to_stage, c, g))
            publish(to, to_stage, c, g)

        each_unit(unit)

    each_chunk(start_x)
    solve_block(X, True)
    reduce_lines(X)
    reduce_lines(Y)

    def first_to_y(c, g):
        neighbours_raw(c, g)
        turn(qs, rs, c, X, Y, g * UNIT, UNIT, every, ends_of(Y, 0, c, g))
        publish(Y, 0, c, g)

    each_unit(first_to_y)

    def step(stage, carry):
        solve_block(Y, True)
        onward(Y, stage - 1, X, stage)
        solve_block(X, True)
        onward(X, stage, Y, stage)
        return carry

    lax.fori_loop(1, STEPS, step, 0)
    solve_block(Y, False)

    def finish(c, g):
        neighbours(Y, STEPS - 1, c, g)
        turn(qs, out, c, Y, X, g * UNIT, UNIT, every, scale=0.5, step_out=SUB)

    each_unit(finish, units - parts_of)
    for g in range(parts_of):
        neighbours(Y, STEPS - 1, chunks - 1, g, g)


def finish_kernel(done, qs, w2, v2, ss, out, fresh, sem):
    last, tiles, lines = done.shape[0] - 1, done.shape[1], done.shape[2] // SUB
    pitch = 2 * tiles

    def place(c, t, src, whole=False):
        step = lines if whole else LANES // 2
        for first in range(0, lines, step):
            copy = pltpu.make_async_copy(src.at[pl.ds(first * SUB, step * SUB)].reshape(step, SUB, LANES),
                                         out.at[pl.ds(first, step), pl.ds(c * SUB, SUB), pl.ds(t * LANES, LANES)], sem.at[c * tiles + t])
            if whole:
                copy.wait()
            else:
                copy.start()

    for c in range(last):
        for t in range(tiles):
            place(c, t, done.at[c, t])
    for kt in range(tiles):
        def column(f, carry):
            for lt in range(tiles):
                rows = pl.ds(kt * LANES * pitch + tiles + lt, LANES, stride=pitch)
                block = qs[last, lt, pl.ds((kt * LANES + 1) * PITCH + f, LANES, stride=PITCH), :]
                near, far = (ss[f // UNIT, side, pl.ds(lt * UNIT + f % UNIT, 1), :] for side in range(2))
                block = block + w2[rows, :] * near + v2[rows, :] * far
                fresh[kt, pl.ds(lt * LANES * SUB + f, LANES, stride=SUB), :] = (block * 0.5).T
            return carry

        lax.fori_loop(0, SUB, column, 0, unroll=True)
        place(last, kt, fresh.at[kt])
    for c in range(last + 1):
        for t in range(tiles):
            place(c, t, done.at[c, t] if c < last else fresh.at[t], whole=True)


def solution(mesh):
    parts_x, parts_y = mesh.shape["row"], mesh.shape["col"]
    strides, stride = {}, 1
    for name in reversed(mesh.axis_names):
        strides[name], stride = stride, stride * mesh.shape[name]
    field_spec = P(("batch", "row"), "col", None)
    coeff_spec = P(("batch", "row"), "col")

    def local_steps(field, *coeffs):
        n, fields = field.shape[0], field.shape[2]
        tiles, chunks = n // LANES, fields // SUB
        packed = pltpu.VMEM((n * 2 * tiles, LANES), F32)
        plane = -(-((n + 2) * PITCH - SUB) // (4 * SUB)) * 4 * SUB + SUB
        big = pltpu.VMEM((chunks, tiles, plane, LANES), F32)
        dma = pltpu.SemaphoreType.DMA
        parts_of = SUB // UNIT
        sends = pltpu.VMEM((chunks, parts_of, 2, tiles * UNIT, LANES), F32)
        line = lambda count: pltpu.VMEM((2, chunks, parts_of, count, tiles * UNIT, LANES), F32)
        table = lambda count: pltpu.VMEM((4 * count + 4, tiles * UNIT, LANES), F32)
        small = pltpu.VMEM((2, chunks, tiles, SUB, LANES), F32)
        message = (4 * tiles, LANES)
        scratch = [
            pltpu.VMEM((6, n, n), F32), big, big, *([packed] * 15),
            pltpu.VMEM((2,) + message, F32), pltpu.VMEM((parts_x,) + message, F32), pltpu.VMEM((parts_y,) + message, F32),
            table(parts_x), table(parts_y), sends, sends, line(parts_x), line(parts_y),
            pltpu.VMEM((chunks, parts_of, parts_x, 2, tiles * UNIT, LANES), F32), pltpu.VMEM((chunks, parts_of, tiles * UNIT, LANES), F32),
            small, small, dma, dma, dma((chunks, parts_of)), dma((2, chunks, parts_of)), dma((2, chunks, parts_of)), dma((2,)),
        ]
        in_hbm = pl.BlockSpec(memory_space=pltpu.HBM)
        turned = jnp.transpose(field, (0, 2, 1))
        in_vmem = pl.BlockSpec(memory_space=pltpu.VMEM)
        shape = lambda *dims: jax.ShapeDtypeStruct(dims, F32)
        handed = (shape(chunks, tiles, n * SUB, LANES), shape(chunks, tiles, plane, LANES), shape(n * 2 * tiles, LANES),
                  shape(n * 2 * tiles, LANES), shape(parts_of, 2, tiles * UNIT, LANES))
        handed = pl.pallas_call(
            functools.partial(adi_kernel, (("row", parts_x), ("col", parts_y)), strides),
            out_shape=handed, in_specs=[in_hbm] * 7, out_specs=(in_vmem,) * len(handed), scratch_shapes=scratch,
            compiler_params=pltpu.CompilerParams(
                collective_id=0, has_side_effects=True, vmem_limit_bytes=36 * 1024 * 1024),
            name="adi_steps",
        )(*(pltpu.with_memory_space_constraint(array, pltpu.HBM) for array in (turned,) + coeffs))
        result = pl.pallas_call(
            finish_kernel, out_shape=jax.ShapeDtypeStruct(turned.shape, F32),
            in_specs=[in_vmem] * len(handed), out_specs=in_hbm,
            scratch_shapes=[pltpu.VMEM((tiles, n * SUB, LANES), F32), dma((chunks * tiles,))],
            compiler_params=pltpu.CompilerParams(vmem_limit_bytes=8 * 1024 * 1024), name="finish",
        )(*handed)
        return jnp.transpose(result, (0, 2, 1))

    return jax.shard_map(local_steps, mesh=mesh, in_specs=(field_spec,) + (coeff_spec,) * 6, out_specs=field_spec, check_vma=False)
```

```python
import functools

import jax
import jax.numpy as jnp
from jax import lax
from jax.experimental import pallas as pl
from jax.experimental.pallas import tpu as pltpu
from jax.sharding import PartitionSpec as P

STEPS = 3
F32 = jnp.float32
LANES = 128
SUB = 8
UNIT = SUB // 2
PITCH = SUB + 1
LOGICAL = pl.DeviceIdType.LOGICAL
X, Y = 0, 1


def adi_kernel(axes, strides, field, lower_x, diag_x, upper_x, lower_y, diag_y, upper_y, out, qs, w2, v2, ss,
               nat, rs, hs, pa, pb, pc, nd, md, ne, me_, ln, cn, un, an, m2, d2, r0, rn,
               gs, gc_x, gc_y, red_x, red_y, sx, sy, ex, ey, raw, gt, halo_s, halo_r,
               load_sem, late_sem, send_sem, recv_x, recv_y, gather_sem):
    (row_name, parts_x), (col_name, parts_y) = axes
    n = lower_x.shape[0]
    tiles = n // LANES
    chunks = field.shape[1] // SUB
    parts_of = SUB // UNIT
    units = chunks * parts_of
    pitch = 2 * tiles
    half = n // 2
    pos = (lax.axis_index(row_name), lax.axis_index(col_name))
    parts = (parts_x, parts_y)
    home = sum(lax.axis_index(name) * stride for name, stride in strides.items())
    exch = (ex, ey)
    recv = (recv_x, recv_y)
    send = (sx, sy)
    reduced = (red_x, red_y)
    gather, gather_sends = (gc_x, gc_y), (late_sem, load_sem)

    def device(axis, other):
        return home + (other - pos[axis]) * strides[(row_name, col_name)[axis]]

    def others(axis):
        count = parts[axis]
        offs = sorted(range(1, count), key=lambda off: (-min(off, count - off), -off))
        return [lax.rem(pos[axis] + off, count) for off in offs]

    def field_piece(c, t, first=0, count=n):
        late = c == chunks - 1 and t == tiles - 1 and first > 0
        return pltpu.make_async_copy(field.at[pl.ds(first, count), pl.ds(c * SUB, SUB), pl.ds(t * LANES, LANES)],
                                     out.at[c, t, pl.ds(first * SUB, count * SUB)].reshape(count, SUB, LANES), recv_x.at[1, 0, 0] if late else send_sem.at[c, t])

    def load_field(c):
        for t in range(tiles):
            for first in range(0, n, LANES):
                field_piece(c, t, first, LANES).start()

    def load_coefficients(axis):
        for slot, ref in enumerate(((lower_x, diag_x, upper_x), (lower_y, diag_y, upper_y))[axis]):
            pltpu.make_async_copy(ref, nat.at[3 * axis + slot], (load_sem, late_sem)[axis]).start()

    for c in range(chunks):
        if c == chunks - 1:
            load_coefficients(X)
        load_field(c)
    load_coefficients(Y)

    halo_r[...] = jnp.zeros_like(halo_r)
    barrier = pltpu.get_barrier_semaphore()
    for axis in (X, Y):
        for other in others(axis):
            pl.semaphore_signal(barrier, 1, device_id=device(axis, other), device_id_type=LOGICAL)

    blank = jnp.zeros((SUB, LANES), F32)
    every = tuple(range(tiles))
    cells = [(c, t) for c in range(chunks) for t in range(tiles)]

    def slab(k):
        return pl.ds((k + 1) * PITCH, SUB)

    def each_chunk(body):
        lax.fori_loop(0, chunks, lambda c, carry: (body(c), carry)[1], 0)

    def turn(src, dst, c, axis, to, base, many, lts, ends=None, kts=None, step_in=PITCH, step_out=PITCH, correct=True, explicit=False, scale=None,
             g_ss=0):
        group = 2

        def column(g, carry):
            fs = [g * group + u for u in range(group)]
            for kt in kts or every:
                heads, tails = [None] * group, [None] * group
                for lt in lts:
                    rows = pl.ds(kt * (LANES * pitch) + (axis * tiles + lt), LANES, stride=pitch)
                    if correct:
                        near, far = w2[rows, :], v2[rows, :]
                    if explicit:
                        own, low, high = 2.0 - pb[rows, :], pa[rows, :], pc[rows, :]
                    if ends:
                        rows = pl.ds(lt * LANES * pitch + to * tiles + kt, LANES, stride=pitch)
                        first_row, last_row = r0[rows, :], rn[rows, :]
                    for u, f in enumerate(fs):
                        origin = kt * LANES * step_in + (step_in if step_in == PITCH else 0) + base + f
                        target = lt * LANES * step_out + (step_out if step_out == PITCH else 0) + base + f
                        block = src[c, lt, pl.ds(origin, LANES, stride=step_in), :]
                        if explicit:
                            block = own * block - (low * src[c, lt, pl.ds(origin - step_in, LANES, stride=step_in), :]
                                                   + high * src[c, lt, pl.ds(origin + step_in, LANES, stride=step_in), :])
                        if correct:
                            block = block + near * ss[g_ss, 0, pl.ds(lt * UNIT + f, 1), :] + far * ss[g_ss, 1, pl.ds(lt * UNIT + f, 1), :]
                        if scale is not None:
                            block = block * scale
                        flipped = block.T
                        dst[c, kt, pl.ds(target, LANES, stride=step_out), :] = flipped
                        if ends:
                            fold = lambda v: v.reshape(LANES // SUB, SUB, LANES).sum(axis=0)
                            h, s = fold(flipped * first_row), fold(flipped * last_row)
                            heads[u] = h if heads[u] is None else heads[u] + h
                            tails[u] = s if tails[u] is None else tails[u] + s
                if ends:
                    for u, f in enumerate(fs):
                        ends[0][pl.ds(kt * UNIT + f, 1), :] = jnp.sum(heads[u], axis=0, keepdims=True)
                        ends[1][pl.ds(kt * UNIT + f, 1), :] = jnp.sum(tails[u], axis=0, keepdims=True)
            return carry

        lax.fori_loop(0, many // group, column, 0, unroll=True)

    me_y = pos[Y]
    has_before, has_after = me_y > 0, me_y < parts_y - 1

    def halo(side, c, other):
        return pltpu.make_async_remote_copy(
            src_ref=halo_s.at[side, c], dst_ref=halo_r.at[1 - side, c], send_sem=send_sem.at[c, side], recv_sem=recv_y.at[1, c, 1 - side],
            device_id=device(Y, other), device_id_type=LOGICAL)

    def send_halo(c):
        for t in every:
            halo_s[0, c, t] = qs[c, t, slab(0), :]
            halo_s[1, c, t] = qs[c, t, slab(n - 1), :]

        @pl.when(has_before)
        def _():
            halo(0, c, me_y - 1).start()

        @pl.when(has_after)
        def _():
            halo(1, c, me_y + 1).start()

    def await_halo(c):
        @pl.when(has_before)
        def _():
            halo(0, c, me_y - 1).wait_send()
            halo(1, c, me_y - 1).wait_recv()

        @pl.when(has_after)
        def _():
            halo(1, c, me_y + 1).wait_send()
            halo(0, c, me_y + 1).wait_recv()

        for t in every:
            qs[c, t, slab(-1), :] = halo_r[0, c, t]
            qs[c, t, slab(n), :] = halo_r[1, c, t]

    def pack_x():
        some = nat.at[pl.ds(0, 3)]
        pltpu.make_async_copy(some, some, load_sem).wait()
        for t in range(tiles):
            cols = pl.ds(t * LANES, LANES)
            pa[pl.ds(t, n, stride=pitch), :] = nat[0, :, cols]
            pb[pl.ds(t, n, stride=pitch), :] = nat[1, :, cols] + 1.0
            pc[pl.ds(t, n, stride=pitch), :] = nat[2, :, cols]

    for c in range(chunks):
        if c == chunks - 1:
            pack_x()
        for t in range(tiles):
            if c < chunks - 1 or t < tiles - 1:
                field_piece(c, t).wait()
                turn(out, qs, c, X, Y, 0, SUB, (t,), step_in=SUB, correct=False)
            else:
                for kt in every:
                    field_piece(c, t, kt * LANES, LANES).wait()
                    turn(out, qs, c, X, Y, 0, SUB, (t,), kts=(kt,), step_in=SUB, correct=False)
        if c == 0:
            pl.semaphore_wait(barrier, parts_x + parts_y - 2)
        send_halo(c)
    some = nat.at[pl.ds(3, 3)]
    pltpu.make_async_copy(some, some, late_sem).wait()
    for t in range(tiles):
        cols = pl.ds(t * LANES, LANES)
        for s in range(tiles):
            rows = pl.ds(s * LANES, LANES)
            dest = pl.ds(t * LANES * pitch + tiles + s, LANES, stride=pitch)
            pa[dest, :] = nat[3, rows, cols].T
            pb[dest, :] = nat[4, rows, cols].T + 1.0
            pc[dest, :] = nat[5, rows, cols].T

    long, deep = 16, 16
    zero = jnp.zeros((pitch, LANES), F32)
    one = jnp.ones((pitch, LANES), F32)

    def at_row(k, u):
        return pl.ds(pl.multiple_of(k * (long * pitch), long * pitch) + u * pitch, pitch)

    def pivots(g, state):
        dp, dq, c_prev, ep, eq, a_next = state
        h = n // long - 1 - g
        for u in range(0, long, 2):
            up, next_up = at_row(g, u), at_row(g, u + 1)
            b, t = pb[up, :], pa[up, :] * c_prev
            next_b, next_t = pb[next_up, :], pa[next_up, :] * pc[up, :]
            new = b * dp - t * dq
            newer = (next_b * b - next_t) * dp - (next_b * t) * dq
            nd[up, :], md[up, :], nd[next_up, :], md[next_up, :] = dp, new, new, newer
            dp, dq, c_prev = newer, new, pc[next_up, :]
            down, next_down = at_row(h, long - 1 - u), at_row(h, long - 2 - u)
            b, t = pb[down, :], a_next * pc[down, :]
            next_b, next_t = pb[next_down, :], pa[down, :] * pc[next_down, :]
            new = b * ep - t * eq
            newer = (next_b * b - next_t) * ep - (next_b * t) * eq
            ne[down, :], me_[down, :], ne[next_down, :], me_[next_down, :] = ep, new, new, newer
            ep, eq, a_next = newer, new, pa[next_down, :]
            if u % 8 == 2:
                scale_d, scale_e = 1.0 / dp, 1.0 / ep
            if u % 8 == 6:
                dp, dq, ep, eq = dp * scale_d, dq * scale_d, ep * scale_e, eq * scale_e
        return dp, dq, c_prev, ep, eq, a_next


    low_half = lax.broadcasted_iota(jnp.int32, (SUB, LANES), 0) < pitch
    blocks = n * pitch // SUB
    step_rows = long * pitch // SUB

    def ratios(g, state):
        prev_m, next_d = state
        for u in range(step_rows):
            up = pl.ds(pl.multiple_of(g * (SUB * step_rows), SUB * step_rows) + u * SUB, SUB)
            down = pl.ds(pl.multiple_of((blocks // step_rows - 1 - g) * (SUB * step_rows), SUB * step_rows)
                         + (step_rows - 1 - u) * SUB, SUB)
            minv = nd[up, :] / md[up, :]
            m2[up, :] = minv + minv
            cn[up, :] = -pc[up, :] * minv
            turned = pltpu.roll(minv, pitch, 0)
            ln[up, :] = -pa[up, :] * jnp.where(low_half, prev_m, turned)
            prev_m = turned
            dinv = ne[down, :] / me_[down, :]
            d2[down, :] = dinv + dinv
            an[down, :] = -pa[down, :] * dinv
            turned = pltpu.roll(dinv, pitch, 0)
            un[down, :] = -pc[down, :] * jnp.where(low_half, turned, next_d)
            next_d = turned
        return prev_m, next_d

    stretches = n // long
    state = lax.fori_loop(1, stretches, lambda g, state: (lambda later: (pivots(g, state[0]), later))(ratios(g - 1, state[1])),
                          (pivots(0, (one, zero, zero, one, zero, zero)), (blank, blank)))
    ratios(stretches - 1, state[1])

    first, last = pl.ds(0, pitch), pl.ds((n - 1) * pitch, pitch)

    def products(g, state):
        col0, row0, coln, rown, un_prev, ln_next = state
        h = n // long - 1 - g
        for u in range(long):
            up, down = at_row(g, u), at_row(h, long - 1 - u)
            start = jnp.logical_and(g == 0, u == 0) if u == 0 else None
            f0, f1 = an[up, :], un_prev
            b0, b1 = cn[down, :], ln_next
            if u == 0:
                f0, f1 = jnp.where(start, one, f0), jnp.where(start, one, f1)
                b0, b1 = jnp.where(start, one, b0), jnp.where(start, one, b1)
            col0, row0, coln, rown = col0 * f0, row0 * f1, coln * b0, rown * b1
            w2[up, :], r0[up, :], v2[down, :], rn[down, :] = col0, row0, coln, rown
            un_prev, ln_next = un[up, :], ln[down, :]
        return col0, row0, coln, rown, un_prev, ln_next

    d_first, m_last = 0.5 * d2[first, :], 0.5 * m2[last, :]
    lax.fori_loop(0, n // long, products,
                  (-pa[first, :] * d2[first, :], d_first, -pc[last, :] * m2[last, :], m_last, one, one))

    def spread(axis):
        for q, (ref, line) in enumerate(((w2, 0), (w2, n - 1), (v2, 0), (v2, n - 1))):
            gs[axis, pl.ds(q * tiles, tiles), :] = -0.5 * ref[pl.ds(line * pitch + axis * tiles, tiles), :]
        gather[axis][pos[axis]] = gs[axis]
        for other in others(axis):
            pltpu.make_async_remote_copy(
                src_ref=gs.at[axis], dst_ref=gather[axis].at[pos[axis]], send_sem=gather_sends[axis], recv_sem=gather_sem.at[axis],
                device_id=device(axis, other), device_id_type=LOGICAL).start()

    spread(X)

    def reduce_lines(axis):
        count, me = parts[axis], pos[axis]
        arrived = gather[axis].at[pl.ds(0, count - 1)]
        pltpu.make_async_copy(arrived, arrived, gather_sem.at[axis]).wait()
        pltpu.make_async_copy(arrived, arrived, gather_sends[axis]).wait()
        part = lambda p, q: gather[axis][p, pl.ds(q * tiles, tiles), :]
        nil = jnp.zeros((tiles, LANES), F32)
        unit = jnp.ones((tiles, LANES), F32)

        def eliminate(order, wf, wt, vf, vt):
            mu, rho, tau = [None] * count, [None] * count, [None] * count
            top, bottom = nil, unit
            for p in order:
                new_top = vt[p] * bottom + (wt[p] * vf[p] - vt[p] * wf[p]) * top
                new_bottom = bottom - wf[p] * top
                inverse = 1.0 / new_bottom
                mu[p], rho[p], tau[p] = wt[p] * top * inverse, wt[p] * bottom * inverse, new_top * inverse
                top, bottom = new_top, new_bottom
            return mu, rho, tau

        wf, wt, vf, vt = ([part(p, q) for p in range(count)] for q in range(4))
        mu, rho, tau = eliminate(range(count), wf, wt, vf, vt)
        nu, omega, sigma = eliminate(reversed(range(count)), vt, vf, wt, wf)
        pick = lambda values, at: sum(jnp.where(at == p, v, nil) for p, v in enumerate(values))
        tau_b, sigma_a = pick(tau, me - 1), pick(sigma, me + 1)
        mu_me, nu_me = pick(mu, me), pick(nu, me)
        wf, wt, vf, vt = (part(me, q) for q in range(4))
        det = 1.0 / ((1.0 - tau_b * wf) * (1.0 - sigma_a * vt) - (tau_b * vf) * (sigma_a * wt))
        k11, k12 = (1.0 - sigma_a * vt) * det, tau_b * vf * det
        k21, k22 = sigma_a * wt * det, (1.0 - tau_b * wf) * det
        low, high = [None] * count, [None] * count
        for p in reversed(range(count)):
            onward = -rho[p + 1] * low[p + 1] if p + 1 < count else nil
            low[p] = jnp.where(me - 1 == p, unit, jnp.where(p < me - 1, onward, nil))
        for p in range(count):
            onward = -omega[p - 1] * high[p - 1] if p else nil
            high[p] = jnp.where(me + 1 == p, unit, jnp.where(p > me + 1, onward, nil))
        table = reduced[axis]

        def put(index, value):
            for t in every:
                table[index, pl.ds(t * UNIT, UNIT), :] = jnp.broadcast_to(value[t:t + 1], (UNIT, LANES))

        for p in range(count):
            put(p, k11 * low[p] + k12 * high[p] + jnp.where(me == p, -k11 * tau_b, nil))
            put(count + 1 + p, k21 * low[p] + k22 * high[p] + jnp.where(me == p, -k21 * tau_b, nil))
        put(count, -k12 * sigma_a)
        put(2 * count + 1, -k22 * sigma_a)
        put(2 * count + 2, mu_me)
        put(2 * count + 3, nu_me)
        if axis == X:
            for p in range(count):
                put(2 * count + 4 + p, jnp.where(p < me, mu[p], unit))
                put(3 * count + 4 + p, jnp.where(p < me, unit, jnp.where(p > me, nu[p], nil)))

    def publish(axis, stage, c, g):
        count, table, way = parts[axis], reduced[axis], lax.rem(stage, 2)
        head, tail = exch[axis][way, c, g, pos[axis]], gt[c, g]
        send[axis][c, g, 1] = tail + table[2 * count + 2] * head
        send[axis][c, g, 0] = head + table[2 * count + 3] * tail
        for other in others(axis):
            sel = jnp.where(other > pos[axis], 1, 0)
            pltpu.make_async_remote_copy(
                src_ref=send[axis].at[c, g, sel], dst_ref=exch[axis].at[way, c, g, pos[axis]],
                send_sem=send_sem.at[c, g], recv_sem=recv[axis].at[way, c, g],
                device_id=device(axis, other), device_id_type=LOGICAL).start()

    def combine(axis, way, c, g, g_ss=0):
        count, table = parts[axis], reduced[axis]
        for side in range(2):
            base = side * (count + 1)
            terms = [table[base + count] * gt[c, g]] + [table[base + p] * exch[axis][way, c, g, p] for p in range(count)]
            while len(terms) > 1:
                terms = [a + b for a, b in zip(terms[::2], terms[1::2])] + terms[len(terms) // 2 * 2:]
            ss[g_ss, side] = terms[0]

    def neighbours(axis, stage, c, g, g_ss=0):
        way = lax.rem(stage, 2)
        arrived = exch[axis].at[way, c, g, pl.ds(0, parts[axis] - 1)]
        pltpu.make_async_copy(arrived, arrived, recv[axis].at[way, c, g]).wait()
        combine(axis, way, c, g, g_ss)
        pltpu.make_async_copy(arrived, arrived, send_sem.at[c, g]).wait()

    def publish_raw(c, g):
        raw[c, g, pos[X], 0] = exch[X][0, c, g, pos[X]]
        raw[c, g, pos[X], 1] = gt[c, g]

        for other in others(X):
            pltpu.make_async_remote_copy(
                src_ref=raw.at[c, g, pos[X]], dst_ref=raw.at[c, g, pos[X]], send_sem=send_sem.at[c, g], recv_sem=recv_x.at[0, c, g],
                device_id=device(X, other), device_id_type=LOGICAL).start()

    def neighbours_raw(c, g):
        arrived = raw.at[c, g, pl.ds(0, parts_x - 1)]
        pltpu.make_async_copy(arrived, arrived, recv_x.at[0, c, g]).wait()
        pltpu.make_async_copy(arrived, arrived, send_sem.at[c, g]).wait()
        count = parts_x
        for p in range(count):
            exch[X][0, c, g, p] = (red_x[2 * count + 4 + p] * raw[c, g, p, 0] + red_x[3 * count + 4 + p] * raw[c, g, p, 1])
        combine(X, 0, c, g)

    def solve_block(axis, minus):
        def coef(array, k, t):
            return array[pl.ds(k * pitch + axis * tiles + t, 1), :]

        def walk(first, sign, count, visit, state):
            def block(g, state):
                line = first + sign * deep * g
                row, coef_row = (line + 1) * PITCH, line * pitch + axis * tiles

                def one(u, state):
                    at = lambda array, t: array[pl.ds(coef_row + t + u * (sign * pitch), 1), :]
                    return visit(pl.ds(row + u * (sign * PITCH), SUB), at, state)

                return lax.fori_loop(0, min(count, deep), one, state, unroll=True)

            return lax.fori_loop(0, max(count // deep, 1), block, state)

        def eliminate(mult):
            def visit(here, at, state):
                values = list(state)
                for t in every:
                    factor = at(mult, t)
                    for c in range(chunks):
                        s = c * tiles + t
                        values[s] = rs[c, t, here, :] + factor * values[s]
                        hs[c, t, here, :] = values[s]
                return tuple(values)
            return visit

        init = tuple(blank for _ in cells)
        ups = walk(0, 1, half, eliminate(ln), init)
        downs = walk(n - 1, -1, half, eliminate(un), init)
        lo, hi = half - 1, half

        def place(c, t, here, value):
            qs[c, t, here, :] = value - rs[c, t, here, :] if minus else value

        low_s, high_s = [], []
        for s, (c, t) in enumerate(cells):
            c_lo, a_hi = coef(cn, lo, t), coef(an, hi, t)
            kappa = 1.0 / (1.0 - c_lo * a_hi)
            h_hi = coef(d2, hi, t) * downs[s]
            s_lo = kappa * (coef(m2, lo, t) * ups[s] + c_lo * h_hi)
            low_s.append(s_lo)
            high_s.append(h_hi + a_hi * s_lo)
            place(c, t, slab(lo), low_s[s])
            place(c, t, slab(hi), high_s[s])

        def substitute(scale, mult):
            def visit(here, at, state):
                values = list(state)
                for t in every:
                    own, factor = at(scale, t), at(mult, t)
                    for c in range(chunks):
                        s = c * tiles + t
                        values[s] = own * hs[c, t, here, :] + factor * values[s]
                        place(c, t, here, values[s])
                return tuple(values)
            return visit

        for first, sign, visit, state in ((lo, -1, substitute(m2, cn), low_s), (hi, 1, substitute(d2, an), high_s)):
            state = walk(first + sign, sign, deep - 1, visit, tuple(state))
            walk(first + sign * deep, sign, half - deep, visit, state)

    def each_unit(body, count=units):
        lax.fori_loop(0, count, lambda u, carry: (body(u // parts_of, lax.rem(u, parts_of)), carry)[1], 0)

    def ends_of(axis, stage, c, g):
        return exch[axis].at[lax.rem(stage, 2), c, g, pos[axis]], gt.at[c, g]

    def start_x(c):
        def unit(g, carry):
            turn(qs, rs, c, Y, X, g * UNIT, UNIT, every, ends_of(X, 0, c, g), correct=False, explicit=True)
            publish_raw(c, g)

            @pl.when((c == 0) & (g == 0))
            def _():
                spread(Y)

            return carry

        await_halo(c)
        lax.fori_loop(0, parts_of, unit, 0)

    def onward(axis, stage, to, to_stage):
        def unit(c, g):
            neighbours(axis, stage, c, g)
            turn(qs, rs, c, axis, to, g * UNIT, UNIT, every, ends_of(to, to_stage, c, g))
            publish(to, to_stage, c, g)

        each_unit(unit)

    each_chunk(start_x)
    solve_block(X, True)
    reduce_lines(X)
    reduce_lines(Y)

    def first_to_y(c, g):
        neighbours_raw(c, g)
        turn(qs, rs, c, X, Y, g * UNIT, UNIT, every, ends_of(Y, 0, c, g))
        publish(Y, 0, c, g)

    each_unit(first_to_y)

    def step(stage, carry):
        solve_block(Y, True)
        onward(Y, stage - 1, X, stage)
        solve_block(X, True)
        onward(X, stage, Y, stage)
        return carry

    lax.fori_loop(1, STEPS, step, 0)
    solve_block(Y, False)

    def finish(c, g):
        neighbours(Y, STEPS - 1, c, g)
        turn(qs, out, c, Y, X, g * UNIT, UNIT, every, scale=0.5, step_out=SUB)

    each_unit(finish, units - parts_of)
    for g in range(parts_of):
        neighbours(Y, STEPS - 1, chunks - 1, g, g)


def finish_kernel(done, qs, w2, v2, ss, out, fresh, sem):
    last, tiles, lines = done.shape[0] - 1, done.shape[1], done.shape[2] // SUB
    pitch = 2 * tiles

    def place(c, t, src, whole=False):
        step = lines if whole else LANES // 2
        for first in range(0, lines, step):
            copy = pltpu.make_async_copy(src.at[pl.ds(first * SUB, step * SUB)].reshape(step, SUB, LANES),
                                         out.at[pl.ds(first, step), pl.ds(c * SUB, SUB), pl.ds(t * LANES, LANES)], sem.at[c * tiles + t])
            if whole:
                copy.wait()
            else:
                copy.start()

    for c in range(last):
        for t in range(tiles):
            place(c, t, done.at[c, t])
    for kt in range(tiles):
        def column(f, carry):
            for lt in range(tiles):
                rows = pl.ds(kt * LANES * pitch + tiles + lt, LANES, stride=pitch)
                block = qs[last, lt, pl.ds((kt * LANES + 1) * PITCH + f, LANES, stride=PITCH), :]
                near, far = (ss[f // UNIT, side, pl.ds(lt * UNIT + f % UNIT, 1), :] for side in range(2))
                block = block + w2[rows, :] * near + v2[rows, :] * far
                fresh[kt, pl.ds(lt * LANES * SUB + f, LANES, stride=SUB), :] = (block * 0.5).T
            return carry

        lax.fori_loop(0, SUB, column, 0, unroll=True)
        place(last, kt, fresh.at[kt])
    for c in range(last + 1):
        for t in range(tiles):
            place(c, t, done.at[c, t] if c < last else fresh.at[t], whole=True)


def solution(mesh):
    parts_x, parts_y = mesh.shape["row"], mesh.shape["col"]
    strides, stride = {}, 1
    for name in reversed(mesh.axis_names):
        strides[name], stride = stride, stride * mesh.shape[name]
    field_spec = P(("batch", "row"), "col", None)
    coeff_spec = P(("batch", "row"), "col")

    def local_steps(field, *coeffs):
        n, fields = field.shape[0], field.shape[2]
        tiles, chunks = n // LANES, fields // SUB
        packed = pltpu.VMEM((n * 2 * tiles, LANES), F32)
        plane = -(-((n + 2) * PITCH - SUB) // (4 * SUB)) * 4 * SUB + SUB
        big = pltpu.VMEM((chunks, tiles, plane, LANES), F32)
        dma = pltpu.SemaphoreType.DMA
        parts_of = SUB // UNIT
        sends = pltpu.VMEM((chunks, parts_of, 2, tiles * UNIT, LANES), F32)
        line = lambda count: pltpu.VMEM((2, chunks, parts_of, count, tiles * UNIT, LANES), F32)
        table = lambda count: pltpu.VMEM((4 * count + 4, tiles * UNIT, LANES), F32)
        small = pltpu.VMEM((2, chunks, tiles, SUB, LANES), F32)
        message = (4 * tiles, LANES)
        scratch = [
            pltpu.VMEM((6, n, n), F32), big, big, *([packed] * 15),
            pltpu.VMEM((2,) + message, F32), pltpu.VMEM((parts_x,) + message, F32), pltpu.VMEM((parts_y,) + message, F32),
            table(parts_x), table(parts_y), sends, sends, line(parts_x), line(parts_y),
            pltpu.VMEM((chunks, parts_of, parts_x, 2, tiles * UNIT, LANES), F32), pltpu.VMEM((chunks, parts_of, tiles * UNIT, LANES), F32),
            small, small, dma, dma, dma((chunks, parts_of)), dma((2, chunks, parts_of)), dma((2, chunks, parts_of)), dma((2,)),
        ]
        in_hbm = pl.BlockSpec(memory_space=pltpu.HBM)
        turned = jnp.transpose(field, (0, 2, 1))
        in_vmem = pl.BlockSpec(memory_space=pltpu.VMEM)
        shape = lambda *dims: jax.ShapeDtypeStruct(dims, F32)
        handed = (shape(chunks, tiles, n * SUB, LANES), shape(chunks, tiles, plane, LANES), shape(n * 2 * tiles, LANES),
                  shape(n * 2 * tiles, LANES), shape(parts_of, 2, tiles * UNIT, LANES))
        handed = pl.pallas_call(
            functools.partial(adi_kernel, (("row", parts_x), ("col", parts_y)), strides),
            out_shape=handed, in_specs=[in_hbm] * 7, out_specs=(in_vmem,) * len(handed), scratch_shapes=scratch,
            compiler_params=pltpu.CompilerParams(
                collective_id=0, has_side_effects=True, vmem_limit_bytes=36 * 1024 * 1024),
            name="adi_steps",
        )(*(pltpu.with_memory_space_constraint(array, pltpu.HBM) for array in (turned,) + coeffs))
        result = pl.pallas_call(
            finish_kernel, out_shape=jax.ShapeDtypeStruct(turned.shape, F32),
            in_specs=[in_vmem] * len(handed), out_specs=in_hbm,
            scratch_shapes=[pltpu.VMEM((tiles, n * SUB, LANES), F32), dma((chunks * tiles,))],
            compiler_params=pltpu.CompilerParams(vmem_limit_bytes=8 * 1024 * 1024), name="finish",
        )(*handed)
        return jnp.transpose(result, (0, 2, 1))

    return jax.shard_map(local_steps, mesh=mesh, in_specs=(field_spec,) + (coeff_spec,) * 6, out_specs=field_spec, check_vma=False)
```

```python
import functools

import jax
import jax.numpy as jnp
from jax import lax
from jax.experimental import pallas as pl
from jax.experimental.pallas import tpu as pltpu
from jax.sharding import PartitionSpec as P

STEPS = 3
F32 = jnp.float32
LANES = 128
SUB = 8
UNIT = SUB // 2
PITCH = SUB + 1
LOGICAL = pl.DeviceIdType.LOGICAL
X, Y = 0, 1


def adi_kernel(axes, strides, field, lower_x, diag_x, upper_x, lower_y, diag_y, upper_y, out, qs, w2, v2, ss,
               nat, rs, hs, pa, pb, pc, nd, md, ne, me_, ln, cn, un, an, m2, d2, r0, rn,
               gs, gc_x, gc_y, red_x, red_y, sx, sy, ex, ey, raw, gt, halo_s, halo_r,
               load_sem, late_sem, send_sem, recv_x, recv_y, gather_sem):
    (row_name, parts_x), (col_name, parts_y) = axes
    n = lower_x.shape[0]
    tiles = n // LANES
    chunks = field.shape[1] // SUB
    parts_of = SUB // UNIT
    units = chunks * parts_of
    pitch = 2 * tiles
    half = n // 2
    pos = (lax.axis_index(row_name), lax.axis_index(col_name))
    parts = (parts_x, parts_y)
    home = sum(lax.axis_index(name) * stride for name, stride in strides.items())
    exch = (ex, ey)
    recv = (recv_x, recv_y)
    send = (sx, sy)
    reduced = (red_x, red_y)
    gather, gather_sends = (gc_x, gc_y), (late_sem, load_sem)

    def device(axis, other):
        return home + (other - pos[axis]) * strides[(row_name, col_name)[axis]]

    def others(axis):
        count = parts[axis]
        offs = sorted(range(1, count), key=lambda off: (-min(off, count - off), -off))
        return [lax.rem(pos[axis] + off, count) for off in offs]

    def field_piece(c, t, first=0, count=n):
        late = c == chunks - 1 and t == tiles - 1 and first > 0
        return pltpu.make_async_copy(field.at[pl.ds(first, count), pl.ds(c * SUB, SUB), pl.ds(t * LANES, LANES)],
                                     out.at[c, t, pl.ds(first * SUB, count * SUB)].reshape(count, SUB, LANES), recv_x.at[1, 0, 0] if late else send_sem.at[c, t])

    def load_field(c):
        for t in range(tiles):
            for first in range(0, n, LANES):
                field_piece(c, t, first, LANES).start()

    def load_coefficients(axis):
        for slot, ref in enumerate(((lower_x, diag_x, upper_x), (lower_y, diag_y, upper_y))[axis]):
            pltpu.make_async_copy(ref, nat.at[3 * axis + slot], (load_sem, late_sem)[axis]).start()

    for c in range(chunks):
        if c == chunks - 1:
            load_coefficients(X)
        load_field(c)
    load_coefficients(Y)

    halo_r[...] = jnp.zeros_like(halo_r)
    barrier = pltpu.get_barrier_semaphore()
    for axis in (X, Y):
        for other in others(axis):
            pl.semaphore_signal(barrier, 1, device_id=device(axis, other), device_id_type=LOGICAL)

    blank = jnp.zeros((SUB, LANES), F32)
    every = tuple(range(tiles))
    cells = [(c, t) for c in range(chunks) for t in range(tiles)]

    def slab(k):
        return pl.ds((k + 1) * PITCH, SUB)

    def each_chunk(body):
        lax.fori_loop(0, chunks, lambda c, carry: (body(c), carry)[1], 0)

    def turn(src, dst, c, axis, to, base, many, lts, ends=None, kts=None, step_in=PITCH, step_out=PITCH, correct=True, explicit=False, scale=None,
             g_ss=0):
        group = 2

        def column(g, carry):
            fs = [g * group + u for u in range(group)]
            sums = {}
            for kt in kts or every:
                heads, tails = [None] * group, [None] * group
                sums[kt] = heads, tails
                for lt in lts:
                    rows = pl.ds(kt * (LANES * pitch) + (axis * tiles + lt), LANES, stride=pitch)
                    if correct:
                        near, far = w2[rows, :], v2[rows, :]
                    if explicit:
                        own, low, high = 2.0 - pb[rows, :], pa[rows, :], pc[rows, :]
                    if ends:
                        rows = pl.ds(lt * LANES * pitch + to * tiles + kt, LANES, stride=pitch)
                        first_row, last_row = r0[rows, :], rn[rows, :]
                    for u, f in enumerate(fs):
                        origin = kt * LANES * step_in + (step_in if step_in == PITCH else 0) + base + f
                        target = lt * LANES * step_out + (step_out if step_out == PITCH else 0) + base + f
                        block = src[c, lt, pl.ds(origin, LANES, stride=step_in), :]
                        if explicit:
                            block = own * block - (low * src[c, lt, pl.ds(origin - step_in, LANES, stride=step_in), :]
                                                   + high * src[c, lt, pl.ds(origin + step_in, LANES, stride=step_in), :])
                        if correct:
                            block = block + near * ss[g_ss, 0, pl.ds(lt * UNIT + f, 1), :] + far * ss[g_ss, 1, pl.ds(lt * UNIT + f, 1), :]
                        if scale is not None:
                            block = block * scale
                        flipped = block.T
                        dst[c, kt, pl.ds(target, LANES, stride=step_out), :] = flipped
                        if ends:
                            fold = lambda v: v.reshape(LANES // SUB, SUB, LANES).sum(axis=0)
                            h, s = fold(flipped * first_row), fold(flipped * last_row)
                            heads[u] = h if heads[u] is None else heads[u] + h
                            tails[u] = s if tails[u] is None else tails[u] + s
            if ends:
                for kt, (heads, tails) in sums.items():
                    for u, f in enumerate(fs):
                        ends[0][pl.ds(kt * UNIT + f, 1), :] = jnp.sum(heads[u], axis=0, keepdims=True)
                        ends[1][pl.ds(kt * UNIT + f, 1), :] = jnp.sum(tails[u], axis=0, keepdims=True)
            return carry

        lax.fori_loop(0, many // group, column, 0, unroll=True)

    me_y = pos[Y]
    has_before, has_after = me_y > 0, me_y < parts_y - 1

    def halo(side, c, other):
        return pltpu.make_async_remote_copy(
            src_ref=halo_s.at[side, c], dst_ref=halo_r.at[1 - side, c], send_sem=send_sem.at[c, side], recv_sem=recv_y.at[1, c, 1 - side],
            device_id=device(Y, other), device_id_type=LOGICAL)

    def send_halo(c):
        for t in every:
            halo_s[0, c, t] = qs[c, t, slab(0), :]
            halo_s[1, c, t] = qs[c, t, slab(n - 1), :]

        @pl.when(has_before)
        def _():
            halo(0, c, me_y - 1).start()

        @pl.when(has_after)
        def _():
            halo(1, c, me_y + 1).start()

    def await_halo(c):
        @pl.when(has_before)
        def _():
            halo(0, c, me_y - 1).wait_send()
            halo(1, c, me_y - 1).wait_recv()

        @pl.when(has_after)
        def _():
            halo(1, c, me_y + 1).wait_send()
            halo(0, c, me_y + 1).wait_recv()

        for t in every:
            qs[c, t, slab(-1), :] = halo_r[0, c, t]
            qs[c, t, slab(n), :] = halo_r[1, c, t]

    def pack_x():
        some = nat.at[pl.ds(0, 3)]
        pltpu.make_async_copy(some, some, load_sem).wait()
        for t in range(tiles):
            cols = pl.ds(t * LANES, LANES)
            pa[pl.ds(t, n, stride=pitch), :] = nat[0, :, cols]
            pb[pl.ds(t, n, stride=pitch), :] = nat[1, :, cols] + 1.0
            pc[pl.ds(t, n, stride=pitch), :] = nat[2, :, cols]

    for c in range(chunks):
        if c == chunks - 1:
            pack_x()
        for t in range(tiles):
            if c < chunks - 1 or t < tiles - 1:
                field_piece(c, t).wait()
                turn(out, qs, c, X, Y, 0, SUB, (t,), step_in=SUB, correct=False)
            else:
                for kt in every:
                    field_piece(c, t, kt * LANES, LANES).wait()
                    turn(out, qs, c, X, Y, 0, SUB, (t,), kts=(kt,), step_in=SUB, correct=False)
        if c == 0:
            pl.semaphore_wait(barrier, parts_x + parts_y - 2)
        send_halo(c)
    some = nat.at[pl.ds(3, 3)]
    pltpu.make_async_copy(some, some, late_sem).wait()
    for t in range(tiles):
        cols = pl.ds(t * LANES, LANES)
        for s in range(tiles):
            rows = pl.ds(s * LANES, LANES)
            dest = pl.ds(t * LANES * pitch + tiles + s, LANES, stride=pitch)
            pa[dest, :] = nat[3, rows, cols].T
            pb[dest, :] = nat[4, rows, cols].T + 1.0
            pc[dest, :] = nat[5, rows, cols].T

    long, deep = 16, 16
    zero = jnp.zeros((pitch, LANES), F32)
    one = jnp.ones((pitch, LANES), F32)

    def at_row(k, u):
        return pl.ds(pl.multiple_of(k * (long * pitch), long * pitch) + u * pitch, pitch)

    def pivots(g, state):
        dp, dq, c_prev, ep, eq, a_next = state
        h = n // long - 1 - g
        for u in range(0, long, 2):
            up, next_up = at_row(g, u), at_row(g, u + 1)
            b, t = pb[up, :], pa[up, :] * c_prev
            next_b, next_t = pb[next_up, :], pa[next_up, :] * pc[up, :]
            new = b * dp - t * dq
            newer = (next_b * b - next_t) * dp - (next_b * t) * dq
            nd[up, :], md[up, :], nd[next_up, :], md[next_up, :] = dp, new, new, newer
            dp, dq, c_prev = newer, new, pc[next_up, :]
            down, next_down = at_row(h, long - 1 - u), at_row(h, long - 2 - u)
            b, t = pb[down, :], a_next * pc[down, :]
            next_b, next_t = pb[next_down, :], pa[down, :] * pc[next_down, :]
            new = b * ep - t * eq
            newer = (next_b * b - next_t) * ep - (next_b * t) * eq
            ne[down, :], me_[down, :], ne[next_down, :], me_[next_down, :] = ep, new, new, newer
            ep, eq, a_next = newer, new, pa[next_down, :]
            if u % 8 == 2:
                scale_d, scale_e = 1.0 / dp, 1.0 / ep
            if u % 8 == 6:
                dp, dq, ep, eq = dp * scale_d, dq * scale_d, ep * scale_e, eq * scale_e
        return dp, dq, c_prev, ep, eq, a_next


    low_half = lax.broadcasted_iota(jnp.int32, (SUB, LANES), 0) < pitch
    blocks = n * pitch // SUB
    step_rows = long * pitch // SUB

    def ratios(g, state):
        prev_m, next_d = state
        for u in range(step_rows):
            up = pl.ds(pl.multiple_of(g * (SUB * step_rows), SUB * step_rows) + u * SUB, SUB)
            down = pl.ds(pl.multiple_of((blocks // step_rows - 1 - g) * (SUB * step_rows), SUB * step_rows)
                         + (step_rows - 1 - u) * SUB, SUB)
            minv = nd[up, :] / md[up, :]
            m2[up, :] = minv + minv
            cn[up, :] = -pc[up, :] * minv
            turned = pltpu.roll(minv, pitch, 0)
            ln[up, :] = -pa[up, :] * jnp.where(low_half, prev_m, turned)
            prev_m = turned
            dinv = ne[down, :] / me_[down, :]
            d2[down, :] = dinv + dinv
            an[down, :] = -pa[down, :] * dinv
            turned = pltpu.roll(dinv, pitch, 0)
            un[down, :] = -pc[down, :] * jnp.where(low_half, turned, next_d)
            next_d = turned
        return prev_m, next_d

    stretches = n // long
    state = lax.fori_loop(1, stretches, lambda g, state: (lambda later: (pivots(g, state[0]), later))(ratios(g - 1, state[1])),
                          (pivots(0, (one, zero, zero, one, zero, zero)), (blank, blank)))
    ratios(stretches - 1, state[1])

    first, last = pl.ds(0, pitch), pl.ds((n - 1) * pitch, pitch)

    def products(g, state):
        col0, row0, coln, rown, un_prev, ln_next = state
        h = n // long - 1 - g
        for u in range(long):
            up, down = at_row(g, u), at_row(h, long - 1 - u)
            start = jnp.logical_and(g == 0, u == 0) if u == 0 else None
            f0, f1 = an[up, :], un_prev
            b0, b1 = cn[down, :], ln_next
            if u == 0:
                f0, f1 = jnp.where(start, one, f0), jnp.where(start, one, f1)
                b0, b1 = jnp.where(start, one, b0), jnp.where(start, one, b1)
            col0, row0, coln, rown = col0 * f0, row0 * f1, coln * b0, rown * b1
            w2[up, :], r0[up, :], v2[down, :], rn[down, :] = col0, row0, coln, rown
            un_prev, ln_next = un[up, :], ln[down, :]
        return col0, row0, coln, rown, un_prev, ln_next

    d_first, m_last = 0.5 * d2[first, :], 0.5 * m2[last, :]
    lax.fori_loop(0, n // long, products,
                  (-pa[first, :] * d2[first, :], d_first, -pc[last, :] * m2[last, :], m_last, one, one))

    def spread(axis):
        for q, (ref, line) in enumerate(((w2, 0), (w2, n - 1), (v2, 0), (v2, n - 1))):
            gs[axis, pl.ds(q * tiles, tiles), :] = -0.5 * ref[pl.ds(line * pitch + axis * tiles, tiles), :]
        gather[axis][pos[axis]] = gs[axis]
        for other in others(axis):
            pltpu.make_async_remote_copy(
                src_ref=gs.at[axis], dst_ref=gather[axis].at[pos[axis]], send_sem=gather_sends[axis], recv_sem=gather_sem.at[axis],
                device_id=device(axis, other), device_id_type=LOGICAL).start()

    spread(X)

    def reduce_lines(axis):
        count, me = parts[axis], pos[axis]
        arrived = gather[axis].at[pl.ds(0, count - 1)]
        pltpu.make_async_copy(arrived, arrived, gather_sem.at[axis]).wait()
        pltpu.make_async_copy(arrived, arrived, gather_sends[axis]).wait()
        part = lambda p, q: gather[axis][p, pl.ds(q * tiles, tiles), :]
        nil = jnp.zeros((tiles, LANES), F32)
        unit = jnp.ones((tiles, LANES), F32)

        def eliminate(order, wf, wt, vf, vt):
            mu, rho, tau = [None] * count, [None] * count, [None] * count
            top, bottom = nil, unit
            for p in order:
                new_top = vt[p] * bottom + (wt[p] * vf[p] - vt[p] * wf[p]) * top
                new_bottom = bottom - wf[p] * top
                inverse = 1.0 / new_bottom
                mu[p], rho[p], tau[p] = wt[p] * top * inverse, wt[p] * bottom * inverse, new_top * inverse
                top, bottom = new_top, new_bottom
            return mu, rho, tau

        wf, wt, vf, vt = ([part(p, q) for p in range(count)] for q in range(4))
        mu, rho, tau = eliminate(range(count), wf, wt, vf, vt)
        nu, omega, sigma = eliminate(reversed(range(count)), vt, vf, wt, wf)
        pick = lambda values, at: sum(jnp.where(at == p, v, nil) for p, v in enumerate(values))
        tau_b, sigma_a = pick(tau, me - 1), pick(sigma, me + 1)
        mu_me, nu_me = pick(mu, me), pick(nu, me)
        wf, wt, vf, vt = (part(me, q) for q in range(4))
        det = 1.0 / ((1.0 - tau_b * wf) * (1.0 - sigma_a * vt) - (tau_b * vf) * (sigma_a * wt))
        k11, k12 = (1.0 - sigma_a * vt) * det, tau_b * vf * det
        k21, k22 = sigma_a * wt * det, (1.0 - tau_b * wf) * det
        low, high = [None] * count, [None] * count
        for p in reversed(range(count)):
            onward = -rho[p + 1] * low[p + 1] if p + 1 < count else nil
            low[p] = jnp.where(me - 1 == p, unit, jnp.where(p < me - 1, onward, nil))
        for p in range(count):
            onward = -omega[p - 1] * high[p - 1] if p else nil
            high[p] = jnp.where(me + 1 == p, unit, jnp.where(p > me + 1, onward, nil))
        table = reduced[axis]

        def put(index, value):
            for t in every:
                table[index, pl.ds(t * UNIT, UNIT), :] = jnp.broadcast_to(value[t:t + 1], (UNIT, LANES))

        for p in range(count):
            put(p, k11 * low[p] + k12 * high[p] + jnp.where(me == p, -k11 * tau_b, nil))
            put(count + 1 + p, k21 * low[p] + k22 * high[p] + jnp.where(me == p, -k21 * tau_b, nil))
        put(count, -k12 * sigma_a)
        put(2 * count + 1, -k22 * sigma_a)
        put(2 * count + 2, mu_me)
        put(2 * count + 3, nu_me)
        if axis == X:
            for p in range(count):
                put(2 * count + 4 + p, jnp.where(p < me, mu[p], unit))
                put(3 * count + 4 + p, jnp.where(p < me, unit, jnp.where(p > me, nu[p], nil)))

    def publish(axis, stage, c, g):
        count, table, way = parts[axis], reduced[axis], lax.rem(stage, 2)
        head, tail = exch[axis][way, c, g, pos[axis]], gt[c, g]
        send[axis][c, g, 1] = tail + table[2 * count + 2] * head
        send[axis][c, g, 0] = head + table[2 * count + 3] * tail
        for other in others(axis):
            sel = jnp.where(other > pos[axis], 1, 0)
            pltpu.make_async_remote_copy(
                src_ref=send[axis].at[c, g, sel], dst_ref=exch[axis].at[way, c, g, pos[axis]],
                send_sem=send_sem.at[c, g], recv_sem=recv[axis].at[way, c, g],
                device_id=device(axis, other), device_id_type=LOGICAL).start()

    def combine(axis, way, c, g, g_ss=0):
        count, table = parts[axis], reduced[axis]
        for side in range(2):
            base = side * (count + 1)
            terms = [table[base + count] * gt[c, g]] + [table[base + p] * exch[axis][way, c, g, p] for p in range(count)]
            while len(terms) > 1:
                terms = [a + b for a, b in zip(terms[::2], terms[1::2])] + terms[len(terms) // 2 * 2:]
            ss[g_ss, side] = terms[0]

    def neighbours(axis, stage, c, g, g_ss=0):
        way = lax.rem(stage, 2)
        arrived = exch[axis].at[way, c, g, pl.ds(0, parts[axis] - 1)]
        pltpu.make_async_copy(arrived, arrived, recv[axis].at[way, c, g]).wait()
        combine(axis, way, c, g, g_ss)
        pltpu.make_async_copy(arrived, arrived, send_sem.at[c, g]).wait()

    def publish_raw(c, g):
        raw[c, g, pos[X], 0] = exch[X][0, c, g, pos[X]]
        raw[c, g, pos[X], 1] = gt[c, g]

        for other in others(X):
            pltpu.make_async_remote_copy(
                src_ref=raw.at[c, g, pos[X]], dst_ref=raw.at[c, g, pos[X]], send_sem=send_sem.at[c, g], recv_sem=recv_x.at[0, c, g],
                device_id=device(X, other), device_id_type=LOGICAL).start()

    def neighbours_raw(c, g):
        arrived = raw.at[c, g, pl.ds(0, parts_x - 1)]
        pltpu.make_async_copy(arrived, arrived, recv_x.at[0, c, g]).wait()
        pltpu.make_async_copy(arrived, arrived, send_sem.at[c, g]).wait()
        count = parts_x
        for p in range(count):
            exch[X][0, c, g, p] = (red_x[2 * count + 4 + p] * raw[c, g, p, 0] + red_x[3 * count + 4 + p] * raw[c, g, p, 1])
        combine(X, 0, c, g)

    def solve_block(axis, minus):
        def coef(array, k, t):
            return array[pl.ds(k * pitch + axis * tiles + t, 1), :]

        def walk(first, sign, count, visit, state):
            def block(g, state):
                line = first + sign * deep * g
                row, coef_row = (line + 1) * PITCH, line * pitch + axis * tiles

                def one(u, state):
                    at = lambda array, t: array[pl.ds(coef_row + t + u * (sign * pitch), 1), :]
                    return visit(pl.ds(row + u * (sign * PITCH), SUB), at, state)

                return lax.fori_loop(0, min(count, deep), one, state, unroll=True)

            return lax.fori_loop(0, max(count // deep, 1), block, state)

        def eliminate(mult):
            def visit(here, at, state):
                values = list(state)
                for t in every:
                    factor = at(mult, t)
                    for c in range(chunks):
                        s = c * tiles + t
                        values[s] = rs[c, t, here, :] + factor * values[s]
                        hs[c, t, here, :] = values[s]
                return tuple(values)
            return visit

        init = tuple(blank for _ in cells)
        ups = walk(0, 1, half, eliminate(ln), init)
        downs = walk(n - 1, -1, half, eliminate(un), init)
        lo, hi = half - 1, half

        def place(c, t, here, value):
            qs[c, t, here, :] = value - rs[c, t, here, :] if minus else value

        low_s, high_s = [], []
        for s, (c, t) in enumerate(cells):
            c_lo, a_hi = coef(cn, lo, t), coef(an, hi, t)
            kappa = 1.0 / (1.0 - c_lo * a_hi)
            h_hi = coef(d2, hi, t) * downs[s]
            s_lo = kappa * (coef(m2, lo, t) * ups[s] + c_lo * h_hi)
            low_s.append(s_lo)
            high_s.append(h_hi + a_hi * s_lo)
            place(c, t, slab(lo), low_s[s])
            place(c, t, slab(hi), high_s[s])

        def substitute(scale, mult):
            def visit(here, at, state):
                values = list(state)
                for t in every:
                    own, factor = at(scale, t), at(mult, t)
                    for c in range(chunks):
                        s = c * tiles + t
                        values[s] = own * hs[c, t, here, :] + factor * values[s]
                        place(c, t, here, values[s])
                return tuple(values)
            return visit

        for first, sign, visit, state in ((lo, -1, substitute(m2, cn), low_s), (hi, 1, substitute(d2, an), high_s)):
            state = walk(first + sign, sign, deep - 1, visit, tuple(state))
            walk(first + sign * deep, sign, half - deep, visit, state)

    def each_unit(body, count=units):
        lax.fori_loop(0, count, lambda u, carry: (body(u // parts_of, lax.rem(u, parts_of)), carry)[1], 0)

    def ends_of(axis, stage, c, g):
        return exch[axis].at[lax.rem(stage, 2), c, g, pos[axis]], gt.at[c, g]

    def start_x(c):
        def unit(g, carry):
            turn(qs, rs, c, Y, X, g * UNIT, UNIT, every, ends_of(X, 0, c, g), correct=False, explicit=True)
            publish_raw(c, g)

            @pl.when((c == 0) & (g == 0))
            def _():
                spread(Y)

            return carry

        await_halo(c)
        lax.fori_loop(0, parts_of, unit, 0)

    def onward(axis, stage, to, to_stage):
        def unit(c, g):
            neighbours(axis, stage, c, g)
            turn(qs, rs, c, axis, to, g * UNIT, UNIT, every, ends_of(to, to_stage, c, g))
            publish(to, to_stage, c, g)

        each_unit(unit)

    each_chunk(start_x)
    solve_block(X, True)
    reduce_lines(X)
    reduce_lines(Y)

    def first_to_y(c, g):
        neighbours_raw(c, g)
        turn(qs, rs, c, X, Y, g * UNIT, UNIT, every, ends_of(Y, 0, c, g))
        publish(Y, 0, c, g)

    each_unit(first_to_y)

    def step(stage, carry):
        solve_block(Y, True)
        onward(Y, stage - 1, X, stage)
        solve_block(X, True)
        onward(X, stage, Y, stage)
        return carry

    lax.fori_loop(1, STEPS, step, 0)
    solve_block(Y, False)

    def finish(c, g):
        neighbours(Y, STEPS - 1, c, g)
        turn(qs, out, c, Y, X, g * UNIT, UNIT, every, scale=0.5, step_out=SUB)

    each_unit(finish, units - parts_of)
    for g in range(parts_of):
        neighbours(Y, STEPS - 1, chunks - 1, g, g)


def finish_kernel(done, qs, w2, v2, ss, out, fresh, sem):
    last, tiles, lines = done.shape[0] - 1, done.shape[1], done.shape[2] // SUB
    pitch = 2 * tiles

    def place(c, t, src, whole=False):
        step = lines if whole else LANES // 2
        for first in range(0, lines, step):
            copy = pltpu.make_async_copy(src.at[pl.ds(first * SUB, step * SUB)].reshape(step, SUB, LANES),
                                         out.at[pl.ds(first, step), pl.ds(c * SUB, SUB), pl.ds(t * LANES, LANES)], sem.at[c * tiles + t])
            if whole:
                copy.wait()
            else:
                copy.start()

    for c in range(last):
        for t in range(tiles):
            place(c, t, done.at[c, t])
    for kt in range(tiles):
        def column(f, carry):
            for lt in range(tiles):
                rows = pl.ds(kt * LANES * pitch + tiles + lt, LANES, stride=pitch)
                block = qs[last, lt, pl.ds((kt * LANES + 1) * PITCH + f, LANES, stride=PITCH), :]
                near, far = (ss[f // UNIT, side, pl.ds(lt * UNIT + f % UNIT, 1), :] for side in range(2))
                block = block + w2[rows, :] * near + v2[rows, :] * far
                fresh[kt, pl.ds(lt * LANES * SUB + f, LANES, stride=SUB), :] = (block * 0.5).T
            return carry

        lax.fori_loop(0, SUB, column, 0, unroll=True)
        place(last, kt, fresh.at[kt])
    for c in range(last + 1):
        for t in range(tiles):
            place(c, t, done.at[c, t] if c < last else fresh.at[t], whole=True)


def solution(mesh):
    parts_x, parts_y = mesh.shape["row"], mesh.shape["col"]
    strides, stride = {}, 1
    for name in reversed(mesh.axis_names):
        strides[name], stride = stride, stride * mesh.shape[name]
    field_spec = P(("batch", "row"), "col", None)
    coeff_spec = P(("batch", "row"), "col")

    def local_steps(field, *coeffs):
        n, fields = field.shape[0], field.shape[2]
        tiles, chunks = n // LANES, fields // SUB
        packed = pltpu.VMEM((n * 2 * tiles, LANES), F32)
        plane = -(-((n + 2) * PITCH - SUB) // (4 * SUB)) * 4 * SUB + SUB
        big = pltpu.VMEM((chunks, tiles, plane, LANES), F32)
        dma = pltpu.SemaphoreType.DMA
        parts_of = SUB // UNIT
        sends = pltpu.VMEM((chunks, parts_of, 2, tiles * UNIT, LANES), F32)
        line = lambda count: pltpu.VMEM((2, chunks, parts_of, count, tiles * UNIT, LANES), F32)
        table = lambda count: pltpu.VMEM((4 * count + 4, tiles * UNIT, LANES), F32)
        small = pltpu.VMEM((2, chunks, tiles, SUB, LANES), F32)
        message = (4 * tiles, LANES)
        scratch = [
            pltpu.VMEM((6, n, n), F32), big, big, *([packed] * 15),
            pltpu.VMEM((2,) + message, F32), pltpu.VMEM((parts_x,) + message, F32), pltpu.VMEM((parts_y,) + message, F32),
            table(parts_x), table(parts_y), sends, sends, line(parts_x), line(parts_y),
            pltpu.VMEM((chunks, parts_of, parts_x, 2, tiles * UNIT, LANES), F32), pltpu.VMEM((chunks, parts_of, tiles * UNIT, LANES), F32),
            small, small, dma, dma, dma((chunks, parts_of)), dma((2, chunks, parts_of)), dma((2, chunks, parts_of)), dma((2,)),
        ]
        in_hbm = pl.BlockSpec(memory_space=pltpu.HBM)
        turned = jnp.transpose(field, (0, 2, 1))
        in_vmem = pl.BlockSpec(memory_space=pltpu.VMEM)
        shape = lambda *dims: jax.ShapeDtypeStruct(dims, F32)
        handed = (shape(chunks, tiles, n * SUB, LANES), shape(chunks, tiles, plane, LANES), shape(n * 2 * tiles, LANES),
                  shape(n * 2 * tiles, LANES), shape(parts_of, 2, tiles * UNIT, LANES))
        handed = pl.pallas_call(
            functools.partial(adi_kernel, (("row", parts_x), ("col", parts_y)), strides),
            out_shape=handed, in_specs=[in_hbm] * 7, out_specs=(in_vmem,) * len(handed), scratch_shapes=scratch,
            compiler_params=pltpu.CompilerParams(
                collective_id=0, has_side_effects=True, vmem_limit_bytes=36 * 1024 * 1024),
            name="adi_steps",
        )(*(pltpu.with_memory_space_constraint(array, pltpu.HBM) for array in (turned,) + coeffs))
        result = pl.pallas_call(
            finish_kernel, out_shape=jax.ShapeDtypeStruct(turned.shape, F32),
            in_specs=[in_vmem] * len(handed), out_specs=in_hbm,
            scratch_shapes=[pltpu.VMEM((tiles, n * SUB, LANES), F32), dma((chunks * tiles,))],
            compiler_params=pltpu.CompilerParams(vmem_limit_bytes=8 * 1024 * 1024), name="finish",
        )(*handed)
        return jnp.transpose(result, (0, 2, 1))

    return jax.shard_map(local_steps, mesh=mesh, in_specs=(field_spec,) + (coeff_spec,) * 6, out_specs=field_spec, check_vma=False)
```
